16 devices in a mesh: dp: 2 (over z), fsdp: 8 (over y, x, core).
Axes of the slice: x: 2, y: 2, z: 2, core: 2. Of those that a mesh axis runs over, the one named last changes fastest.
Arguments:
- tokens: bfloat16 [256, 128, 2560], P(('dp', 'fsdp')), parts along dimension 0
- gain_in: bfloat16 [2560], P('fsdp')
- w_dq: bfloat16 [2560, 768], P('fsdp')
- gain_q: bfloat16 [768], P('fsdp')
- w_uq: bfloat16 [768, 3840], P('fsdp')
- w_dkv: bfloat16 [2560, 288], P('fsdp')
- gain_kv: bfloat16 [256], P('fsdp')
- w_ukv: bfloat16 [256, 5120], P('fsdp')
- w_out: bfloat16 [2560, 2560], P('fsdp')
Outputs:
- output 1: bfloat16 [256, 128, 2560], P(('dp', 'fsdp')), parts along dimension 0
- output 2: bfloat16 [256, 128, 256], P(('dp', 'fsdp')), parts along dimension 0
- output 3: bfloat16 [256, 128, 32], P(('dp', 'fsdp')), parts along dimension 0
There are 2 independent parts. The reference program is written for one: setup_inputs(seed, part) draws one part's arguments, and reference() takes and returns one part's arrays. A program takes and returns all parts, laid end to end along the dimension named above; an argument that names none is the same for every part.
All inputs are finite; a program needn't handle non-finite values.
Results may differ from the reference program's by a relative error of at most 0.00647502.
Values are sent between devices in bfloat16 or wider.
A program may use at most 1 GiB of HBM per device.

```python
import jax
import jax.numpy as jnp
from jax import lax

PROMPTS = 128
SEQ_LEN = 128
D_MODEL = 2560
N_HEADS = 40
Q_RANK = 768
KV_RANK = 256
NOPE_DIM = 64
ROPE_DIM = 32
V_DIM = 64
EPSILON = 1e-6
ROPE_THETA = 10000.0


def setup_inputs(seed: int = 0, part: int = 0) -> dict:
    key_list = jax.random.split(jax.random.key(seed), 9)

    def draw_weight(sub_key, n_rows, n_cols):
        drawn = jax.random.normal(sub_key, (n_rows, n_cols), jnp.float32) * (n_rows ** -0.5)
        return drawn.astype(jnp.bfloat16)

    def draw_gain(sub_key, n_items, centre):
        drawn = centre * (1.0 + 0.3 * jax.random.normal(sub_key, (n_items,), jnp.float32))
        return drawn.astype(jnp.bfloat16)

    tok_key = jax.random.fold_in(key_list[0], part)
    tokens = jax.random.normal(tok_key, (PROMPTS, SEQ_LEN, D_MODEL), jnp.float32).astype(jnp.bfloat16)
    return {
        'tokens': tokens,
        'gain_in': draw_gain(key_list[1], D_MODEL, 1.0),
        'w_dq': draw_weight(key_list[2], D_MODEL, Q_RANK),
        'gain_q': draw_gain(key_list[3], Q_RANK, 2.0),
        'w_uq': draw_weight(key_list[4], Q_RANK, N_HEADS * (NOPE_DIM + ROPE_DIM)),
        'w_dkv': draw_weight(key_list[5], D_MODEL, KV_RANK + ROPE_DIM),
        'gain_kv': draw_gain(key_list[6], KV_RANK, 1.0),
        'w_ukv': draw_weight(key_list[7], KV_RANK, N_HEADS * (NOPE_DIM + V_DIM)),
        'w_out': draw_weight(key_list[8], N_HEADS * V_DIM, D_MODEL),
    }


def rms_scale(values_in, gain_vec):
    values_f32 = values_in.astype(jnp.float32)
    inv_rms = lax.rsqrt(jnp.mean(values_f32 * values_f32, axis=-1, keepdims=True) + EPSILON)
    return values_f32 * inv_rms * gain_vec.astype(jnp.float32)


def rope_tables():
    half_dim = ROPE_DIM // 2
    inv_freq = ROPE_THETA ** (-2.0 * jnp.arange(half_dim, dtype=jnp.float32) / ROPE_DIM)
    angles = jnp.arange(SEQ_LEN, dtype=jnp.float32)[:, None] * inv_freq[None, :]
    return jnp.cos(angles), jnp.sin(angles)


def apply_rope(values_in, cos_t, sin_t):
    half_dim = values_in.shape[-1] // 2
    lo_half = values_in[..., :half_dim]
    hi_half = values_in[..., half_dim:]
    return jnp.concatenate([lo_half * cos_t - hi_half * sin_t, hi_half * cos_t + lo_half * sin_t], axis=-1)


def one_prompt(tok_rows, gain_in, w_dq, gain_q, w_uq, w_dkv, gain_kv, w_ukv, w_out):
    cos_t, sin_t = rope_tables()
    normed = rms_scale(tok_rows, gain_in).astype(jnp.bfloat16)
    q_down = jnp.dot(normed, w_dq, preferred_element_type=jnp.float32)
    q_lat = rms_scale(q_down, gain_q).astype(jnp.bfloat16)
    q_full = jnp.dot(q_lat, w_uq, preferred_element_type=jnp.float32).reshape(SEQ_LEN, N_HEADS, NOPE_DIM + ROPE_DIM)
    q_nope = q_full[:, :, :NOPE_DIM].astype(jnp.bfloat16)
    q_pe = apply_rope(q_full[:, :, NOPE_DIM:], cos_t[:, None, :], sin_t[:, None, :]).astype(jnp.bfloat16)
    kv_down = jnp.dot(normed, w_dkv, preferred_element_type=jnp.float32)
    latent = rms_scale(kv_down[:, :KV_RANK], gain_kv).astype(jnp.bfloat16)
    k_pe = apply_rope(kv_down[:, KV_RANK:], cos_t, sin_t).astype(jnp.bfloat16)
    kv_up = jnp.dot(latent, w_ukv, preferred_element_type=jnp.float32).astype(jnp.bfloat16)
    kv_up = kv_up.reshape(SEQ_LEN, N_HEADS, NOPE_DIM + V_DIM)
    k_nope = kv_up[:, :, :NOPE_DIM].astype(jnp.float32)
    values = kv_up[:, :, NOPE_DIM:].astype(jnp.float32)
    score_scale = (NOPE_DIM + ROPE_DIM) ** -0.5
    scores = jnp.einsum('qhd,khd->hqk', q_nope.astype(jnp.float32), k_nope)
    scores = scores + jnp.einsum('qhd,kd->hqk', q_pe.astype(jnp.float32), k_pe.astype(jnp.float32))
    causal = jnp.arange(SEQ_LEN)[:, None] >= jnp.arange(SEQ_LEN)[None, :]
    scores = jnp.where(causal[None, :, :], scores * score_scale, -1e30)
    attn_probs = jax.nn.softmax(scores, axis=-1).astype(jnp.bfloat16)
    attn_out = jnp.einsum('hqk,khd->qhd', attn_probs.astype(jnp.float32), values).astype(jnp.bfloat16)
    attn_out = attn_out.reshape(SEQ_LEN, N_HEADS * V_DIM)
    proj_out = jnp.dot(attn_out, w_out, preferred_element_type=jnp.float32)
    y_rows = (tok_rows.astype(jnp.float32) + proj_out).astype(jnp.bfloat16)
    return y_rows, latent, k_pe


def reference(tokens, gain_in, w_dq, gain_q, w_uq, w_dkv, gain_kv, w_ukv, w_out):
    def per_prompt(tok_rows):
        return one_prompt(tok_rows, gain_in, w_dq, gain_q, w_uq, w_dkv, gain_kv, w_ukv, w_out)

    y_out, kv_cache, pe_cache = lax.map(per_prompt, tokens)
    return (y_out, kv_cache, pe_cache)
```

```python
import functools
import jax, jax.numpy as jnp
from jax import lax
from jax.experimental import pallas as pl
from jax.experimental.pallas import tpu as pltpu
F32, BF16 = jnp.float32, jnp.bfloat16
EPS = 1e-6
T, D, QR, KR, RD, H, ND, VD = 2048, 2560, 768, 256, 32, 40, 64, 64
S = 128
LOG2E = 1.4426950408889634
SC = (ND + RD) ** -0.5 * LOG2E

def dot(a, b):
    return jnp.dot(a, b, preferred_element_type=F32)

def down_kernel(x_ref, g1_ref, wdq_ref, gq_ref, wkv_ref, gkv_ref, cos_ref, sin_ref, cqT_ref, c_ref, cT_ref, r_ref):
    x = x_ref[...].astype(F32)
    inv = lax.rsqrt(jnp.mean(x * x, axis=-1, keepdims=True) + EPS)
    a = (x * inv * g1_ref[...].astype(F32)).astype(BF16)
    qd = dot(a, wdq_ref[...])
    inv = lax.rsqrt(jnp.mean(qd * qd, axis=-1, keepdims=True) + EPS)
    cq = (qd * inv * gq_ref[...].astype(F32)).astype(BF16)
    cqT_ref[...] = cq.T
    kd = dot(a, wkv_ref[...])
    kc = kd[:, :KR]
    inv = lax.rsqrt(jnp.mean(kc * kc, axis=-1, keepdims=True) + EPS)
    c = (kc * inv * gkv_ref[...].astype(F32)).astype(BF16)
    c_ref[...] = c
    cT_ref[...] = c.T
    kp = kd[:, KR:]
    lo, hi = kp[:, :16], kp[:, 16:]
    co, si = cos_ref[...], sin_ref[...]
    r_ref[...] = jnp.concatenate([lo * co - hi * si, hi * co + lo * si], axis=-1).astype(BF16)

def down(x, g1, wdq, gq, wkv, gkv, cos, sin, tm=256):
    full = lambda shape: pl.BlockSpec(shape, lambda i: (0, 0))
    cos = jnp.tile(cos, (tm // S, 1)); sin = jnp.tile(sin, (tm // S, 1))
    return pl.pallas_call(
        down_kernel, grid=(T // tm,), name="down", cost_estimate=pl.CostEstimate(flops=2 * T * D * 1056, bytes_accessed=20 << 20, transcendentals=0),
        in_specs=[pl.BlockSpec((tm, D), lambda i: (i, 0)), full((1, D)), full((D, QR)), full((1, QR)), full((D, KR + RD)), full((1, KR)), full((tm, 16)), full((tm, 16))],
        out_specs=[pl.BlockSpec((QR, tm), lambda i: (0, i)), pl.BlockSpec((tm, KR), lambda i: (i, 0)), pl.BlockSpec((KR, tm), lambda i: (0, i)), pl.BlockSpec((tm, RD), lambda i: (i, 0))],
        out_shape=[jax.ShapeDtypeStruct((QR, T), BF16), jax.ShapeDtypeStruct((T, KR), BF16), jax.ShapeDtypeStruct((KR, T), BF16), jax.ShapeDtypeStruct((T, RD), BF16)],
        compiler_params=pltpu.CompilerParams(vmem_limit_bytes=60 << 20),
    )(x, g1, wdq, gq, wkv, gkv, cos, sin)

HG = 8
TC = 512
def attn_unit(k, qT, vT, keep):
    s = dot(k, qT) * SC
    s = jnp.where(keep, s, -1e30)
    m = jnp.max(s, axis=0, keepdims=True)
    e = jnp.exp2(s - m)
    p = (e * (1.0 / jnp.sum(e, axis=0, keepdims=True))).astype(BF16)
    return dot(vT, p)

def attn_kernel(cqT_ref, c_ref, cT_ref, r_ref, wuq_ref, wukv_ref, cosT_ref, sinT_ref, o_ref, wqT, wk, wvT, qT, kbuf, vT):
    g = pl.program_id(0)
    wqT[...] = wuq_ref[...].T
    for j in range(HG // 2):
        t0 = wukv_ref[:, 256 * j:256 * j + 128]
        t1 = wukv_ref[:, 256 * j + 128:256 * j + 256]
        wk[:, 128 * j:128 * j + 128] = jnp.concatenate([t0[:, :64], t1[:, :64]], axis=1)
        wvT[128 * j:128 * j + 128, :] = jnp.concatenate([t0[:, 64:], t1[:, 64:]], axis=1).T
    for h in range(HG):
        z = 128 * h + (96 if h % 2 == 0 else 32)
        qT[z:z + 32, :] = jnp.zeros((32, TC), BF16)
    keep = lax.broadcasted_iota(jnp.int32, (S, S), 0) <= lax.broadcasted_iota(jnp.int32, (S, S), 1)
    lane = lax.broadcasted_iota(jnp.int32, (S, 128), 1)
    co, si = cosT_ref[...], sinT_ref[...]

    def chunk(tc, _):
        tok = pl.multiple_of(tc * TC, TC)
        for n in range(TC // 256):
            q = dot(wqT[...], cqT_ref[:, pl.ds(tok + 256 * n, 256)])
            cols = slice(256 * n, 256 * n + 256)
            for h in range(HG):
                nope = q[96 * h:96 * h + 64]
                lo, hi = q[96 * h + 64:96 * h + 80], q[96 * h + 80:96 * h + 96]
                b = 128 * h
                qn, qp = (b, b + 64) if h % 2 == 0 else (b + 64, b)
                qT[qn:qn + 64, cols] = nope.astype(BF16)
                qT[qp:qp + 16, cols] = (lo * co - hi * si).astype(BF16)
                qT[qp + 16:qp + 32, cols] = (hi * co + lo * si).astype(BF16)
        kbuf[...] = dot(c_ref[pl.ds(tok, TC), :], wk[...]).astype(BF16)
        vT[...] = dot(wvT[...], cT_ref[:, pl.ds(tok, TC)]).astype(BF16)

        for p in range(TC // S):
            row = p * S
            r = r_ref[pl.ds(tok + row, S), :]
            z32 = jnp.zeros((S, 32), BF16)
            z64 = jnp.zeros((S, 64), BF16)
            r_hi = jnp.concatenate([z64, r, z32], axis=1)
            r_lo = jnp.concatenate([r, z32, z64], axis=1)
            for j in range(HG // 2):
                k2 = kbuf[row:row + S, 128 * j:128 * j + 128]
                outs = []
                for par in range(2):
                    h = 2 * j + par
                    k = jnp.where(lane < 64, k2, r_hi) if par == 0 else jnp.where(lane < 64, r_lo, k2)
                    outs.append(attn_unit(k, qT[128 * h:128 * h + 128, row:row + S], vT[64 * h:64 * h + 64, row:row + S], keep))
                oT = jnp.concatenate(outs, axis=0)
                o_ref[pl.ds(tok + row, S), 128 * j:128 * j + 128] = oT.astype(BF16).T
        return 0
    lax.fori_loop(0, T // TC, chunk, 0)

def attn(cqT, c, cT, r, wuq, wukv, cosT, sinT):
    full = lambda shape: pl.BlockSpec(shape, lambda g: (0, 0))
    return pl.pallas_call(
        attn_kernel, grid=(H // HG,), name="attn", cost_estimate=pl.CostEstimate(flops=40 * 10**9, bytes_accessed=24 << 20, transcendentals=0),
        in_specs=[full((QR, T)), full((T, KR)), full((KR, T)), full((T, RD)),
                  pl.BlockSpec((QR, HG * 96), lambda g: (0, g)), pl.BlockSpec((KR, HG * 128), lambda g: (0, g)), full((16, 256)), full((16, 256))],
        out_specs=pl.BlockSpec((T, HG * 64), lambda g: (0, g)),
        out_shape=jax.ShapeDtypeStruct((T, H * VD), BF16),
        scratch_shapes=[pltpu.VMEM((HG * 96, QR), BF16), pltpu.VMEM((KR, HG * 64), BF16), pltpu.VMEM((HG * 64, KR), BF16),
                        pltpu.VMEM((HG * 128, TC), BF16), pltpu.VMEM((TC, HG * 64), BF16), pltpu.VMEM((HG * 64, TC), BF16)],
        compiler_params=pltpu.CompilerParams(vmem_limit_bytes=60 << 20),
    )(cqT, c, cT, r, wuq, wukv, cosT, sinT)

def out_kernel(o_ref, w_ref, x_ref, y_ref):
    y_ref[...] = (x_ref[...].astype(F32) + dot(o_ref[...], w_ref[...])).astype(BF16)

def outp(o, w, x, tm=512, tn=512):
    return pl.pallas_call(
        out_kernel, grid=(T // tm, D // tn), name="outp", cost_estimate=pl.CostEstimate(flops=2 * T * D * D, bytes_accessed=40 << 20, transcendentals=0),
        in_specs=[pl.BlockSpec((tm, D), lambda i, j: (i, 0)), pl.BlockSpec((D, tn), lambda i, j: (0, j)), pl.BlockSpec((tm, tn), lambda i, j: (i, j))],
        out_specs=pl.BlockSpec((tm, tn), lambda i, j: (i, j)),
        out_shape=jax.ShapeDtypeStruct((T, D), BF16),
        compiler_params=pltpu.CompilerParams(vmem_limit_bytes=60 << 20),
    )(o, w, x)

def tables():
    half = RD // 2
    inv_freq = 10000.0 ** (-2.0 * jnp.arange(half, dtype=F32) / RD)
    ang = jnp.arange(S, dtype=F32)[:, None] * inv_freq[None, :]
    return jnp.cos(ang), jnp.sin(ang)


def solution(mesh):
    from jax.sharding import PartitionSpec as P
    batch, row, mat = P(('dp', 'fsdp')), P('fsdp'), P('fsdp', None)

    def local(tok, g1, wdq, gq, wuq, wkv, gkv, wukv, wo):
        cos, sin = tables()
        gains = lax.all_gather(jnp.concatenate([g1, gq, gkv]), 'fsdp')
        g1a, gqa, gkva = (gains[:, :320].reshape(1, D), gains[:, 320:416].reshape(1, QR), gains[:, 416:].reshape(1, KR))
        ag = lambda w: lax.all_gather(w, 'fsdp', tiled=True)
        x = tok.reshape(T, D)
        cqT, c, cT, r = down(x, g1a, ag(wdq), gqa, ag(wkv), gkva, cos, sin)
        o = attn(cqT, c, cT, r, ag(wuq), ag(wukv), jnp.tile(cos.T, (1, 2)), jnp.tile(sin.T, (1, 2)))
        y = outp(o, ag(wo), x)
        return y.reshape(tok.shape), c.reshape(-1, S, KR), r.reshape(-1, S, RD)

    return jax.shard_map(local, mesh=mesh, in_specs=(batch, row, mat, row, mat, mat, row, mat, mat),
                         out_specs=(batch,) * 3, check_vma=False)
```

```python
import functools
import numpy as np
import jax
import jax.numpy as jnp
from jax import lax
from jax.experimental import pallas as pl
from jax.experimental.pallas import tpu as pltpu
from jax.sharding import PartitionSpec as P

F32, BF16 = jnp.float32, jnp.bfloat16
MESH = pl.DeviceIdType.MESH
EPS = 1e-6
T, D, QR, KR, RD, H, ND, VD = 2048, 2560, 768, 256, 32, 40, 64, 64
S = 128
SC = (ND + RD) ** -0.5 * 1.4426950408889634
HG, TC = 8, 512
NCH = T // TC
STEPS = (H // HG) * NCH
TA = 256


def dot(a, b):
    return jnp.dot(a, b, preferred_element_type=F32)


def rms(v):
    return lax.rsqrt(jnp.mean(v * v, axis=-1, keepdims=True) + EPS)


def attn_unit(k, qT, vT, keep):
    s = dot(k, qT) * SC
    s = jnp.where(keep, s, -1e30)
    m = jnp.max(s, axis=0, keepdims=True)
    e = jnp.exp2(s - m)
    p = (e * (1.0 / jnp.sum(e, axis=0, keepdims=True))).astype(BF16)
    return dot(vT, p)


PIECES = (
    ('dq', 'dq', False, 320, 0, 768, 96),
    ('dkv', 'dkv', False, 320, 0, 288, 96),
    ('uq0', 'uq', False, 96, 0, 768, 32),
    ('ukv0', 'ukv', True, 32, 0, 1024, 384),
    ('uq1', 'uq', False, 96, 768, 1536, 32),
    ('ukv1', 'ukv', True, 32, 1024, 2048, 640),
    ('uq2', 'uq', False, 96, 2304, 1536, 32),
    ('ukv2', 'ukv', True, 32, 3072, 2048, 640),
    ('o', 'o', False, 320, 0, 2560, 112),
)
PIDX = {p[0]: i for i, p in enumerate(PIECES)}
KINDS = ('XE', 'YE', 'XS', 'YS', 'S0', 'Z1', 'Z2', 'DY', 'DX', 'Z3', 'S1', 'S2', 'S3')
KIDX = {k: i for i, k in enumerate(KINDS)}
D0, U0, U1, U2, O0 = ('dq', 'dkv'), ('uq0', 'ukv0'), ('uq1', 'ukv1'), ('uq2', 'ukv2'), ('o',)


def front_kernel(x_hbm, g1_s, gq_s, gkv_s, dq_s, dkv_s, uq_s, ukv_s, o_s, cos_ref, sin_ref, cosT_ref, sinT_ref,
                 attn_hbm, wo_hbm, c_hbm, r_hbm,
                 xa, wdq, wdkv, wuq, wukv, ostage, g1b, gqb, gkvb, accq, acck, cqT, cbuf, cT, rbuf,
                 wqT, wk, wvT, qT, kbuf, vT, obuf,
                 ssem, rsem, lsem, gss, grs, xsem, osem, csem):
    z, f = lax.axis_index('dp'), lax.axis_index('fsdp')
    core, xx, yy = f % 2, (f // 2) % 2, f // 4

    def idx(dx, dy, dc):
        return ((yy + dy) % 2) * 4 + ((xx + dx) % 2) * 2 + (core + dc) % 2

    fx, fy, fd = idx(1, 0, 0), idx(0, 1, 0), idx(1, 1, 0)
    dev = {'X': (z, fx), 'Y': (z, fy), 'Z': (1 - z, f), 'S': (z, idx(0, 0, 1))}
    plane = [idx(dx, dy, dc) for dx in range(2) for dy in range(2) for dc in range(2) if dx + dy + dc]
    src = {'dq': dq_s, 'dkv': dkv_s, 'uq': uq_s, 'ukv': ukv_s, 'o': ostage}
    buf = {'dq': wdq, 'dkv': wdkv, 'uq': wuq, 'ukv': wukv, 'o': wo_hbm}

    def region(piece, shard, part, base):
        name, arr, bycol, rows, c0, nc, e = piece
        n = nc if bycol else rows
        off, size = {'E': (z * (n - e), e), 'S': (e, n - 2 * e), 'A': (0, n)}[part]
        if bycol:
            row = shard * rows if base else 0
            return pl.ds(pl.multiple_of(row, 16), rows), pl.ds(pl.multiple_of(c0 + off, 128), size)
        row = (shard * rows if base else 0) + off
        return pl.ds(pl.multiple_of(row, 16), size), pl.ds(c0, nc)

    def copy(name, kind):
        piece = PIECES[PIDX[name]]
        arr = piece[1]
        shard = {'X': f, 'Y': f}.get(kind[0]) if kind in ('XE', 'YE', 'XS', 'YS') else None
        if kind in ('XE', 'YE', 'XS', 'YS', 'S0'):
            part = 'A' if kind == 'S0' else kind[1]
            r0, c0 = region(piece, f, part, False)
            r1, c1 = region(piece, f, part, True)
            s_ref, d_ref = src[arr].at[r0, c0], buf[arr].at[r1, c1]
            to = dev[kind[0]]
        else:
            shard, part, to = {'Z1': (fx, 'E', 'Z'), 'Z2': (fy, 'E', 'Z'), 'Z3': (fd, 'E', 'Z'), 'DY': (fx, 'E', 'Y'),
                               'DX': (fy, 'S', 'X'), 'S1': (fx, 'A', 'S'), 'S2': (fy, 'A', 'S'), 'S3': (fd, 'A', 'S')}[kind]
            to = dev[to]
            r1, c1 = region(piece, shard, part, True)
            s_ref = d_ref = buf[arr].at[r1, c1]
        i, j = PIDX[name], KIDX[kind]
        return pltpu.make_async_remote_copy(src_ref=s_ref, dst_ref=d_ref, send_sem=ssem.at[i, j], recv_sem=rsem.at[i, j],
                                            device_id=to, device_id_type=MESH)

    def local(name):
        piece = PIECES[PIDX[name]]
        r0, c0 = region(piece, f, 'A', False)
        r1, c1 = region(piece, f, 'A', True)
        return pltpu.make_async_copy(src[piece[1]].at[r0, c0], buf[piece[1]].at[r1, c1], lsem.at[PIDX[name]])

    def start(names, *kinds):
        for k in kinds:
            for n in names:
                copy(n, k).start()

    def recv(names, *kinds):
        for k in kinds:
            for n in names:
                copy(n, k).wait_recv()

    def st0(names):
        start(names, 'XE', 'YE', 'XS', 'YS', 'S0')
        for n in names:
            local(n).start()

    def st1(names):
        recv(names, 'XE', 'YE')
        start(names, 'Z1', 'Z2', 'DY')

    def st2(names):
        recv(names, 'XS', 'YS')
        start(names, 'DX')

    def st3(names):
        recv(names, 'DY')
        start(names, 'Z3')

    def st4(names):
        recv(names, 'Z1')
        start(names, 'S1')
        recv(names, 'Z2')
        start(names, 'S2')

    def st5(names):
        recv(names, 'DX', 'Z3')
        start(names, 'S3')

    def stage(names):
        stage_o.wait()

    def fin(names):
        for n in names:
            local(n).wait()
        recv(names, 'S0', 'S1', 'S2', 'S3')

    for i in range(T // TA):
        pltpu.make_async_copy(x_hbm.at[pl.ds(i * TA, TA)], xa.at[pl.ds(i * TA, TA)], xsem.at[i]).start()
    stage_o = pltpu.make_async_copy(o_s, ostage, osem.at[2])
    stage_o.start()

    barrier = pltpu.get_barrier_semaphore()
    for p in plane:
        pl.semaphore_signal(barrier, inc=1, device_id=(z, p), device_id_type=MESH)
    pl.semaphore_signal(barrier, inc=1, device_id=dev['Z'], device_id_type=MESH)
    pl.semaphore_wait(barrier, 8)

    gains = []
    for j, (gs, gb) in enumerate(((g1_s, g1b), (gq_s, gqb), (gkv_s, gkvb))):
        for i, p in enumerate(plane):
            gains.append(pltpu.make_async_remote_copy(src_ref=gs, dst_ref=gb.at[f], send_sem=gss.at[j, i], recv_sem=grs.at[j, i],
                                                      device_id=(z, p), device_id_type=MESH))
            gains[-1].start()
        own = pltpu.make_async_copy(gs, gb.at[f], gss.at[j, 7])
        own.start()
        gains.append(own)
    st0(D0)
    for g in gains:
        g.wait()

    def row_of(gb):
        return jnp.concatenate([gb[i].astype(F32) for i in range(8)], axis=-1)

    g1, gq, gkv = row_of(g1b), row_of(gqb), row_of(gkvb)

    def norm_tile(i, _):
        pltpu.make_async_copy(x_hbm.at[pl.ds(i * TA, TA)], xa.at[pl.ds(i * TA, TA)], xsem.at[i]).wait()
        for h in range(TA // 64):
            rows = pl.ds(pl.multiple_of(i * TA + h * 64, 64), 64)
            v = xa[rows, :].astype(F32)
            xa[rows, :] = (v * rms(v) * g1).astype(BF16)
        return 0

    def part(quarter, first):
        cols = pl.ds(pl.multiple_of(quarter * 640, 128), 640)

        def tile(i, _):
            rows = pl.ds(pl.multiple_of(i * TA, TA), TA)
            a = xa[rows, cols]
            pq, pk = dot(a, wdq[cols, :]), dot(a, wdkv[cols, :])
            if first:
                accq[rows, :], acck[rows, :] = pq, pk
            else:
                accq[rows, :] += pq
                acck[rows, :] += pk
            return 0
        lax.fori_loop(0, T // TA, tile, 0)

    cos2 = jnp.concatenate([cos_ref[...]] * (TA // S), axis=0)
    sin2 = jnp.concatenate([sin_ref[...]] * (TA // S), axis=0)

    def last_part(quarter):
        cols = pl.ds(pl.multiple_of(quarter * 640, 128), 640)

        def tile(i, _):
            rows = pl.ds(pl.multiple_of(i * TA, TA), TA)
            a = xa[rows, cols]
            qd = accq[rows, :] + dot(a, wdq[cols, :])
            kd = acck[rows, :] + dot(a, wdkv[cols, :])
            cqT[:, rows] = (qd * rms(qd) * gq).astype(BF16).T
            kc = kd[:, :KR]
            c = (kc * rms(kc) * gkv).astype(BF16)
            cbuf[rows, :] = c
            cT[:, rows] = c.T
            lo, hi = kd[:, KR:KR + 16], kd[:, KR + 16:]
            rbuf[rows, :] = jnp.concatenate([lo * cos2 - hi * sin2, hi * cos2 + lo * sin2], axis=-1).astype(BF16)
            return 0
        lax.fori_loop(0, T // TA, tile, 0)

    lax.fori_loop(0, 4, norm_tile, 0)
    st1(D0)
    lax.fori_loop(4, 8, norm_tile, 0)
    for n in D0:
        local(n).wait()
    recv(D0, 'S0')
    part(f // 2, True)
    st2(D0)
    st0(U0)
    st3(D0)
    st4(D0)
    recv(D0, 'S1')
    part(fx // 2, False)
    st5(D0)
    st1(U0)
    recv(D0, 'S2')
    part(fy // 2, False)
    st2(U0)
    st0(U1)
    st3(U0)
    recv(D0, 'S3')
    last_part(fd // 2)
    outs = [pltpu.make_async_copy(cbuf, c_hbm, csem.at[0]), pltpu.make_async_copy(rbuf, r_hbm, csem.at[1])]
    for o in outs:
        o.start()
    st4(U0)
    st5(U0)
    fin(U0)

    keep = lax.broadcasted_iota(jnp.int32, (S, S), 0) <= lax.broadcasted_iota(jnp.int32, (S, S), 1)
    lane = lax.broadcasted_iota(jnp.int32, (S, 128), 1)
    co, si = cosT_ref[...], sinT_ref[...]
    for h in range(HG):
        zr = 128 * h + (96 if h % 2 == 0 else 32)
        qT[zr:zr + 32, :] = jnp.zeros((32, TC), BF16)

    def load_group(g):
        uc = pl.ds(pl.multiple_of(g * (HG * 96), 128), HG * 96)
        wqT[...] = wuq[:, uc].T
        for j in range(HG // 2):
            t0 = wukv[:, pl.ds(pl.multiple_of(g * (HG * 128) + 256 * j, 128), 128)]
            t1 = wukv[:, pl.ds(pl.multiple_of(g * (HG * 128) + 256 * j + 128, 128), 128)]
            wk[:, 128 * j:128 * j + 128] = jnp.concatenate([t0[:, :64], t1[:, :64]], axis=1)
            wvT[128 * j:128 * j + 128, :] = jnp.concatenate([t0[:, 64:], t1[:, 64:]], axis=1).T

    def out_copy(i):
        g, tc = i // NCH, i % NCH
        return pltpu.make_async_copy(obuf.at[i % 2], attn_hbm.at[pl.ds(pl.multiple_of(tc * TC, TC), TC), pl.ds(pl.multiple_of(g * (HG * 64), 128), HG * 64)], osem.at[i % 2])

    sched = {
        0: ((st1, U1),),
        1: ((st2, U1), (st0, U2), (st3, U1)),
        2: ((st4, U1), (st5, U1), (st1, U2)),
        3: ((st2, U2), (stage, O0), (st0, O0), (st3, U2)),
        4: ((fin, U1), (st4, U2), (st5, U2)),
        6: ((fin, U2),),
        7: ((st1, O0),),
        10: ((st2, O0), (st3, O0)),
        13: ((st4, O0),),
        15: ((st5, O0),),
    }

    def act(todo):
        for fn, names in todo:
            fn(names)

    def step(i, _):
        g, tc = i // NCH, i % NCH
        tok = pl.multiple_of(tc * TC, TC)
        for s, todo in sched.items():
            pl.when(i == s)(functools.partial(act, todo))

        @pl.when(tc == 0)
        def _():
            load_group(g)

        @pl.when(i >= 2)
        def _():
            out_copy(i - 2).wait()

        slot = i % 2
        for n in range(TC // 256):
            q = dot(wqT[...], cqT[:, pl.ds(tok + 256 * n, 256)])
            cols = slice(256 * n, 256 * n + 256)
            for h in range(HG):
                nope = q[96 * h:96 * h + 64]
                lo, hi = q[96 * h + 64:96 * h + 80], q[96 * h + 80:96 * h + 96]
                b = 128 * h
                qn, qp = (b, b + 64) if h % 2 == 0 else (b + 64, b)
                qT[qn:qn + 64, cols] = nope.astype(BF16)
                qT[qp:qp + 16, cols] = (lo * co - hi * si).astype(BF16)
                qT[qp + 16:qp + 32, cols] = (hi * co + lo * si).astype(BF16)
        kbuf[...] = dot(cbuf[pl.ds(tok, TC), :], wk[...]).astype(BF16)
        vT[...] = dot(wvT[...], cT[:, pl.ds(tok, TC)]).astype(BF16)

        for p in range(TC // S):
            row = p * S
            r = rbuf[pl.ds(tok + row, S), :]
            z32, z64 = jnp.zeros((S, 32), BF16), jnp.zeros((S, 64), BF16)
            r_hi = jnp.concatenate([z64, r, z32], axis=1)
            r_lo = jnp.concatenate([r, z32, z64], axis=1)
            for j in range(HG // 2):
                k2 = kbuf[row:row + S, 128 * j:128 * j + 128]
                both = []
                for par in range(2):
                    h = 2 * j + par
                    k = jnp.where(lane < 64, k2, r_hi) if par == 0 else jnp.where(lane < 64, r_lo, k2)
                    both.append(attn_unit(k, qT[128 * h:128 * h + 128, row:row + S], vT[64 * h:64 * h + 64, row:row + S], keep))
                obuf[slot, row:row + S, 128 * j:128 * j + 128] = jnp.concatenate(both, axis=0).astype(BF16).T
        out_copy(i).start()
        return 0

    lax.fori_loop(0, STEPS, step, 0)
    fin(O0)
    for i in (STEPS - 2, STEPS - 1):
        out_copy(i).wait()
    for o in outs:
        o.wait()
    for p in PIECES:
        for k in KINDS:
            copy(p[0], k).wait_send()


def front(x, gains, ws, cos, sin):
    anyspace, vm = pl.BlockSpec(memory_space=pl.ANY), pl.BlockSpec(memory_space=pltpu.VMEM)
    V = pltpu.VMEM
    dma = pltpu.SemaphoreType.DMA
    tab = [cos, sin, np.tile(cos.T, (1, 2)), np.tile(sin.T, (1, 2))]
    return pl.pallas_call(
        front_kernel, name='front',
        in_specs=[anyspace] + [vm] * 3 + [anyspace] * 5 + [vm] * 4,
        out_specs=[anyspace] * 4,
        out_shape=[jax.ShapeDtypeStruct((T, H * VD), BF16), jax.ShapeDtypeStruct((H * VD, D), BF16), jax.ShapeDtypeStruct((T, KR), BF16), jax.ShapeDtypeStruct((T, RD), BF16)],
        scratch_shapes=[
            V((T, D), BF16), V((D, QR), BF16), V((D, KR + RD), BF16), V((QR, H * 96), BF16), V((KR, H * 128), BF16), V((320, D), BF16),
            V((8, 1, 320), BF16), V((8, 1, 96), BF16), V((8, 1, 32), BF16), V((T, QR), F32), V((T, KR + RD), F32),
            V((QR, T), BF16), V((T, KR), BF16), V((KR, T), BF16), V((T, RD), BF16),
            V((HG * 96, QR), BF16), V((KR, HG * 64), BF16), V((HG * 64, KR), BF16), V((HG * 128, TC), BF16), V((TC, HG * 64), BF16), V((HG * 64, TC), BF16), V((2, TC, HG * 64), BF16),
            dma((len(PIECES), len(KINDS))), dma((len(PIECES), len(KINDS))), dma((len(PIECES),)), dma((3, 8)), dma((3, 7)), dma((T // TA,)), dma((3,)), dma((2,)),
        ],
        compiler_params=pltpu.CompilerParams(collective_id=0, has_side_effects=True, vmem_limit_bytes=63 << 20),
    )(x, *gains, *ws, *(jnp.asarray(t) for t in tab))


def out_kernel(o_ref, w_ref, x_ref, c_ref, r_ref, y_ref, c_out, r_out):
    y_ref[...] = (x_ref[...].astype(F32) + dot(o_ref[...], w_ref[...])).astype(BF16)

    @pl.when(pl.program_id(1) == 0)
    def _():
        c_out[...] = c_ref[...]
        r_out[...] = r_ref[...]


def outp(o, w, x, c, r, tm=512, tn=512):
    return pl.pallas_call(
        out_kernel, grid=(T // tm, D // tn), name='outp',
        in_specs=[pl.BlockSpec((tm, D), lambda i, j: (i, 0)), pl.BlockSpec((D, tn), lambda i, j: (0, j)), pl.BlockSpec((tm, tn), lambda i, j: (i, j)),
                  pl.BlockSpec((tm, KR), lambda i, j: (i, 0)), pl.BlockSpec((tm, RD), lambda i, j: (i, 0))],
        out_specs=[pl.BlockSpec((tm, tn), lambda i, j: (i, j)), pl.BlockSpec((tm, KR), lambda i, j: (i, 0)), pl.BlockSpec((tm, RD), lambda i, j: (i, 0))],
        out_shape=[jax.ShapeDtypeStruct((T, D), BF16), jax.ShapeDtypeStruct((T, KR), BF16), jax.ShapeDtypeStruct((T, RD), BF16)],
        compiler_params=pltpu.CompilerParams(vmem_limit_bytes=60 << 20),
    )(o, w, x, c, r)


def tables():
    half = RD // 2
    freq = np.float32(10000.0) ** (np.float32(-2.0) * np.arange(half, dtype=np.float32) / np.float32(RD))
    ang = np.arange(S, dtype=np.float32)[:, None] * freq[None, :].astype(np.float32)
    return np.cos(ang).astype(np.float32), np.sin(ang).astype(np.float32)


def solution(mesh):
    batch, row, mat = P(('dp', 'fsdp')), P('fsdp'), P('fsdp', None)

    def local(tok, g1, wdq, gq, wuq, wkv, gkv, wukv, wo):
        cos, sin = tables()
        x = tok.reshape(T, D)
        o, w, c, r = front(x, (g1[None], gq[None], gkv[None]), (wdq, wkv, wuq, wukv, wo), cos, sin)
        y, c, r = outp(o, w, x, c, r)
        return y.reshape(tok.shape), c.reshape(-1, S, KR), r.reshape(-1, S, RD)

    return jax.shard_map(local, mesh=mesh, in_specs=(batch, row, mat, row, mat, mat, row, mat, mat),
                         out_specs=(batch,) * 3, check_vma=False)
```

```python
import functools
import numpy as np
import jax
import jax.numpy as jnp
from jax import lax
from jax.experimental import pallas as pl
from jax.experimental.pallas import tpu as pltpu
from jax.sharding import PartitionSpec as P

F32, BF16 = jnp.float32, jnp.bfloat16
MESH = pl.DeviceIdType.MESH
EPS = 1e-6
T, D, QR, KR, RD, H, ND, VD = 2048, 2560, 768, 256, 32, 40, 64, 64
S = 128
SC = (ND + RD) ** -0.5 * 1.4426950408889634
HG, TC = 8, 512
NCH = T // TC
STEPS = (H // HG) * NCH
TA = 256


def dot(a, b):
    return jnp.dot(a, b, preferred_element_type=F32)


def rms(v):
    return lax.rsqrt(jnp.mean(v * v, axis=-1, keepdims=True) + EPS)


def attn_unit(k, qT, vT, keep):
    s = dot(k, qT) * SC
    s = jnp.where(keep, s, -1e30)
    m = jnp.max(s, axis=0, keepdims=True)
    e = jnp.exp2(s - m)
    p = (e * (1.0 / jnp.sum(e, axis=0, keepdims=True))).astype(BF16)
    return dot(vT, p)


PIECES = (
    ('dq', 'dq', False, 320, 0, 768, 96),
    ('dkv', 'dkv', False, 320, 0, 288, 96),
    ('uq0', 'uq', False, 96, 0, 768, 32),
    ('ukv0', 'ukv', True, 32, 0, 1024, 384),
    ('uq1', 'uq', False, 96, 768, 1536, 32),
    ('ukv1', 'ukv', True, 32, 1024, 2048, 640),
    ('uq2', 'uq', False, 96, 2304, 1536, 32),
    ('ukv2', 'ukv', True, 32, 3072, 2048, 640),
    ('o0', 'o', False, 320, 0, 640, 112),
    ('o1', 'o', False, 320, 640, 640, 112),
    ('o2', 'o', False, 320, 1280, 640, 112),
    ('o3', 'o', False, 320, 1920, 640, 112),
)
PIDX = {p[0]: i for i, p in enumerate(PIECES)}
KINDS = ('XE', 'YE', 'XS', 'YS', 'S0', 'Z1', 'Z2', 'DY', 'DX', 'Z3', 'S1', 'S2', 'S3')
KIDX = {k: i for i, k in enumerate(KINDS)}
D0, U0, U1, U2 = ('dq', 'dkv'), ('uq0', 'ukv0'), ('uq1', 'ukv1'), ('uq2', 'ukv2')
O0, O1, O2, O3 = ('o0',), ('o1',), ('o2',), ('o3',)


def front_kernel(x_hbm, g1_s, gq_s, gkv_s, dq_s, dkv_s, uq_s, ukv_s, o_s, cos_ref, sin_ref, cosT_ref, sinT_ref,
                 attn_hbm, wo_hbm, c_hbm, r_hbm,
                 xa, wdq, wdkv, wuq, wukv, ostage, g1b, gqb, gkvb, accq, acck, inv, cqT, cbuf, cT, rbuf, rT,
                 wqT, wk, wvT, qT, kbuf, vT, obuf,
                 ssem, rsem, lsem, gss, grs, xsem, osem, csem):
    z, f = lax.axis_index('dp'), lax.axis_index('fsdp')
    core, xx, yy = f % 2, (f // 2) % 2, f // 4

    def idx(dx, dy, dc):
        return ((yy + dy) % 2) * 4 + ((xx + dx) % 2) * 2 + (core + dc) % 2

    fx, fy, fd = idx(1, 0, 0), idx(0, 1, 0), idx(1, 1, 0)
    dev = {'X': (z, fx), 'Y': (z, fy), 'Z': (1 - z, f), 'S': (z, idx(0, 0, 1))}
    plane = [idx(dx, dy, dc) for dx in range(2) for dy in range(2) for dc in range(2) if dx + dy + dc]
    src = {'dq': dq_s, 'dkv': dkv_s, 'uq': uq_s, 'ukv': ukv_s, 'o': ostage}
    buf = {'dq': wdq, 'dkv': wdkv, 'uq': wuq, 'ukv': wukv, 'o': wo_hbm}

    def region(piece, shard, part, base):
        name, arr, bycol, rows, c0, nc, e = piece
        n = nc if bycol else rows
        off, size = {'E': (z * (n - e), e), 'S': (e, n - 2 * e), 'A': (0, n)}[part]
        if bycol:
            row = shard * rows if base else 0
            return pl.ds(pl.multiple_of(row, 16), rows), pl.ds(pl.multiple_of(c0 + off, 128), size)
        row = (shard * rows if base else 0) + off
        return pl.ds(pl.multiple_of(row, 16), size), pl.ds(c0, nc)

    def copy(name, kind):
        piece = PIECES[PIDX[name]]
        arr = piece[1]
        shard = {'X': f, 'Y': f}.get(kind[0]) if kind in ('XE', 'YE', 'XS', 'YS') else None
        if kind in ('XE', 'YE', 'XS', 'YS', 'S0'):
            part = 'A' if kind == 'S0' else kind[1]
            r0, c0 = region(piece, f, part, False)
            r1, c1 = region(piece, f, part, True)
            s_ref, d_ref = src[arr].at[r0, c0], buf[arr].at[r1, c1]
            to = dev[kind[0]]
        else:
            shard, part, to = {'Z1': (fx, 'E', 'Z'), 'Z2': (fy, 'E', 'Z'), 'Z3': (fd, 'E', 'Z'), 'DY': (fx, 'E', 'Y'),
                               'DX': (fy, 'S', 'X'), 'S1': (fx, 'A', 'S'), 'S2': (fy, 'A', 'S'), 'S3': (fd, 'A', 'S')}[kind]
            to = dev[to]
            r1, c1 = region(piece, shard, part, True)
            s_ref = d_ref = buf[arr].at[r1, c1]
        i, j = PIDX[name], KIDX[kind]
        return pltpu.make_async_remote_copy(src_ref=s_ref, dst_ref=d_ref, send_sem=ssem.at[i, j], recv_sem=rsem.at[i, j],
                                            device_id=to, device_id_type=MESH)

    def local(name):
        piece = PIECES[PIDX[name]]
        r0, c0 = region(piece, f, 'A', False)
        r1, c1 = region(piece, f, 'A', True)
        return pltpu.make_async_copy(src[piece[1]].at[r0, c0], buf[piece[1]].at[r1, c1], lsem.at[PIDX[name]])

    def start(names, *kinds):
        for k in kinds:
            for n in names:
                copy(n, k).start()

    def recv(names, *kinds):
        for k in kinds:
            for n in names:
                copy(n, k).wait_recv()

    def st0(names):
        start(names, 'XE', 'YE', 'XS', 'YS', 'S0')
        for n in names:
            local(n).start()

    def st1(names):
        recv(names, 'XE', 'YE')
        start(names, 'Z1', 'Z2', 'DY')

    def st2(names):
        recv(names, 'XS', 'YS')
        start(names, 'DX')

    def st3(names):
        recv(names, 'DY')
        start(names, 'Z3')

    def st4x(names):
        recv(names, 'Z1')
        start(names, 'S1')

    def st4y(names):
        recv(names, 'Z2')
        start(names, 'S2')

    def st4(names):
        st4x(names)
        st4y(names)

    def st5(names):
        recv(names, 'DX', 'Z3')
        start(names, 'S3')

    def stage(names):
        stage_o.wait()

    def fin(names):
        for n in names:
            local(n).wait()
        recv(names, 'S0', 'S1', 'S2', 'S3')

    def act(*todo):
        stages = {'st0': st0, 'st1': st1, 'st2': st2, 'st3': st3, 'st4': st4, 'st4x': st4x, 'st4y': st4y, 'st5': st5, 'fin': fin, 'stage': stage}
        for k in range(0, len(todo), 2):
            stages[todo[k]](todo[k + 1])

    for i in range(T // TA):
        pltpu.make_async_copy(x_hbm.at[pl.ds(i * TA, TA)], xa.at[pl.ds(i * TA, TA)], xsem.at[i]).start()
    stage_o = pltpu.make_async_copy(o_s, ostage, osem.at[2])
    stage_o.start()

    barrier = pltpu.get_barrier_semaphore()
    with jax.named_scope('barrier'):
        for p in plane:
            pl.semaphore_signal(barrier, inc=1, device_id=(z, p), device_id_type=MESH)
        pl.semaphore_signal(barrier, inc=1, device_id=dev['Z'], device_id_type=MESH)
        pl.semaphore_wait(barrier, 8)

    gains = []
    for j, (gs, gb) in enumerate(((g1_s, g1b), (gq_s, gqb), (gkv_s, gkvb))):
        for i, p in enumerate(plane):
            gains.append(pltpu.make_async_remote_copy(src_ref=gs, dst_ref=gb.at[f], send_sem=gss.at[j, i], recv_sem=grs.at[j, i],
                                                      device_id=(z, p), device_id_type=MESH))
            gains[-1].start()
        own = pltpu.make_async_copy(gs, gb.at[f], gss.at[j, 7])
        own.start()
        gains.append(own)
    st0(D0)

    def stat_tile(i, _):
        pltpu.make_async_copy(x_hbm.at[pl.ds(i * TA, TA)], xa.at[pl.ds(i * TA, TA)], xsem.at[i]).wait()
        for h in range(TA // 64):
            rows = pl.ds(pl.multiple_of(i * TA + h * 64, 64), 64)
            inv[rows, :] = jnp.broadcast_to(rms(xa[rows, :].astype(F32)), (64, 128))
        return 0

    with jax.named_scope('stats'):
        lax.fori_loop(0, T // TA, stat_tile, 0)
    with jax.named_scope('gains'):
        for g in gains:
            g.wait()

    def row_of(gb):
        return jnp.concatenate([gb[i].astype(F32) for i in range(8)], axis=-1)

    g1, gq, gkv = row_of(g1b), row_of(gqb), row_of(gkvb)

    def norm_tile(i, _):
        for h in range(TA // 64):
            rows = pl.ds(pl.multiple_of(i * TA + h * 64, 64), 64)
            scale = inv[rows, :]
            for j in range(D // 128):
                cols = slice(128 * j, 128 * j + 128)
                xa[rows, cols] = (xa[rows, cols].astype(F32) * scale * g1[:, cols]).astype(BF16)
        return 0

    def part(quarter, first, lo, hi):
        cols = pl.ds(pl.multiple_of(quarter * 640, 128), 640)

        def tile(i, _):
            rows = pl.ds(pl.multiple_of(i * 512, 512), 512)
            a = xa[rows, cols]
            pq, pk = dot(a, wdq[cols, :]), dot(a, wdkv[cols, :])
            if first:
                accq[rows, :], acck[rows, :] = pq, pk
            else:
                accq[rows, :] += pq
                acck[rows, :] += pk
            return 0
        lax.fori_loop(lo, hi, tile, 0)

    cos2 = jnp.concatenate([cos_ref[...]] * (TA // S), axis=0)
    sin2 = jnp.concatenate([sin_ref[...]] * (TA // S), axis=0)

    def last_part(quarter, a0, a1):
        cols = pl.ds(pl.multiple_of(quarter * 640, 128), 640)

        def tile(i, _):
            rows = pl.ds(pl.multiple_of(i * TA, TA), TA)
            a = xa[rows, cols]
            qd = accq[rows, :] + dot(a, wdq[cols, :])
            kd = acck[rows, :] + dot(a, wdkv[cols, :])
            cqT[:, rows] = (qd * rms(qd) * gq).astype(BF16).T
            kc = kd[:, :KR]
            c = (kc * rms(kc) * gkv).astype(BF16)
            cbuf[rows, :] = c
            cT[:, rows] = c.T
            lo, hi = kd[:, KR:KR + 16], kd[:, KR + 16:]
            rbuf[rows, :] = jnp.concatenate([lo * cos2 - hi * sin2, hi * cos2 + lo * sin2], axis=-1).astype(BF16)
            for h in range(TA // S):
                rT[i * (TA // S) + h] = rbuf[pl.ds(pl.multiple_of(i * TA + h * S, S), S), :].T
            return 0
        lax.fori_loop(a0, a1, tile, 0)

    def run(name, fn, *args):
        with jax.named_scope(name):
            fn(*args)

    run('norm_a', lax.fori_loop, 0, 4, norm_tile, 0)
    run('c_a', act, 'st1', D0, 'st0', U0)
    run('norm_b', lax.fori_loop, 4, 8, norm_tile, 0)
    for n in D0:
        local(n).wait()
    run('c_b', recv, D0, 'S0')
    run('own_a', part, f // 2, True, 0, 2)
    run('c_c', act, 'st2', D0, 'st4x', D0)
    run('own_b', part, f // 2, True, 2, 4)
    run('c_d', act, 'st0', U1, 'st4y', D0)
    run('c_e', recv, D0, 'S1')
    run('x_a', part, fx // 2, False, 0, 2)
    run('c_f', act, 'st3', D0, 'st1', U0)
    run('x_b', part, fx // 2, False, 2, 4)
    run('c_g', recv, D0, 'S2')
    run('y_a', part, fy // 2, False, 0, 2)
    run('c_h', act, 'st5', D0, 'st2', U0, 'st0', U2)
    run('y_b', part, fy // 2, False, 2, 4)
    run('c_i', act, 'st3', U0, 'st4', U0)
    run('c_j', recv, D0, 'S3')
    run('d_a', last_part, fd // 2, 0, 4)
    run('c_k', act, 'st1', U1, 'stage', O0, 'st0', O0)
    run('d_b', last_part, fd // 2, 4, 8)
    run('c_l', act, 'st5', U0, 'st2', U1)
    outs = [pltpu.make_async_copy(cbuf, c_hbm, csem.at[0]), pltpu.make_async_copy(rT, r_hbm, csem.at[1])]
    for o in outs:
        o.start()
    run('c_m', fin, U0)

    keep = lax.broadcasted_iota(jnp.int32, (S, S), 0) <= lax.broadcasted_iota(jnp.int32, (S, S), 1)
    lane = lax.broadcasted_iota(jnp.int32, (S, 128), 1)
    co, si = cosT_ref[...], sinT_ref[...]
    for h in range(HG):
        zr = 128 * h + (96 if h % 2 == 0 else 32)
        qT[zr:zr + 32, :] = jnp.zeros((32, TC), BF16)

    def load_group(g):
        uc = pl.ds(pl.multiple_of(g * (HG * 96), 128), HG * 96)
        wqT[...] = wuq[:, uc].T
        for j in range(HG // 2):
            t0 = wukv[:, pl.ds(pl.multiple_of(g * (HG * 128) + 256 * j, 128), 128)]
            t1 = wukv[:, pl.ds(pl.multiple_of(g * (HG * 128) + 256 * j + 128, 128), 128)]
            wk[:, 128 * j:128 * j + 128] = jnp.concatenate([t0[:, :64], t1[:, :64]], axis=1)
            wvT[128 * j:128 * j + 128, :] = jnp.concatenate([t0[:, 64:], t1[:, 64:]], axis=1).T

    def out_copy(i):
        g, tc = i // NCH, i % NCH
        return pltpu.make_async_copy(obuf.at[i % 2], attn_hbm.at[pl.ds(pl.multiple_of(tc * TC, TC), TC), pl.ds(pl.multiple_of(g * (HG * 64), 128), HG * 64)], osem.at[i % 2])

    sched = {
        1: ('st3', U1, 'st4', U1, 'st1', U2),
        2: ('st2', U2, 'st0', O1, 'st5', U1),
        3: ('fin', U1, 'st3', U2, 'st4', U2),
        5: ('st1', O0, 'st5', U2, 'st0', O2),
        6: ('fin', U2, 'st2', O0),
        8: ('st3', O0, 'st4', O0, 'st1', O1),
        9: ('st0', O3, 'st2', O1),
        11: ('st5', O0, 'st3', O1, 'st4', O1),
        13: ('st1', O2, 'st2', O2, 'st5', O1),
        15: ('st3', O2, 'st4', O2, 'st1', O3),
        17: ('st2', O3, 'st5', O2),
        18: ('st3', O3, 'st4', O3),
    }

    def step(i, _):
        g, tc = i // NCH, i % NCH
        tok = pl.multiple_of(tc * TC, TC)
        for s, todo in sched.items():
            pl.when(i == s)(functools.partial(run, f'comm_{s}', act, *todo))

        @pl.when(tc == 0)
        def _():
            with jax.named_scope('load_group'):
                load_group(g)

        @pl.when(i >= 2)
        def _():
            out_copy(i - 2).wait()

        slot = i % 2
        for n in range(TC // 256):
            q = dot(wqT[...], cqT[:, pl.ds(tok + 256 * n, 256)])
            cols = slice(256 * n, 256 * n + 256)
            for h in range(HG):
                nope = q[96 * h:96 * h + 64]
                lo, hi = q[96 * h + 64:96 * h + 80], q[96 * h + 80:96 * h + 96]
                b = 128 * h
                qn, qp = (b, b + 64) if h % 2 == 0 else (b + 64, b)
                qT[qn:qn + 64, cols] = nope.astype(BF16)
                qT[qp:qp + 16, cols] = (lo * co - hi * si).astype(BF16)
                qT[qp + 16:qp + 32, cols] = (hi * co + lo * si).astype(BF16)
        kbuf[...] = dot(cbuf[pl.ds(tok, TC), :], wk[...]).astype(BF16)
        vT[...] = dot(wvT[...], cT[:, pl.ds(tok, TC)]).astype(BF16)

        for p in range(TC // S):
            row = p * S
            r = rbuf[pl.ds(tok + row, S), :]
            z32, z64 = jnp.zeros((S, 32), BF16), jnp.zeros((S, 64), BF16)
            r_hi = jnp.concatenate([z64, r, z32], axis=1)
            r_lo = jnp.concatenate([r, z32, z64], axis=1)
            for j in range(HG // 2):
                k2 = kbuf[row:row + S, 128 * j:128 * j + 128]
                both = []
                for par in range(2):
                    h = 2 * j + par
                    k = jnp.where(lane < 64, k2, r_hi) if par == 0 else jnp.where(lane < 64, r_lo, k2)
                    both.append(attn_unit(k, qT[128 * h:128 * h + 128, row:row + S], vT[64 * h:64 * h + 64, row:row + S], keep))
                obuf[slot, row:row + S, 128 * j:128 * j + 128] = jnp.concatenate(both, axis=0).astype(BF16).T
        out_copy(i).start()
        return 0

    lax.fori_loop(0, STEPS, step, 0)
    with jax.named_scope('fin_O'):
        st5(O3)
        for names in (O0, O1, O2, O3):
            fin(names)
    for i in (STEPS - 2, STEPS - 1):
        out_copy(i).wait()
    for o in outs:
        o.wait()
    for p in PIECES:
        for k in KINDS:
            copy(p[0], k).wait_send()


def front(x, gains, ws, cos, sin):
    anyspace, vm = pl.BlockSpec(memory_space=pl.ANY), pl.BlockSpec(memory_space=pltpu.VMEM)
    V = pltpu.VMEM
    dma = pltpu.SemaphoreType.DMA
    tab = [cos, sin, np.tile(cos.T, (1, 2)), np.tile(sin.T, (1, 2))]
    return pl.pallas_call(
        front_kernel, name='front',
        in_specs=[anyspace] + [vm] * 3 + [anyspace] * 5 + [vm] * 4,
        out_specs=[anyspace] * 4,
        out_shape=[jax.ShapeDtypeStruct((T, H * VD), BF16), jax.ShapeDtypeStruct((H * VD, D), BF16), jax.ShapeDtypeStruct((T, KR), BF16), jax.ShapeDtypeStruct((T // S, RD, S), BF16)],
        scratch_shapes=[
            V((T, D), BF16), V((D, QR), BF16), V((D, KR + RD), BF16), V((QR, H * 96), BF16), V((KR, H * 128), BF16), V((320, D), BF16),
            V((8, 1, 320), BF16), V((8, 1, 96), BF16), V((8, 1, 32), BF16), V((T, QR), F32), V((T, KR + RD), F32), V((T, 128), F32),
            V((QR, T), BF16), V((T, KR), BF16), V((KR, T), BF16), V((T, RD), BF16), V((T // S, RD, S), BF16),
            V((HG * 96, QR), BF16), V((KR, HG * 64), BF16), V((HG * 64, KR), BF16), V((HG * 128, TC), BF16), V((TC, HG * 64), BF16), V((HG * 64, TC), BF16), V((2, TC, HG * 64), BF16),
            dma((len(PIECES), len(KINDS))), dma((len(PIECES), len(KINDS))), dma((len(PIECES),)), dma((3, 8)), dma((3, 7)), dma((T // TA,)), dma((3,)), dma((2,)),
        ],
        compiler_params=pltpu.CompilerParams(collective_id=0, has_side_effects=True, vmem_limit_bytes=63 << 20),
    )(x, *gains, *ws, *(jnp.asarray(t) for t in tab))


def out_kernel(o_ref, w_ref, x_ref, c_ref, r_ref, y_ref, c_out, r_out):
    for n in range(0, y_ref.shape[1], 256):
        cols = slice(n, n + 256)
        y_ref[:, cols] = (x_ref[:, cols].astype(F32) + dot(o_ref[...], w_ref[:, cols])).astype(BF16)
    c_out[...] = c_ref[...]
    r_out[...] = r_ref[...]


def outp(o, w, x, c, r, tm=1024, tn=1280):
    nt = D // tn
    cr = T // ((T // tm) * nt)
    step = lambda j, i: j * (T // tm) + i
    return pl.pallas_call(
        out_kernel, grid=(nt, T // tm), name='outp',
        in_specs=[pl.BlockSpec((tm, D), lambda j, i: (i, 0)), pl.BlockSpec((D, tn), lambda j, i: (0, j)), pl.BlockSpec((tm, tn), lambda j, i: (i, j)),
                  pl.BlockSpec((cr, KR), lambda j, i: (step(j, i), 0)), pl.BlockSpec((cr // S, RD, S), lambda j, i: (step(j, i), 0, 0))],
        out_specs=[pl.BlockSpec((tm, tn), lambda j, i: (i, j)), pl.BlockSpec((cr, KR), lambda j, i: (step(j, i), 0)), pl.BlockSpec((cr // S, RD, S), lambda j, i: (step(j, i), 0, 0))],
        out_shape=[jax.ShapeDtypeStruct((T, D), BF16), jax.ShapeDtypeStruct((T, KR), BF16), jax.ShapeDtypeStruct((T // S, RD, S), BF16)],
        compiler_params=pltpu.CompilerParams(vmem_limit_bytes=62 << 20),
    )(o, w, x, c, r)


def tables():
    half = RD // 2
    freq = np.float32(10000.0) ** (np.float32(-2.0) * np.arange(half, dtype=np.float32) / np.float32(RD))
    ang = np.arange(S, dtype=np.float32)[:, None] * freq[None, :].astype(np.float32)
    return np.cos(ang).astype(np.float32), np.sin(ang).astype(np.float32)


def solution(mesh):
    batch, row, mat = P(('dp', 'fsdp')), P('fsdp'), P('fsdp', None)

    def local(tok, g1, wdq, gq, wuq, wkv, gkv, wukv, wo):
        cos, sin = tables()
        x = tok.reshape(T, D)
        o, w, c, r = front(x, (g1[None], gq[None], gkv[None]), (wdq, wkv, wuq, wukv, wo), cos, sin)
        y, c, r = outp(o, w, x, c, r)
        return y.reshape(tok.shape), c.reshape(-1, S, KR), jnp.swapaxes(r, 1, 2)

    return jax.shard_map(local, mesh=mesh, in_specs=(batch, row, mat, row, mat, mat, row, mat, mat),
                         out_specs=(batch,) * 3, check_vma=False)
```

```python
import functools
import numpy as np
import jax
import jax.numpy as jnp
from jax import lax
from jax.experimental import pallas as pl
from jax.experimental.pallas import tpu as pltpu
from jax.sharding import PartitionSpec as P

F32, BF16 = jnp.float32, jnp.bfloat16
MESH = pl.DeviceIdType.MESH
EPS = 1e-6
T, D, QR, KR, RD, H, ND, VD = 2048, 2560, 768, 256, 32, 40, 64, 64
S = 128
SC = (ND + RD) ** -0.5 * 1.4426950408889634
HG, TC = 8, 512
NCH = T // TC
STEPS = (H // HG) * NCH
TA = 256


def dot(a, b):
    return jnp.dot(a, b, preferred_element_type=F32)


def rms(v):
    return lax.rsqrt(jnp.mean(v * v, axis=-1, keepdims=True) + EPS)


def attn_unit(k, qT, vT, keep):
    s = dot(k, qT) * SC
    s = jnp.where(keep, s, -1e30)
    m = jnp.max(s, axis=0, keepdims=True)
    e = jnp.exp2(s - m)
    p = (e * (1.0 / jnp.sum(e, axis=0, keepdims=True))).astype(BF16)
    return dot(vT, p)


PIECES = (
    ('dq', 'dq', False, 320, 0, 768, 96),
    ('dkv', 'dkv', False, 320, 0, 288, 96),
    ('uq0', 'uq', False, 96, 0, 768, 32),
    ('ukv0', 'ukv', True, 32, 0, 1024, 384),
    ('uq1', 'uq', False, 96, 768, 1536, 32),
    ('ukv1', 'ukv', True, 32, 1024, 2048, 640),
    ('uq2', 'uq', False, 96, 2304, 1536, 32),
    ('ukv2', 'ukv', True, 32, 3072, 2048, 640),
    ('o0', 'o', False, 320, 0, 640, 112),
    ('o1', 'o', False, 320, 640, 640, 112),
    ('o2', 'o', False, 320, 1280, 640, 112),
    ('o3', 'o', False, 320, 1920, 640, 112),
)
PIDX = {p[0]: i for i, p in enumerate(PIECES)}
SPLIT = ('S1a', 'S1b', 'S2a', 'S2b', 'S3a', 'S3b')
KINDS = ('XE', 'YE', 'XS', 'YS', 'S0', 'Z1', 'Z2', 'DY', 'DX', 'Z3', 'S1', 'S2', 'S3') + SPLIT
KIDX = {k: i for i, k in enumerate(KINDS)}
GROUPS = {'dq': ('dq',), 'dkv': ('dkv',), 'U0': ('uq0', 'ukv0'), 'U1': ('uq1', 'ukv1'), 'U2': ('uq2', 'ukv2'),
          'O0': ('o0',), 'O1': ('o1',), 'O2': ('o2',), 'O3': ('o3',)}
STAGES = {
    'st0': ((), ('XE', 'YE', 'XS', 'YS', 'S0')),
    'st1': (('XE', 'YE'), ('Z1', 'Z2', 'DY')),
    'st2': (('XS', 'YS'), ('DX',)),
    'st4x': (('Z1',), ('S1',)),
    'st3': (('DY',), ('Z3',)),
    'st4y': (('Z2',), ('S2',)),
    'st5': (('DX', 'Z3'), ('S3',)),
    'fin': (('S0', 'S1', 'S2', 'S3'), ()),
    'st2d': (('XS', 'YS'), ('DX', 'S1a', 'S2a')),
    'st4xd': (('Z1',), ('S1b',)),
    'st4yd': (('Z2',), ('S2b',)),
    'st5a': (('DX',), ('S3a',)),
    'st5b': (('Z3',), ('S3b',)),
    'find': ((), ()),
}
SCHED = {
    'stats0': (('st0', 'dq'),),
    'norm0': (('st0', 'dkv'),),
    'part0': (('st1', 'dq'), ('recv', 'dq', 'S0'), ('recv', 'dkv', 'S0')),
    'part3': (('st0', 'U0'),),
    'part4': (('st2d', 'dq'), ('st4xd', 'dq'), ('recv', 'dq', 'S1a+S1b'), ('st1', 'dkv'), ('st2d', 'dkv'), ('st4xd', 'dkv'), ('st3', 'dq'), ('st4yd', 'dq'), ('st0', 'U1'), ('recv', 'dkv', 'S1a+S1b')),
    'part5': (('st1', 'U0'),),
    'part6': (('st2', 'U0'),),
    'part7': (('st5a', 'dq'), ('st3', 'dkv'), ('st4yd', 'dkv')),
    'part8': (('st5b', 'dq'), ('find', 'dq'), ('st5a', 'dkv'), ('st0', 'U2'), ('recv', 'dq', 'S2a+S2b'), ('recv', 'dkv', 'S2a+S2b'), ('st4x', 'U0')),
    'part10': (('st1', 'U1'),),
    'part11': (('st5b', 'dkv'), ('find', 'dkv')),
    'd0': (('recv', 'dq', 'S3a+S3b'), ('recv', 'dkv', 'S3a+S3b')),
    'd1': (('st3', 'U0'), ('st4y', 'U0'), ('st2', 'U1')),
    'd2': (('st4x', 'U1'), ('st0', 'O0')),
    'd3': (('st1', 'U2'),),
    's0': (('st5', 'U0'), ('st2', 'U2'), ('fin', 'U0'), ('st3', 'U1'), ('st4y', 'U1')),
    's1': (('st4x', 'U2'), ('st0', 'O1')),
    's2': (('st1', 'O0'),),
    's3': (('st5', 'U1'), ('st2', 'O0')),
    's4': (('fin', 'U1'), ('st3', 'U2'), ('st4y', 'U2'), ('st0', 'O2')),
    's5': (('st4x', 'O0'), ('st1', 'O1')),
    's6': (('st2', 'O1'),),
    's7': (('st5', 'U2'), ('st3', 'O0'), ('st4y', 'O0')),
    's8': (('fin', 'U2'), ('st4x', 'O1'), ('st0', 'O3')),
    's9': (('st1', 'O2'), ('st2', 'O2')),
    's10': (('st5', 'O0'), ('st3', 'O1'), ('st4y', 'O1')),
    's11': (('fin', 'O0'),),
    's12': (('st4x', 'O2'), ('st1', 'O3')),
    's13': (('st3', 'O2'), ('st4y', 'O2'), ('st2', 'O3')),
    's14': (('st5', 'O1'),),
    's15': (('fin', 'O1'), ('st4x', 'O3'), ('st3', 'O3')),
    's16': (('st4y', 'O3'),),
    's17': (('st5', 'O2'),),
    's18': (('fin', 'O2'),),
    's19': (('st5', 'O3'),),
    'end': (('fin', 'O3'),),
    'stats1': (),
}


def front_kernel(x_hbm, g1_s, gq_s, gkv_s, dq_s, dkv_s, uq_s, ukv_s, o_s, cos_ref, sin_ref, cosT_ref, sinT_ref,
                 attn_hbm, wo_hbm, c_hbm, r_hbm,
                 xa, wdq, wdkv, wuq, wukv, ostage, g1b, gqb, gkvb, accq, acck, inv, cqT, cbuf, cT, rbuf, rT,
                 wqT, wk, wvT, qT, kbuf, vT, obuf,
                 ssem, rsem, lsem, gss, grs, xsem, osem, csem):
    z, f = lax.axis_index('dp'), lax.axis_index('fsdp')
    core, xx, yy = f % 2, (f // 2) % 2, f // 4

    def idx(dx, dy, dc):
        return ((yy + dy) % 2) * 4 + ((xx + dx) % 2) * 2 + (core + dc) % 2

    fx, fy, fd = idx(1, 0, 0), idx(0, 1, 0), idx(1, 1, 0)
    dev = {'X': (z, fx), 'Y': (z, fy), 'Z': (1 - z, f), 'S': (z, idx(0, 0, 1))}
    plane = [idx(dx, dy, dc) for dx in range(2) for dy in range(2) for dc in range(2) if dx + dy + dc]
    src = {'dq': dq_s, 'dkv': dkv_s, 'uq': uq_s, 'ukv': ukv_s, 'o': ostage}
    buf = {'dq': wdq, 'dkv': wdkv, 'uq': wuq, 'ukv': wukv, 'o': wo_hbm}

    def region(piece, shard, part, base):
        name, arr, bycol, rows, c0, nc, e = piece
        n = nc if bycol else rows
        off, size = {'E': (z * (n - e), e), 'S': (e, n - 2 * e), 'A': (0, n), 'B': (z * e, n - e), 'M': ((1 - z) * (n - e), e)}[part]
        if bycol:
            row = shard * rows if base else 0
            return pl.ds(pl.multiple_of(row, 16), rows), pl.ds(pl.multiple_of(c0 + off, 128), size)
        row = (shard * rows if base else 0) + off
        return pl.ds(pl.multiple_of(row, 16), size), pl.ds(c0, nc)

    def copy(name, kind):
        piece = PIECES[PIDX[name]]
        arr = piece[1]
        shard = {'X': f, 'Y': f}.get(kind[0]) if kind in ('XE', 'YE', 'XS', 'YS') else None
        if kind in ('XE', 'YE', 'XS', 'YS', 'S0'):
            part = 'A' if kind == 'S0' else kind[1]
            r0, c0 = region(piece, f, part, False)
            r1, c1 = region(piece, f, part, True)
            s_ref, d_ref = src[arr].at[r0, c0], buf[arr].at[r1, c1]
            to = dev[kind[0]]
        else:
            shard, part, to = {'Z1': (fx, 'E', 'Z'), 'Z2': (fy, 'E', 'Z'), 'Z3': (fd, 'E', 'Z'), 'DY': (fx, 'E', 'Y'),
                               'DX': (fy, 'S', 'X'), 'S1': (fx, 'A', 'S'), 'S2': (fy, 'A', 'S'), 'S3': (fd, 'A', 'S'),
                               'S1a': (fx, 'B', 'S'), 'S1b': (fx, 'M', 'S'), 'S2a': (fy, 'B', 'S'), 'S2b': (fy, 'M', 'S'),
                               'S3a': (fd, 'B', 'S'), 'S3b': (fd, 'M', 'S')}[kind]
            to = dev[to]
            r1, c1 = region(piece, shard, part, True)
            s_ref = d_ref = buf[arr].at[r1, c1]
        i, j = PIDX[name], KIDX[kind]
        return pltpu.make_async_remote_copy(src_ref=s_ref, dst_ref=d_ref, send_sem=ssem.at[i, j], recv_sem=rsem.at[i, j],
                                            device_id=to, device_id_type=MESH)

    def local(name):
        piece = PIECES[PIDX[name]]
        r0, c0 = region(piece, f, 'A', False)
        r1, c1 = region(piece, f, 'A', True)
        return pltpu.make_async_copy(src[piece[1]].at[r0, c0], buf[piece[1]].at[r1, c1], lsem.at[PIDX[name]])

    def start(names, *kinds):
        for k in kinds:
            for n in names:
                copy(n, k).start()

    def recv(names, *kinds):
        for k in kinds:
            for n in names:
                copy(n, k).wait_recv()

    def comm(todo):
        for op in todo:
            stage, piece = op[0], op[1]
            names = GROUPS[piece]
            if stage == 'recv':
                recv(names, *op[2].split('+'))
                continue
            if stage == 'st0' and piece == 'O0':
                stage_o.wait()
            waits, starts = STAGES[stage]
            recv(names, *waits)
            start(names, *starts)
            if stage == 'st0':
                for n in names:
                    local(n).start()
            if stage in ('fin', 'find'):
                for n in names:
                    if piece not in ('dq', 'dkv'):
                        local(n).wait()

    def at(seg, i):
        for name, todo in SCHED.items():
            if name.startswith(seg) and name[len(seg):].isdigit() and todo:
                @pl.when(i == int(name[len(seg):]))
                def _(todo=todo, name=name):
                    with jax.named_scope('comm_' + name):
                        comm(todo)

    for i in range(T // TA):
        pltpu.make_async_copy(x_hbm.at[pl.ds(i * TA, TA)], xa.at[pl.ds(i * TA, TA)], xsem.at[i]).start()
    stage_o = pltpu.make_async_copy(o_s, ostage, osem.at[2])
    stage_o.start()

    barrier = pltpu.get_barrier_semaphore()
    with jax.named_scope('barrier'):
        for p in plane:
            pl.semaphore_signal(barrier, inc=1, device_id=(z, p), device_id_type=MESH)
        pl.semaphore_signal(barrier, inc=1, device_id=dev['Z'], device_id_type=MESH)
        pl.semaphore_wait(barrier, 8)

    gains = []
    for j, (gs, gb) in enumerate(((g1_s, g1b), (gq_s, gqb), (gkv_s, gkvb))):
        for i, p in enumerate(plane):
            gains.append(pltpu.make_async_remote_copy(src_ref=gs, dst_ref=gb.at[f], send_sem=gss.at[j, i], recv_sem=grs.at[j, i],
                                                      device_id=(z, p), device_id_type=MESH))
            gains[-1].start()
        own = pltpu.make_async_copy(gs, gb.at[f], gss.at[j, 7])
        own.start()
        gains.append(own)
    comm(SCHED['stats0'])

    def stat_tile(i, _):
        @pl.when(i == 4)
        def _():
            comm(SCHED['stats1'])
        pltpu.make_async_copy(x_hbm.at[pl.ds(i * TA, TA)], xa.at[pl.ds(i * TA, TA)], xsem.at[i]).wait()
        zero = jnp.zeros((TA, 128), F32)
        for j in range(QR // 128):
            accq[pl.ds(pl.multiple_of(i * TA, TA), TA), 128 * j:128 * j + 128] = zero
        acck[pl.ds(pl.multiple_of(i * TA, TA), TA), :] = jnp.zeros((TA, KR + RD), F32)
        for h in range(TA // 64):
            rows = pl.ds(pl.multiple_of(i * TA + h * 64, 64), 64)
            inv[rows, :] = jnp.broadcast_to(rms(xa[rows, :].astype(F32)), (64, 128))
        return 0

    with jax.named_scope('stats'):
        lax.fori_loop(0, T // TA, stat_tile, 0)
    with jax.named_scope('gains'):
        for g in gains:
            g.wait()

    def row_of(gb):
        return jnp.concatenate([gb[i].astype(F32) for i in range(8)], axis=-1)

    g1, gq, gkv = row_of(g1b), row_of(gqb), row_of(gkvb)

    def norm_tile(i, _):
        pl.when(i % 2 == 0)(functools.partial(at, 'norm', i // 2))
        for h in range(TA // 64):
            rows = pl.ds(pl.multiple_of(i * TA + h * 64, 64), 64)
            scale = inv[rows, :]
            for j in range(D // 128):
                cols = slice(128 * j, 128 * j + 128)
                xa[rows, cols] = (xa[rows, cols].astype(F32) * scale * g1[:, cols]).astype(BF16)
        return 0

    def part(i, _):
        at('part', i)
        which, t = i // 4, i % 4
        quarter = ((yy + which // 2) % 2) * 2 + (xx + which % 2) % 2
        cols = pl.ds(pl.multiple_of(quarter * 640, 128), 640)
        rows = pl.ds(pl.multiple_of(t * 512, 512), 512)
        a = xa[rows, cols]
        accq[rows, :] += dot(a, wdq[cols, :])
        acck[rows, :] += dot(a, wdkv[cols, :])
        return 0

    cos2 = jnp.concatenate([cos_ref[...]] * (TA // S), axis=0)
    sin2 = jnp.concatenate([sin_ref[...]] * (TA // S), axis=0)

    def last_part():
        cols = pl.ds(pl.multiple_of((fd // 2) * 640, 128), 640)

        def tile(i, _):
            pl.when(i % 2 == 0)(functools.partial(at, 'd', i // 2))
            rows = pl.ds(pl.multiple_of(i * TA, TA), TA)
            a = xa[rows, cols]
            qd = accq[rows, :] + dot(a, wdq[cols, :])
            kd = acck[rows, :] + dot(a, wdkv[cols, :])
            cqT[:, rows] = (qd * rms(qd) * gq).astype(BF16).T
            kc = kd[:, :KR]
            c = (kc * rms(kc) * gkv).astype(BF16)
            cbuf[rows, :] = c
            cT[:, rows] = c.T
            lo, hi = kd[:, KR:KR + 16], kd[:, KR + 16:]
            rbuf[rows, :] = jnp.concatenate([lo * cos2 - hi * sin2, hi * cos2 + lo * sin2], axis=-1).astype(BF16)
            for h in range(TA // S):
                rT[i * (TA // S) + h] = rbuf[pl.ds(pl.multiple_of(i * TA + h * S, S), S), :].T
            return 0
        lax.fori_loop(0, T // TA, tile, 0)

    with jax.named_scope('norm'):
        lax.fori_loop(0, T // TA, norm_tile, 0)
    for n in ('dq', 'dkv'):
        local(n).wait()
    with jax.named_scope('parts'):
        lax.fori_loop(0, 12, part, 0)
    with jax.named_scope('last'):
        last_part()
    outs = [pltpu.make_async_copy(cbuf, c_hbm, csem.at[0]), pltpu.make_async_copy(rT, r_hbm, csem.at[1])]
    for o in outs:
        o.start()

    keep = lax.broadcasted_iota(jnp.int32, (S, S), 0) <= lax.broadcasted_iota(jnp.int32, (S, S), 1)
    lane = lax.broadcasted_iota(jnp.int32, (S, 128), 1)
    co, si = cosT_ref[...], sinT_ref[...]
    for h in range(HG):
        zr = 128 * h + (96 if h % 2 == 0 else 32)
        qT[zr:zr + 32, :] = jnp.zeros((32, TC), BF16)

    def load_group(g):
        uc = pl.ds(pl.multiple_of(g * (HG * 96), 128), HG * 96)
        wqT[...] = wuq[:, uc].T
        for j in range(HG // 2):
            t0 = wukv[:, pl.ds(pl.multiple_of(g * (HG * 128) + 256 * j, 128), 128)]
            t1 = wukv[:, pl.ds(pl.multiple_of(g * (HG * 128) + 256 * j + 128, 128), 128)]
            wk[:, 128 * j:128 * j + 128] = jnp.concatenate([t0[:, :64], t1[:, :64]], axis=1)
            wvT[128 * j:128 * j + 128, :] = jnp.concatenate([t0[:, 64:], t1[:, 64:]], axis=1).T

    def out_copy(i):
        g, tc = i // NCH, i % NCH
        return pltpu.make_async_copy(obuf.at[i % 2], attn_hbm.at[pl.ds(pl.multiple_of(tc * TC, TC), TC), pl.ds(pl.multiple_of(g * (HG * 64), 128), HG * 64)], osem.at[i % 2])

    def step(i, _):
        g, tc = i // NCH, i % NCH
        tok = pl.multiple_of(tc * TC, TC)
        at('s', i)

        @pl.when(tc == 0)
        def _():
            with jax.named_scope('load_group'):
                load_group(g)

        @pl.when(i >= 2)
        def _():
            out_copy(i - 2).wait()

        slot = i % 2
        for n in range(TC // 256):
            q = dot(wqT[...], cqT[:, pl.ds(tok + 256 * n, 256)])
            cols = slice(256 * n, 256 * n + 256)
            for h in range(HG):
                nope = q[96 * h:96 * h + 64]
                lo, hi = q[96 * h + 64:96 * h + 80], q[96 * h + 80:96 * h + 96]
                b = 128 * h
                qn, qp = (b, b + 64) if h % 2 == 0 else (b + 64, b)
                qT[qn:qn + 64, cols] = nope.astype(BF16)
                qT[qp:qp + 16, cols] = (lo * co - hi * si).astype(BF16)
                qT[qp + 16:qp + 32, cols] = (hi * co + lo * si).astype(BF16)
        kbuf[...] = dot(cbuf[pl.ds(tok, TC), :], wk[...]).astype(BF16)
        vT[...] = dot(wvT[...], cT[:, pl.ds(tok, TC)]).astype(BF16)

        for p in range(TC // S):
            row = p * S
            r = rbuf[pl.ds(tok + row, S), :]
            z32, z64 = jnp.zeros((S, 32), BF16), jnp.zeros((S, 64), BF16)
            r_hi = jnp.concatenate([z64, r, z32], axis=1)
            r_lo = jnp.concatenate([r, z32, z64], axis=1)
            for j in range(HG // 2):
                k2 = kbuf[row:row + S, 128 * j:128 * j + 128]
                both = []
                for par in range(2):
                    h = 2 * j + par
                    k = jnp.where(lane < 64, k2, r_hi) if par == 0 else jnp.where(lane < 64, r_lo, k2)
                    both.append(attn_unit(k, qT[128 * h:128 * h + 128, row:row + S], vT[64 * h:64 * h + 64, row:row + S], keep))
                obuf[slot, row:row + S, 128 * j:128 * j + 128] = jnp.concatenate(both, axis=0).astype(BF16).T
        out_copy(i).start()
        return 0

    lax.fori_loop(0, STEPS, step, 0)
    with jax.named_scope('fin_O'):
        comm(SCHED['end'])
    for i in (STEPS - 2, STEPS - 1):
        out_copy(i).wait()
    for o in outs:
        o.wait()
    for p in PIECES:
        for k in KINDS:
            if k in (('S1', 'S2', 'S3') if p[1] in ('dq', 'dkv') else SPLIT):
                continue
            copy(p[0], k).wait_send()


def front(x, gains, ws, cos, sin):
    anyspace, vm = pl.BlockSpec(memory_space=pl.ANY), pl.BlockSpec(memory_space=pltpu.VMEM)
    V = pltpu.VMEM
    dma = pltpu.SemaphoreType.DMA
    tab = [cos, sin, np.tile(cos.T, (1, 2)), np.tile(sin.T, (1, 2))]
    return pl.pallas_call(
        front_kernel, name='front',
        in_specs=[anyspace] + [vm] * 3 + [anyspace] * 5 + [vm] * 4,
        out_specs=[anyspace] * 4,
        out_shape=[jax.ShapeDtypeStruct((T, H * VD), BF16), jax.ShapeDtypeStruct((H * VD, D), BF16), jax.ShapeDtypeStruct((T, KR), BF16), jax.ShapeDtypeStruct((T // S, RD, S), BF16)],
        scratch_shapes=[
            V((T, D), BF16), V((D, QR), BF16), V((D, KR + RD), BF16), V((QR, H * 96), BF16), V((KR, H * 128), BF16), V((320, D), BF16),
            V((8, 1, 320), BF16), V((8, 1, 96), BF16), V((8, 1, 32), BF16), V((T, QR), F32), V((T, KR + RD), F32), V((T, 128), F32),
            V((QR, T), BF16), V((T, KR), BF16), V((KR, T), BF16), V((T, RD), BF16), V((T // S, RD, S), BF16),
            V((HG * 96, QR), BF16), V((KR, HG * 64), BF16), V((HG * 64, KR), BF16), V((HG * 128, TC), BF16), V((TC, HG * 64), BF16), V((HG * 64, TC), BF16), V((2, TC, HG * 64), BF16),
            dma((len(PIECES), len(KINDS))), dma((len(PIECES), len(KINDS))), dma((len(PIECES),)), dma((3, 8)), dma((3, 7)), dma((T // TA,)), dma((3,)), dma((2,)),
        ],
        compiler_params=pltpu.CompilerParams(collective_id=0, has_side_effects=True, vmem_limit_bytes=63 << 20),
    )(x, *gains, *ws, *(jnp.asarray(t) for t in tab))


def out_kernel(o_ref, w_ref, x_ref, c_ref, r_ref, y_ref, c_out, r_out):
    for n in range(0, y_ref.shape[1], 256):
        cols = slice(n, n + 256)
        y_ref[:, cols] = (x_ref[:, cols].astype(F32) + dot(o_ref[...], w_ref[:, cols])).astype(BF16)
    c_out[...] = c_ref[...]
    r_out[...] = r_ref[...]


def outp(o, w, x, c, r, tm=1024, tn=1280):
    nt = D // tn
    cr = T // ((T // tm) * nt)
    step = lambda j, i: j * (T // tm) + i
    return pl.pallas_call(
        out_kernel, grid=(nt, T // tm), name='outp',
        in_specs=[pl.BlockSpec((tm, D), lambda j, i: (i, 0)), pl.BlockSpec((D, tn), lambda j, i: (0, j)), pl.BlockSpec((tm, tn), lambda j, i: (i, j)),
                  pl.BlockSpec((cr, KR), lambda j, i: (step(j, i), 0)), pl.BlockSpec((cr // S, RD, S), lambda j, i: (step(j, i), 0, 0))],
        out_specs=[pl.BlockSpec((tm, tn), lambda j, i: (i, j)), pl.BlockSpec((cr, KR), lambda j, i: (step(j, i), 0)), pl.BlockSpec((cr // S, RD, S), lambda j, i: (step(j, i), 0, 0))],
        out_shape=[jax.ShapeDtypeStruct((T, D), BF16), jax.ShapeDtypeStruct((T, KR), BF16), jax.ShapeDtypeStruct((T // S, RD, S), BF16)],
        compiler_params=pltpu.CompilerParams(vmem_limit_bytes=62 << 20),
    )(o, w, x, c, r)


def tables():
    half = RD // 2
    freq = np.float32(10000.0) ** (np.float32(-2.0) * np.arange(half, dtype=np.float32) / np.float32(RD))
    ang = np.arange(S, dtype=np.float32)[:, None] * freq[None, :].astype(np.float32)
    return np.cos(ang).astype(np.float32), np.sin(ang).astype(np.float32)


def solution(mesh):
    batch, row, mat = P(('dp', 'fsdp')), P('fsdp'), P('fsdp', None)

    def local(tok, g1, wdq, gq, wuq, wkv, gkv, wukv, wo):
        cos, sin = tables()
        x = tok.reshape(T, D)
        o, w, c, r = front(x, (g1[None], gq[None], gkv[None]), (wdq, wkv, wuq, wukv, wo), cos, sin)
        y, c, r = outp(o, w, x, c, r)
        return y.reshape(tok.shape), c.reshape(-1, S, KR), jnp.swapaxes(r, 1, 2)

    return jax.shard_map(local, mesh=mesh, in_specs=(batch, row, mat, row, mat, mat, row, mat, mat),
                         out_specs=(batch,) * 3, check_vma=False)
```

```python
import functools
import numpy as np
import jax
import jax.numpy as jnp
from jax import lax
from jax.experimental import pallas as pl
from jax.experimental.pallas import tpu as pltpu
from jax.sharding import PartitionSpec as P

F32, BF16 = jnp.float32, jnp.bfloat16
MESH = pl.DeviceIdType.MESH
EPS = 1e-6
T, D, QR, KR, RD, H, ND, VD = 2048, 2560, 768, 256, 32, 40, 64, 64
S = 128
SC = (ND + RD) ** -0.5 * 1.4426950408889634
HG, TC = 8, 512
NCH = T // TC
STEPS = (H // HG) * NCH
TA = 256


def dot(a, b):
    return jnp.dot(a, b, preferred_element_type=F32)


def rms(v):
    return lax.rsqrt(jnp.mean(v * v, axis=-1, keepdims=True) + EPS)


def attn_unit(k, qT, vT, keep):
    s = dot(k, qT) * SC
    s = jnp.where(keep, s, -1e30)
    m = jnp.max(s, axis=0, keepdims=True)
    e = jnp.exp2(s - m)
    p = (e * (1.0 / jnp.sum(e, axis=0, keepdims=True))).astype(BF16)
    return dot(vT, p)


PIECES = (
    ('dq', 'dq', False, 320, 0, 768, 112),
    ('dkv', 'dkv', False, 320, 0, 288, 112),
    ('uq0', 'uq', False, 96, 0, 768, 32),
    ('ukv0', 'ukv', True, 32, 0, 1024, 384),
    ('uq1', 'uq', False, 96, 768, 1536, 32),
    ('ukv1', 'ukv', True, 32, 1024, 2048, 640),
    ('uq2', 'uq', False, 96, 2304, 1536, 32),
    ('ukv2', 'ukv', True, 32, 3072, 2048, 640),
    ('o0', 'o', False, 320, 0, 640, 112),
    ('o1', 'o', False, 320, 640, 640, 112),
    ('o2', 'o', False, 320, 1280, 640, 112),
    ('o3', 'o', False, 320, 1920, 640, 112),
)
PIDX = {p[0]: i for i, p in enumerate(PIECES)}
SPLIT = ('S1a', 'S1b', 'S2a', 'S2b', 'S3a', 'S3b')
KINDS = ('XE', 'YE', 'XS', 'YS', 'S0', 'Z1', 'Z2', 'DY', 'DX', 'Z3', 'S1', 'S2', 'S3') + SPLIT
RSEM = {'XE': 0, 'YE': 0, 'XS': 1, 'YS': 1, 'Z1': 2, 'Z2': 3, 'DY': 4, 'DX': 5, 'Z3': 5, 'S0': 6, 'S1': 6, 'S2': 6, 'S3': 6}
RSEM_SPLIT = dict(RSEM, Z3=7, S1a=8, S1b=8, S2a=9, S2b=9, S3a=10, S3b=10)
SPLIT_ARRS = ('dq', 'dkv')
GROUPS = {'dq': ('dq',), 'dkv': ('dkv',), 'U0': ('uq0', 'ukv0'), 'U1': ('uq1', 'ukv1'), 'U2': ('uq2', 'ukv2'),
          'O0': ('o0',), 'O1': ('o1',), 'O2': ('o2',), 'O3': ('o3',)}
STAGES = {
    'st0': ((), ('XE', 'YE', 'XS', 'YS', 'S0')),
    'st1': (('XYE',), ('Z1', 'Z2', 'DY')),
    'st2': (('XYS',), ('DX',)),
    'st4x': (('Z1',), ('S1',)),
    'st3': (('DY',), ('Z3',)),
    'st4y': (('Z2',), ('S2',)),
    'st5': (('DXZ',), ('S3',)),
    'fin': (('SS',), ()),
    'st2d': (('XYS',), ('DX', 'S1a', 'S2a')),
    'st4xd': (('Z1',), ('S1b',)),
    'st4yd': (('Z2',), ('S2b',)),
    'st5a': (('DX',), ('S3a',)),
    'st5b': (('Z3',), ('S3b',)),
    'find': ((), ()),
}
SCHED = {
    'stats0': (('st0', 'dq'),),
    'norm1': (('st0', 'dkv'),),
    'part0': (('recv', 'dq', 'S0'), ('recv', 'dkv', 'S0')),
    'part1': (('st1', 'dq'),),
    'part3': (('st2d', 'dq'),),
    'part4': (('st4xd', 'dq'), ('st1', 'dkv'), ('recv', 'dq', 'S1a+S1b'), ('st2d', 'dkv'), ('st0', 'U0'), ('st4xd', 'dkv'), ('st3', 'dq'), ('st4yd', 'dq'), ('st5a', 'dq'), ('st0', 'U1'), ('recv', 'dkv', 'S1a+S1b'), ('st3', 'dkv')),
    'part5': (('st4yd', 'dkv'), ('st5a', 'dkv'), ('st1', 'U0')),
    'part6': (('st2', 'U0'),),
    'part8': (('st0', 'U2'), ('recv', 'dq', 'S2a+S2b'), ('recv', 'dkv', 'S2a+S2b')),
    'part9': (('st5b', 'dq'), ('st1', 'U1')),
    'part10': (('st5b', 'dkv'),),
    'd0': (('st4x', 'U0'), ('st2', 'U1'), ('recv', 'dq', 'S3a+S3b'), ('recv', 'dkv', 'S3a+S3b')),
    'd1': (('st3', 'U0'), ('st4y', 'U0')),
    'd2': (('st4x', 'U1'), ('st1', 'U2')),
    's0': (('st2', 'U2'), ('st0', 'O0'), ('st5', 'U0'), ('fin', 'U0'), ('st3', 'U1'), ('st4y', 'U1')),
    's1': (('st4x', 'U2'), ('st3', 'U2'), ('st0', 'O1')),
    's2': (('st4y', 'U2'),),
    's3': (('st5', 'U1'), ('st1', 'O0')),
    's4': (('st5', 'U2'), ('st2', 'O0'), ('fin', 'U1')),
    's5': (('fin', 'U2'), ('st4x', 'O0'), ('st1', 'O1')),
    's6': (('st2', 'O1'), ('st0', 'O2')),
    's7': (('st3', 'O0'), ('st4y', 'O0')),
    's8': (('st4x', 'O1'),),
    's9': (('st3', 'O1'), ('st4y', 'O1'), ('st0', 'O3')),
    's10': (('st1', 'O2'),),
    's11': (('st5', 'O0'), ('st2', 'O2')),
    's12': (('st5', 'O1'), ('st1', 'O3')),
    's13': (('fin', 'O0'), ('fin', 'O1'), ('st4x', 'O2'), ('st2', 'O3')),
    's14': (('st3', 'O2'), ('st4y', 'O2')),
    's16': (('st4x', 'O3'), ('st3', 'O3')),
    's17': (('st4y', 'O3'),),
    's18': (('st5', 'O2'),),
    's19': (('st5', 'O3'),),
    'end': (('fin', 'O2'), ('fin', 'O3')),
    'stats1': (),
}


def front_kernel(x_hbm, g1_s, gq_s, gkv_s, dq_s, dkv_s, uq_s, ukv_s, o_s, cos_ref, sin_ref, cosT_ref, sinT_ref,
                 attn_hbm, wo_hbm, c_hbm, r_hbm,
                 xa, wdq, wdkv, wuq, wukv, ostage, g1b, gqb, gkvb, accq, acck, inv, cqT, cbuf, cT, rbuf, rT,
                 wqT, wk, wvT, qT, kbuf, vT, obuf,
                 ssem, rsem, dsem, lsem, gss, grs, xsem, osem, csem):
    z, f = lax.axis_index('dp'), lax.axis_index('fsdp')
    core, xx, yy = f % 2, (f // 2) % 2, f // 4

    def idx(dx, dy, dc):
        return ((yy + dy) % 2) * 4 + ((xx + dx) % 2) * 2 + (core + dc) % 2

    fx, fy, fd = idx(1, 0, 0), idx(0, 1, 0), idx(1, 1, 0)
    dev = {'X': (z, fx), 'Y': (z, fy), 'Z': (1 - z, f), 'S': (z, idx(0, 0, 1))}
    plane = [idx(dx, dy, dc) for dx in range(2) for dy in range(2) for dc in range(2) if dx + dy + dc]
    src = {'dq': dq_s, 'dkv': dkv_s, 'uq': uq_s, 'ukv': ukv_s, 'o': ostage}
    buf = {'dq': wdq, 'dkv': wdkv, 'uq': wuq, 'ukv': wukv, 'o': wo_hbm}

    def region(piece, shard, part, base):
        name, arr, bycol, rows, c0, nc, e = piece
        n = nc if bycol else rows
        off, size = {'E': (z * (n - e), e), 'S': (e, n - 2 * e), 'A': (0, n), 'B': (z * e, n - e), 'M': ((1 - z) * (n - e), e)}[part]
        if bycol:
            row = shard * rows if base else 0
            return pl.ds(pl.multiple_of(row, 16), rows), pl.ds(pl.multiple_of(c0 + off, 128), size)
        row = (shard * rows if base else 0) + off
        return pl.ds(pl.multiple_of(row, 16), size), pl.ds(c0, nc)

    def copy(name, kind):
        piece = PIECES[PIDX[name]]
        arr = piece[1]
        shard = {'X': f, 'Y': f}.get(kind[0]) if kind in ('XE', 'YE', 'XS', 'YS') else None
        if kind in ('XE', 'YE', 'XS', 'YS', 'S0'):
            part = 'A' if kind == 'S0' else kind[1]
            r0, c0 = region(piece, f, part, False)
            r1, c1 = region(piece, f, part, True)
            s_ref, d_ref = src[arr].at[r0, c0], buf[arr].at[r1, c1]
            to = dev[kind[0]]
        else:
            shard, part, to = {'Z1': (fx, 'E', 'Z'), 'Z2': (fy, 'E', 'Z'), 'Z3': (fd, 'E', 'Z'), 'DY': (fx, 'E', 'Y'),
                               'DX': (fy, 'S', 'X'), 'S1': (fx, 'A', 'S'), 'S2': (fy, 'A', 'S'), 'S3': (fd, 'A', 'S'),
                               'S1a': (fx, 'B', 'S'), 'S1b': (fx, 'M', 'S'), 'S2a': (fy, 'B', 'S'), 'S2b': (fy, 'M', 'S'),
                               'S3a': (fd, 'B', 'S'), 'S3b': (fd, 'M', 'S')}[kind]
            to = dev[to]
            r1, c1 = region(piece, shard, part, True)
            s_ref = d_ref = buf[arr].at[r1, c1]
        return pltpu.make_async_remote_copy(src_ref=s_ref, dst_ref=d_ref, send_sem=ssem.at[PIDX[name]], recv_sem=rsem_of(name, kind),
                                            device_id=to, device_id_type=MESH)

    def rsem_of(name, kind):
        if PIECES[PIDX[name]][1] in SPLIT_ARRS:
            return dsem.at[PIDX[name], RSEM_SPLIT[kind]]
        return rsem.at[PIDX[name] - 2, RSEM[kind]]

    def take(name, n, sem, rows_too=True):
        _, arr, bycol, rows, c0, nc, e = PIECES[PIDX[name]]
        ref = buf[arr]
        if bycol:
            k = max(1, -(-n // nc))
            assert n % k == 0
            part = ref.at[pl.ds(0, rows * k), pl.ds(c0, n // k)]
        else:
            part = ref.at[pl.ds(0, n), pl.ds(c0, nc)]
        pltpu.make_async_copy(part, part, sem).wait()

    def units(name, what):
        _, arr, bycol, rows, c0, nc, e = PIECES[PIDX[name]]
        n = nc if bycol else rows
        return {'XYE': 2 * e, 'XYS': 2 * (n - 2 * e), 'Z1': e, 'Z2': e, 'DY': e, 'DX': n - 2 * e, 'Z3': e, 'DXZ': n - e, 'SS': 4 * n,
                'S0': n, 'S1': n, 'S2': n, 'S3': n, 'sent': 7 * n}[what]

    FIRST = {'XYE': 'XE', 'XYS': 'XS', 'DXZ': 'DX', 'SS': 'S0'}

    def local(name):
        piece = PIECES[PIDX[name]]
        r0, c0 = region(piece, f, 'A', False)
        r1, c1 = region(piece, f, 'A', True)
        return pltpu.make_async_copy(src[piece[1]].at[r0, c0], buf[piece[1]].at[r1, c1], lsem.at[PIDX[name]])

    def start(names, *kinds):
        for k in kinds:
            for n in names:
                copy(n, k).start()

    def recv(names, *kinds):
        for k in kinds:
            for n in names:
                k = {'S1a+S1b': 'S1', 'S2a+S2b': 'S2', 'S3a+S3b': 'S3'}.get(k, k)
                first = k + 'a' if k in ('S1', 'S2', 'S3') else FIRST.get(k, k)
                take(n, units(n, k), rsem_of(n, first))

    def comm(todo):
        for op in todo:
            stage, piece = op[0], op[1]
            names = GROUPS[piece]
            if stage == 'recv':
                recv(names, op[2])
                continue
            if stage == 'st0' and piece == 'O0':
                stage_o.wait()
            waits, starts = STAGES[stage]
            recv(names, *waits)
            start(names, *starts)
            if stage == 'st0':
                for n in names:
                    local(n).start()
            if stage in ('fin', 'find'):
                for n in names:
                    if piece not in ('dq', 'dkv'):
                        local(n).wait()

    def at(seg, i):
        marks = sorted((int(n[len(seg):]), n) for n in SCHED if n.startswith(seg) and n[len(seg):].isdigit() and SCHED[n])

        def tree(ms):
            if len(ms) == 1:
                @pl.when(i == ms[0][0])
                def _():
                    with jax.named_scope('comm_' + ms[0][1]):
                        comm(SCHED[ms[0][1]])
            elif ms:
                h = len(ms) // 2
                lax.cond(i < ms[h][0], lambda: tree(ms[:h]), lambda: tree(ms[h:]))
        tree(marks)

    for i in range(T // TA):
        pltpu.make_async_copy(x_hbm.at[pl.ds(i * TA, TA)], xa.at[pl.ds(i * TA, TA)], xsem.at[i]).start()
    stage_o = pltpu.make_async_copy(o_s, ostage, osem.at[2])
    stage_o.start()

    barrier = pltpu.get_barrier_semaphore()
    with jax.named_scope('barrier'):
        for p in plane:
            pl.semaphore_signal(barrier, inc=1, device_id=(z, p), device_id_type=MESH)
        pl.semaphore_signal(barrier, inc=1, device_id=dev['Z'], device_id_type=MESH)
        pl.semaphore_wait(barrier, 8)

    for j, (gs, gb) in enumerate(((g1_s, g1b), (gq_s, gqb), (gkv_s, gkvb))):
        for p in plane:
            pltpu.make_async_remote_copy(src_ref=gs, dst_ref=gb.at[f], send_sem=gss.at[j], recv_sem=grs.at[j],
                                         device_id=(z, p), device_id_type=MESH).start()
        pltpu.make_async_copy(gs, gb.at[f], grs.at[j]).start()
    comm(SCHED['stats0'])

    def stat_tile(i, _):
        @pl.when(i == 4)
        def _():
            comm(SCHED['stats1'])
        pltpu.make_async_copy(x_hbm.at[pl.ds(i * TA, TA)], xa.at[pl.ds(i * TA, TA)], xsem.at[i]).wait()
        zero = jnp.zeros((TA, 128), F32)
        for j in range(QR // 128):
            accq[pl.ds(pl.multiple_of(i * TA, TA), TA), 128 * j:128 * j + 128] = zero
        acck[pl.ds(pl.multiple_of(i * TA, TA), TA), :] = jnp.zeros((TA, KR + RD), F32)
        for h in range(TA // 64):
            rows = pl.ds(pl.multiple_of(i * TA + h * 64, 64), 64)
            inv[rows, :] = jnp.broadcast_to(rms(xa[rows, :].astype(F32)), (64, 128))
        return 0

    with jax.named_scope('stats'):
        lax.fori_loop(0, T // TA, stat_tile, 0)
    with jax.named_scope('gains'):
        for j, gb in enumerate((g1b, gqb, gkvb)):
            pltpu.make_async_copy(gb, gb, grs.at[j]).wait()

    def row_of(gb):
        return jnp.concatenate([gb[i].astype(F32) for i in range(8)], axis=-1)

    g1, gq, gkv = row_of(g1b), row_of(gqb), row_of(gkvb)

    def norm_tile(i, _):
        pl.when(i % 2 == 0)(functools.partial(at, 'norm', i // 2))
        for h in range(TA // 64):
            rows = pl.ds(pl.multiple_of(i * TA + h * 64, 64), 64)
            scale = inv[rows, :]
            for j in range(D // 128):
                cols = slice(128 * j, 128 * j + 128)
                xa[rows, cols] = (xa[rows, cols].astype(F32) * scale * g1[:, cols]).astype(BF16)
        return 0

    def part(i, _):
        at('part', i)
        which, t = i // 4, i % 4
        quarter = ((yy + which // 2) % 2) * 2 + (xx + which % 2) % 2
        cols = pl.ds(pl.multiple_of(quarter * 640, 128), 640)
        rows = pl.ds(pl.multiple_of(t * 512, 512), 512)
        a = xa[rows, cols]
        accq[rows, :] += dot(a, wdq[cols, :])
        acck[rows, :] += dot(a, wdkv[cols, :])
        return 0

    cos2 = jnp.concatenate([cos_ref[...]] * (TA // S), axis=0)
    sin2 = jnp.concatenate([sin_ref[...]] * (TA // S), axis=0)

    def last_part():
        cols = pl.ds(pl.multiple_of((fd // 2) * 640, 128), 640)

        def tile(i, _):
            pl.when(i % 2 == 0)(functools.partial(at, 'd', i // 2))
            rows = pl.ds(pl.multiple_of(i * TA, TA), TA)
            a = xa[rows, cols]
            qd = accq[rows, :] + dot(a, wdq[cols, :])
            kd = acck[rows, :] + dot(a, wdkv[cols, :])
            cqT[:, rows] = (qd * rms(qd) * gq).astype(BF16).T
            kc = kd[:, :KR]
            c = (kc * rms(kc) * gkv).astype(BF16)
            cbuf[rows, :] = c
            cT[:, rows] = c.T
            lo, hi = kd[:, KR:KR + 16], kd[:, KR + 16:]
            rbuf[rows, :] = jnp.concatenate([lo * cos2 - hi * sin2, hi * cos2 + lo * sin2], axis=-1).astype(BF16)
            for h in range(TA // S):
                rT[i * (TA // S) + h] = rbuf[pl.ds(pl.multiple_of(i * TA + h * S, S), S), :].T
            return 0
        lax.fori_loop(0, T // TA, tile, 0)

    with jax.named_scope('norm'):
        lax.fori_loop(0, T // TA, norm_tile, 0)
    for n in ('dq', 'dkv'):
        local(n).wait()
    with jax.named_scope('parts'):
        lax.fori_loop(0, 12, part, 0)
    with jax.named_scope('last'):
        last_part()
    outs = [pltpu.make_async_copy(cbuf, c_hbm, csem.at[0]), pltpu.make_async_copy(rT, r_hbm, csem.at[1])]
    for o in outs:
        o.start()

    keep = lax.broadcasted_iota(jnp.int32, (S, S), 0) <= lax.broadcasted_iota(jnp.int32, (S, S), 1)
    lane = lax.broadcasted_iota(jnp.int32, (S, 128), 1)
    co, si = cosT_ref[...], sinT_ref[...]
    for h in range(HG):
        zr = 128 * h + (96 if h % 2 == 0 else 32)
        qT[zr:zr + 32, :] = jnp.zeros((32, TC), BF16)

    def load_group(g):
        uc = pl.ds(pl.multiple_of(g * (HG * 96), 128), HG * 96)
        wqT[...] = wuq[:, uc].T
        for j in range(HG // 2):
            t0 = wukv[:, pl.ds(pl.multiple_of(g * (HG * 128) + 256 * j, 128), 128)]
            t1 = wukv[:, pl.ds(pl.multiple_of(g * (HG * 128) + 256 * j + 128, 128), 128)]
            wk[:, 128 * j:128 * j + 128] = jnp.concatenate([t0[:, :64], t1[:, :64]], axis=1)
            wvT[128 * j:128 * j + 128, :] = jnp.concatenate([t0[:, 64:], t1[:, 64:]], axis=1).T

    def out_copy(i):
        g, tc = i // NCH, i % NCH
        return pltpu.make_async_copy(obuf.at[i % 2], attn_hbm.at[pl.ds(pl.multiple_of(tc * TC, TC), TC), pl.ds(pl.multiple_of(g * (HG * 64), 128), HG * 64)], osem.at[i % 2])

    def step(i, _):
        g, tc = i // NCH, i % NCH
        tok = pl.multiple_of(tc * TC, TC)
        at('s', i)

        @pl.when(tc == 0)
        def _():
            with jax.named_scope('load_group'):
                load_group(g)

        @pl.when(i >= 2)
        def _():
            out_copy(i - 2).wait()

        slot = i % 2
        for n in range(TC // 256):
            q = dot(wqT[...], cqT[:, pl.ds(tok + 256 * n, 256)])
            cols = slice(256 * n, 256 * n + 256)
            for h in range(HG):
                nope = q[96 * h:96 * h + 64]
                lo, hi = q[96 * h + 64:96 * h + 80], q[96 * h + 80:96 * h + 96]
                b = 128 * h
                qn, qp = (b, b + 64) if h % 2 == 0 else (b + 64, b)
                qT[qn:qn + 64, cols] = nope.astype(BF16)
                qT[qp:qp + 16, cols] = (lo * co - hi * si).astype(BF16)
                qT[qp + 16:qp + 32, cols] = (hi * co + lo * si).astype(BF16)
        kbuf[...] = dot(cbuf[pl.ds(tok, TC), :], wk[...]).astype(BF16)
        vT[...] = dot(wvT[...], cT[:, pl.ds(tok, TC)]).astype(BF16)

        for p in range(TC // S):
            row = p * S
            r = rbuf[pl.ds(tok + row, S), :]
            z32, z64 = jnp.zeros((S, 32), BF16), jnp.zeros((S, 64), BF16)
            r_hi = jnp.concatenate([z64, r, z32], axis=1)
            r_lo = jnp.concatenate([r, z32, z64], axis=1)
            for j in range(HG // 2):
                k2 = kbuf[row:row + S, 128 * j:128 * j + 128]
                both = []
                for par in range(2):
                    h = 2 * j + par
                    k = jnp.where(lane < 64, k2, r_hi) if par == 0 else jnp.where(lane < 64, r_lo, k2)
                    both.append(attn_unit(k, qT[128 * h:128 * h + 128, row:row + S], vT[64 * h:64 * h + 64, row:row + S], keep))
                obuf[slot, row:row + S, 128 * j:128 * j + 128] = jnp.concatenate(both, axis=0).astype(BF16).T
        out_copy(i).start()
        return 0

    lax.fori_loop(0, STEPS, step, 0)
    with jax.named_scope('fin_O'):
        comm(SCHED['end'])
    with jax.named_scope('tail_out'):
        for i in (STEPS - 2, STEPS - 1):
            out_copy(i).wait()
        for o in outs:
            o.wait()
    with jax.named_scope('tail_sends'):
        for j, gb in enumerate((g1b, gqb, gkvb)):
            pltpu.make_async_copy(gb.at[pl.ds(0, 7)], gb.at[pl.ds(0, 7)], gss.at[j]).wait()
        for p in PIECES:
            take(p[0], units(p[0], 'sent'), ssem.at[PIDX[p[0]]])


def front(x, gains, ws, cos, sin):
    anyspace, vm = pl.BlockSpec(memory_space=pl.ANY), pl.BlockSpec(memory_space=pltpu.VMEM)
    V = pltpu.VMEM
    dma = pltpu.SemaphoreType.DMA
    tab = [cos, sin, np.tile(cos.T, (1, 2)), np.tile(sin.T, (1, 2))]
    return pl.pallas_call(
        front_kernel, name='front',
        in_specs=[anyspace] + [vm] * 3 + [anyspace] * 5 + [vm] * 4,
        out_specs=[anyspace] * 4,
        out_shape=[jax.ShapeDtypeStruct((T, H * VD), BF16), jax.ShapeDtypeStruct((H * VD, D), BF16), jax.ShapeDtypeStruct((T, KR), BF16), jax.ShapeDtypeStruct((T // S, RD, S), BF16)],
        scratch_shapes=[
            V((T, D), BF16), V((D, QR), BF16), V((D, KR + RD), BF16), V((QR, H * 96), BF16), V((KR, H * 128), BF16), V((320, D), BF16),
            V((8, 1, 320), BF16), V((8, 1, 96), BF16), V((8, 1, 32), BF16), V((T, QR), F32), V((T, KR + RD), F32), V((T, 128), F32),
            V((QR, T), BF16), V((T, KR), BF16), V((KR, T), BF16), V((T, RD), BF16), V((T // S, RD, S), BF16),
            V((HG * 96, QR), BF16), V((KR, HG * 64), BF16), V((HG * 64, KR), BF16), V((HG * 128, TC), BF16), V((TC, HG * 64), BF16), V((HG * 64, TC), BF16), V((2, TC, HG * 64), BF16),
            dma((len(PIECES),)), dma((len(PIECES) - 2, 7)), dma((2, 11)), dma((len(PIECES),)), dma((3,)), dma((3,)), dma((T // TA,)), dma((3,)), dma((2,)),
        ],
        compiler_params=pltpu.CompilerParams(collective_id=0, has_side_effects=True, vmem_limit_bytes=63 << 20),
    )(x, *gains, *ws, *(jnp.asarray(t) for t in tab))


def out_kernel(o_ref, w_ref, x_ref, c_ref, r_ref, y_ref, c_out, r_out):
    for n in range(0, y_ref.shape[1], 256):
        cols = slice(n, n + 256)
        y_ref[:, cols] = (x_ref[:, cols].astype(F32) + dot(o_ref[...], w_ref[:, cols])).astype(BF16)
    c_out[...] = c_ref[...]
    r_out[...] = r_ref[...]


def outp(o, w, x, c, r, tm=1024, tn=1280):
    nt = D // tn
    cr = T // ((T // tm) * nt)
    step = lambda j, i: j * (T // tm) + i
    return pl.pallas_call(
        out_kernel, grid=(nt, T // tm), name='outp',
        in_specs=[pl.BlockSpec((tm, D), lambda j, i: (i, 0)), pl.BlockSpec((D, tn), lambda j, i: (0, j)), pl.BlockSpec((tm, tn), lambda j, i: (i, j)),
                  pl.BlockSpec((cr, KR), lambda j, i: (step(j, i), 0)), pl.BlockSpec((cr // S, RD, S), lambda j, i: (step(j, i), 0, 0))],
        out_specs=[pl.BlockSpec((tm, tn), lambda j, i: (i, j)), pl.BlockSpec((cr, KR), lambda j, i: (step(j, i), 0)), pl.BlockSpec((cr // S, RD, S), lambda j, i: (step(j, i), 0, 0))],
        out_shape=[jax.ShapeDtypeStruct((T, D), BF16), jax.ShapeDtypeStruct((T, KR), BF16), jax.ShapeDtypeStruct((T // S, RD, S), BF16)],
        compiler_params=pltpu.CompilerParams(vmem_limit_bytes=62 << 20),
    )(o, w, x, c, r)


def tables():
    half = RD // 2
    freq = np.float32(10000.0) ** (np.float32(-2.0) * np.arange(half, dtype=np.float32) / np.float32(RD))
    ang = np.arange(S, dtype=np.float32)[:, None] * freq[None, :].astype(np.float32)
    return np.cos(ang).astype(np.float32), np.sin(ang).astype(np.float32)


def solution(mesh):
    batch, row, mat = P(('dp', 'fsdp')), P('fsdp'), P('fsdp', None)

    def local(tok, g1, wdq, gq, wuq, wkv, gkv, wukv, wo):
        cos, sin = tables()
        x = tok.reshape(T, D)
        o, w, c, r = front(x, (g1[None], gq[None], gkv[None]), (wdq, wkv, wuq, wukv, wo), cos, sin)
        y, c, r = outp(o, w, x, c, r)
        return y.reshape(tok.shape), c.reshape(-1, S, KR), jnp.swapaxes(r, 1, 2)

    return jax.shard_map(local, mesh=mesh, in_specs=(batch, row, mat, row, mat, mat, row, mat, mat),
                         out_specs=(batch,) * 3, check_vma=False)
```

```python
import functools
import numpy as np
import jax
import jax.numpy as jnp
from jax import lax
from jax.experimental import pallas as pl
from jax.experimental.pallas import tpu as pltpu
from jax.sharding import PartitionSpec as P

F32, BF16 = jnp.float32, jnp.bfloat16
MESH = pl.DeviceIdType.MESH
EPS = 1e-6
T, D, QR, KR, RD, H, ND, VD = 2048, 2560, 768, 256, 32, 40, 64, 64
S = 128
SC = (ND + RD) ** -0.5 * 1.4426950408889634
HG, TC = 8, 512
NCH = T // TC
STEPS = (H // HG) * NCH
TA = 256


def dot(a, b):
    return jnp.dot(a, b, preferred_element_type=F32)


def rms(v):
    return lax.rsqrt(jnp.mean(v * v, axis=-1, keepdims=True) + EPS)


def attn_unit(k, qT, vT, keep):
    s = dot(k, qT) * SC
    s = jnp.where(keep, s, -1e30)
    m = jnp.max(s, axis=0, keepdims=True)
    e = jnp.exp2(s - m)
    p = (e * (1.0 / jnp.sum(e, axis=0, keepdims=True))).astype(BF16)
    return dot(vT, p)


PIECES = (
    ('dq', 'dq', False, 320, 0, 768, 96),
    ('dkv', 'dkv', False, 320, 0, 288, 96),
    ('uq0', 'uq', False, 96, 0, 768, 32),
    ('ukv0', 'ukv', True, 32, 0, 1024, 384),
    ('uq1', 'uq', False, 96, 768, 1536, 32),
    ('ukv1', 'ukv', True, 32, 1024, 2048, 512),
    ('uq2', 'uq', False, 96, 2304, 1536, 32),
    ('ukv2', 'ukv', True, 32, 3072, 2048, 512),
    ('o0', 'o', False, 320, 0, 512, 96),
    ('o1', 'o', False, 320, 512, 512, 96),
    ('o2', 'o', False, 320, 1024, 512, 96),
    ('o3', 'o', False, 320, 1536, 512, 96),
    ('o4', 'o', False, 320, 2048, 512, 96),
)
PIDX = {p[0]: i for i, p in enumerate(PIECES)}
SPLIT = ('S1a', 'S1b', 'S2a', 'S2b', 'S3a', 'S3b')
KINDS = ('XE', 'YE', 'XS', 'YS', 'S0', 'Z1', 'Z2', 'DY', 'DX', 'Z3', 'S1', 'S2', 'S3') + SPLIT
RSEM = {'XE': 0, 'YE': 0, 'XS': 1, 'YS': 1, 'Z1': 2, 'Z2': 3, 'DY': 4, 'DX': 5, 'Z3': 5, 'S0': 6, 'S1': 6, 'S2': 6, 'S3': 6}
RSEM_SPLIT = dict(RSEM, Z3=7, S1a=8, S1b=8, S2a=9, S2b=9, S3a=10, S3b=10)
SPLIT_ARRS = ('dq', 'dkv')
GROUPS = {'K': ('dkv',), 'D': ('dq',), 'U0': ('uq0', 'ukv0'), 'U1': ('uq1', 'ukv1'), 'U2': ('uq2', 'ukv2'),
          'O0': ('o0',), 'O1': ('o1',), 'O2': ('o2',), 'O3': ('o3',), 'O4': ('o4',)}
STAGES = {
    'st0': ((), ('XE', 'YE', 'XS', 'YS', 'S0')),
    'st1': (('XYE',), ('Z1', 'Z2', 'DY')),
    'st2': (('XYS',), ('DX',)),
    'st4x': (('Z1',), ('S1',)),
    'st3': (('DY',), ('Z3',)),
    'st4y': (('Z2',), ('S2',)),
    'st5': (('DXZ',), ('S3',)),
    'fin': (('SS',), ()),
    'st2d': (('XYS',), ('DX', 'S1a', 'S2a')),
    'st4xd': (('Z1',), ('S1b',)),
    'st4yd': (('Z2',), ('S2b',)),
    'st5a': (('DX',), ('S3a',)),
    'st5b': (('Z3',), ('S3b',)),
    'find': ((), ()),
}
SCHED = {
    'stats0': (('st0', 'K'),),
    'stats1': (('st0', 'D'),),
    'norm1': (('st1', 'K'),),
    'part0': (('st2d', 'K'), ('recv', 'K', 'S0'), ('recv', 'D', 'S0')),
    'part2': (('st4xd', 'K'), ('st0', 'U0'), ('st1', 'D')),
    'k0': (('recv', 'K', 'S1a+S1b'),),
    'k2': (('st2d', 'D'), ('st3', 'K'), ('st4yd', 'K'), ('st4xd', 'D'), ('recv', 'K', 'S2a+S2b'), ('st5a', 'K')),
    'k3': (('st1', 'U0'),),
    'k4': (('st5b', 'K'), ('st2', 'U0'), ('recv', 'K', 'S3a+S3b'), ('st0', 'U1'), ('st0', 'U2')),
    'k5': (('st3', 'D'), ('st4yd', 'D'), ('st4x', 'U0')),
    'q0': (('st5a', 'D'), ('recv', 'D', 'S1a+S1b')),
    'q1': (('st3', 'U0'), ('st4y', 'U0')),
    'q4': (('st1', 'U1'), ('st5b', 'D'), ('recv', 'D', 'S2a+S2b')),
    'q6': (('st5', 'U0'),),
    'd0': (('st2', 'U1'), ('recv', 'D', 'S3a+S3b')),
    'd1': (('fin', 'U0'),),
    'd2': (('st4x', 'U1'), ('st1', 'U2')),
    's0': (('st2', 'U2'),),
    's1': (('st3', 'U1'), ('st4y', 'U1'), ('st4x', 'U2'), ('st0', 'O0'), ('st0', 'O1')),
    's2': (('st3', 'U2'), ('st4y', 'U2')),
    's3': (('st5', 'U1'),),
    's4': (('st1', 'O0'), ('fin', 'U1')),
    's5': (('st5', 'U2'), ('st2', 'O0'), ('st1', 'O1')),
    's6': (('fin', 'U2'), ('st4x', 'O0'), ('st2', 'O1'), ('st0', 'O2')),
    's7': (('st3', 'O0'), ('st4y', 'O0')),
    's8': (('st4x', 'O1'), ('st3', 'O1'), ('st0', 'O3')),
    's9': (('st5', 'O0'), ('st4y', 'O1'), ('st1', 'O2')),
    's10': (('fin', 'O0'), ('st5', 'O1'), ('st2', 'O2')),
    's11': (('fin', 'O1'), ('st4x', 'O2'), ('st1', 'O3')),
    's12': (('st2', 'O3'), ('st0', 'O4')),
    's13': (('st3', 'O2'), ('st4y', 'O2'), ('st4x', 'O3')),
    's14': (('st3', 'O3'), ('st4y', 'O3')),
    's15': (('st5', 'O2'), ('st1', 'O4')),
    's16': (('fin', 'O2'), ('st5', 'O3'), ('st2', 'O4')),
    's17': (('fin', 'O3'), ('st4x', 'O4'), ('st3', 'O4')),
    's18': (('st4y', 'O4'),),
    's19': (('st5', 'O4'),),
    'end': (('fin', 'O4'),),
}
SWAPPED = ('dkv', 'uq1', 'ukv1', 'o0', 'o3', 'o4')


def front_kernel(x_hbm, g1_s, gq_s, gkv_s, dq_s, dkv_s, uq_s, ukv_s, o_s, cos_ref, sin_ref, cosT_ref, sinT_ref,
                 attn_hbm, wo_hbm, c_hbm, r_hbm,
                 xa, wdq, wdkv, wuq, wukv, ostage, g1b, gqb, gkvb, accq, acck, inv, cqT, cbuf, cT, rbuf, rT,
                 wqT, wk, wvT, qT, kbuf, vT, obuf,
                 ssem, rsem, dsem, lsem, gss, grs, xsem, osem, csem):
    z, f = lax.axis_index('dp'), lax.axis_index('fsdp')
    core, xx, yy = f % 2, (f // 2) % 2, f // 4

    def idx(dx, dy, dc):
        return ((yy + dy) % 2) * 4 + ((xx + dx) % 2) * 2 + (core + dc) % 2

    fx, fy, fd = idx(1, 0, 0), idx(0, 1, 0), idx(1, 1, 0)
    dev = {'X': (z, fx), 'Y': (z, fy), 'Z': (1 - z, f), 'S': (z, idx(0, 0, 1))}
    plane = [idx(dx, dy, dc) for dx in range(2) for dy in range(2) for dc in range(2) if dx + dy + dc]
    src = {'dq': dq_s, 'dkv': dkv_s, 'uq': uq_s, 'ukv': ukv_s, 'o': ostage}
    buf = {'dq': wdq, 'dkv': wdkv, 'uq': wuq, 'ukv': wukv, 'o': wo_hbm}

    def region(piece, shard, part, base):
        name, arr, bycol, rows, c0, nc, e = piece
        n = nc if bycol else rows
        off, size = {'E': (z * (n - e), e), 'S': (e, n - 2 * e), 'A': (0, n), 'B': (z * e, n - e), 'M': ((1 - z) * (n - e), e)}[part]
        if bycol:
            row = shard * rows if base else 0
            return pl.ds(pl.multiple_of(row, 16), rows), pl.ds(pl.multiple_of(c0 + off, 128), size)
        row = (shard * rows if base else 0) + off
        return pl.ds(pl.multiple_of(row, 16), size), pl.ds(c0, nc)

    def copy(name, kind):
        piece = PIECES[PIDX[name]]
        arr = piece[1]
        shard = {'X': f, 'Y': f}.get(kind[0]) if kind in ('XE', 'YE', 'XS', 'YS') else None
        if kind in ('XE', 'YE', 'XS', 'YS', 'S0'):
            part = 'A' if kind == 'S0' else kind[1]
            r0, c0 = region(piece, f, part, False)
            r1, c1 = region(piece, f, part, True)
            s_ref, d_ref = src[arr].at[r0, c0], buf[arr].at[r1, c1]
            to = dev[kind[0]]
        else:
            shard, part, to = {'Z1': (fx, 'E', 'Z'), 'Z2': (fy, 'E', 'Z'), 'Z3': (fd, 'E', 'Z'), 'DY': (fx, 'E', 'Y'),
                               'DX': (fy, 'S', 'X'), 'S1': (fx, 'A', 'S'), 'S2': (fy, 'A', 'S'), 'S3': (fd, 'A', 'S'),
                               'S1a': (fx, 'B', 'S'), 'S1b': (fx, 'M', 'S'), 'S2a': (fy, 'B', 'S'), 'S2b': (fy, 'M', 'S'),
                               'S3a': (fd, 'B', 'S'), 'S3b': (fd, 'M', 'S')}[kind]
            if name in SWAPPED and kind in ('DX', 'DY'):
                shard, to = {'DX': (fx, 'Y'), 'DY': (fy, 'X')}[kind]
            to = dev[to]
            r1, c1 = region(piece, shard, part, True)
            s_ref = d_ref = buf[arr].at[r1, c1]
        return pltpu.make_async_remote_copy(src_ref=s_ref, dst_ref=d_ref, send_sem=ssem.at[PIDX[name]], recv_sem=rsem_of(name, kind),
                                            device_id=to, device_id_type=MESH)

    def rsem_of(name, kind):
        if PIECES[PIDX[name]][1] in SPLIT_ARRS:
            return dsem.at[PIDX[name], RSEM_SPLIT[kind]]
        return rsem.at[PIDX[name] - 2, RSEM[kind]]

    def take(name, n, sem, rows_too=True):
        _, arr, bycol, rows, c0, nc, e = PIECES[PIDX[name]]
        ref = buf[arr]
        if bycol:
            k = max(1, -(-n // nc))
            assert n % k == 0
            part = ref.at[pl.ds(0, rows * k), pl.ds(c0, n // k)]
        else:
            part = ref.at[pl.ds(0, n), pl.ds(c0, nc)]
        pltpu.make_async_copy(part, part, sem).wait()

    def units(name, what):
        _, arr, bycol, rows, c0, nc, e = PIECES[PIDX[name]]
        n = nc if bycol else rows
        return {'XYE': 2 * e, 'XYS': 2 * (n - 2 * e), 'Z1': e, 'Z2': e, 'DY': e, 'DX': n - 2 * e, 'Z3': e, 'DXZ': n - e, 'SS': 4 * n,
                'S0': n, 'S1': n, 'S2': n, 'S3': n, 'sent': 7 * n}[what]

    FIRST = {'XYE': 'XE', 'XYS': 'XS', 'DXZ': 'DX', 'SS': 'S0'}

    def local(name):
        piece = PIECES[PIDX[name]]
        r0, c0 = region(piece, f, 'A', False)
        r1, c1 = region(piece, f, 'A', True)
        return pltpu.make_async_copy(src[piece[1]].at[r0, c0], buf[piece[1]].at[r1, c1], lsem.at[PIDX[name]])

    def start(names, *kinds):
        for k in kinds:
            for n in names:
                copy(n, k).start()

    def recv(names, *kinds):
        for k in kinds:
            for n in names:
                k = {'S1a+S1b': 'S1', 'S2a+S2b': 'S2', 'S3a+S3b': 'S3'}.get(k, k)
                first = k + 'a' if k in ('S1', 'S2', 'S3') else FIRST.get(k, k)
                take(n, units(n, k), rsem_of(n, first))

    def comm(todo):
        for op in todo:
            stage, piece = op[0], op[1]
            names = GROUPS[piece]
            if stage == 'recv':
                recv(names, op[2])
                continue
            if stage == 'st0' and piece == 'O0':
                stage_o.wait()
            waits, starts = STAGES[stage]
            recv(names, *waits)
            start(names, *starts)
            if stage == 'st0':
                for n in names:
                    local(n).start()
            if stage in ('fin', 'find'):
                for n in names:
                    if piece not in ('K', 'D'):
                        local(n).wait()

    def at(seg, i):
        marks = sorted((int(n[len(seg):]), n) for n in SCHED if n.startswith(seg) and n[len(seg):].isdigit() and SCHED[n])

        def tree(ms):
            if len(ms) == 1:
                @pl.when(i == ms[0][0])
                def _():
                    with jax.named_scope('comm_' + ms[0][1]):
                        comm(SCHED[ms[0][1]])
            elif ms:
                h = len(ms) // 2
                lax.cond(i < ms[h][0], lambda: tree(ms[:h]), lambda: tree(ms[h:]))
        tree(marks)

    for i in range(T // TA):
        pltpu.make_async_copy(x_hbm.at[pl.ds(i * TA, TA)], xa.at[pl.ds(i * TA, TA)], xsem.at[i]).start()
    stage_o = pltpu.make_async_copy(o_s, ostage, osem.at[2])
    stage_o.start()

    barrier = pltpu.get_barrier_semaphore()
    with jax.named_scope('barrier'):
        for p in plane:
            pl.semaphore_signal(barrier, inc=1, device_id=(z, p), device_id_type=MESH)
        pl.semaphore_signal(barrier, inc=1, device_id=dev['Z'], device_id_type=MESH)
        pl.semaphore_wait(barrier, 8)

    for j, (gs, gb) in enumerate(((g1_s, g1b), (gq_s, gqb), (gkv_s, gkvb))):
        for p in plane:
            pltpu.make_async_remote_copy(src_ref=gs, dst_ref=gb.at[f], send_sem=gss.at[j], recv_sem=grs.at[j],
                                         device_id=(z, p), device_id_type=MESH).start()
        pltpu.make_async_copy(gs, gb.at[f], grs.at[j]).start()
    comm(SCHED['stats0'])

    def stat_tile(i, _):
        @pl.when(i == 4)
        def _():
            comm(SCHED['stats1'])
        pltpu.make_async_copy(x_hbm.at[pl.ds(i * TA, TA)], xa.at[pl.ds(i * TA, TA)], xsem.at[i]).wait()
        for h in range(TA // 64):
            rows = pl.ds(pl.multiple_of(i * TA + h * 64, 64), 64)
            inv[rows, :] = jnp.broadcast_to(rms(xa[rows, :].astype(F32)), (64, 128))
        return 0

    with jax.named_scope('stats'):
        lax.fori_loop(0, T // TA, stat_tile, 0)
    with jax.named_scope('gains'):
        for j, gb in enumerate((g1b, gqb, gkvb)):
            pltpu.make_async_copy(gb, gb, grs.at[j]).wait()

    def row_of(gb):
        return jnp.concatenate([gb[i].astype(F32) for i in range(8)], axis=-1)

    g1, gq, gkv = row_of(g1b), row_of(gqb), row_of(gkvb)

    def norm_tile(i, _):
        pl.when(i % 2 == 0)(functools.partial(at, 'norm', i // 2))
        for h in range(TA // 64):
            rows = pl.ds(pl.multiple_of(i * TA + h * 64, 64), 64)
            scale = inv[rows, :]
            for j in range(D // 128):
                cols = slice(128 * j, 128 * j + 128)
                xa[rows, cols] = (xa[rows, cols].astype(F32) * scale * g1[:, cols]).astype(BF16)
        return 0

    def quarter_cols(dy, dx):
        quarter = ((yy + dy) % 2) * 2 + (xx + dx) % 2
        return pl.ds(pl.multiple_of(quarter * 640, 128), 640)

    def own_part(i, _):
        at('part', i)
        cols, rows = quarter_cols(0, 0), pl.ds(pl.multiple_of(i * 512, 512), 512)
        a = xa[rows, cols]
        accq[rows, :] = dot(a, wdq[cols, :])
        acck[rows, :] = dot(a, wdkv[cols, :])
        return 0

    def kv_part(i, _):
        at('k', i)
        q = i // 2 + 1
        cols, rows = quarter_cols(q // 2, q % 2), pl.ds(pl.multiple_of((i % 2) * 1024, 1024), 1024)
        acck[rows, :] += dot(xa[rows, cols], wdkv[cols, :])
        return 0

    def q_part(x_not_y, i, _):
        at('q', i if x_not_y else i + 4)
        if x_not_y:
            finish_kv(2 * i)
            finish_kv(2 * i + 1)
        cols, rows = quarter_cols(0, 1) if x_not_y else quarter_cols(1, 0), pl.ds(pl.multiple_of(i * 512, 512), 512)
        accq[rows, :] += dot(xa[rows, cols], wdq[cols, :])
        return 0

    cos2 = jnp.concatenate([cos_ref[...]] * (TA // S), axis=0)
    sin2 = jnp.concatenate([sin_ref[...]] * (TA // S), axis=0)

    def finish_kv(i):
        rows = pl.ds(pl.multiple_of(i * TA, TA), TA)
        kd = acck[rows, :]
        kc = kd[:, :KR]
        c = (kc * rms(kc) * gkv).astype(BF16)
        cbuf[rows, :] = c
        cT[:, rows] = c.T
        lo, hi = kd[:, KR:KR + 16], kd[:, KR + 16:]
        r = jnp.concatenate([lo * cos2 - hi * sin2, hi * cos2 + lo * sin2], axis=-1).astype(BF16)
        rbuf[rows, :] = r
        for h in range(TA // S):
            rT[i * (TA // S) + h] = r[h * S:h * S + S].T

    def finish_q(i):
        rows = pl.ds(pl.multiple_of(i * TA, TA), TA)
        qd = accq[rows, :]
        cqT[:, rows] = (qd * rms(qd) * gq).astype(BF16).T

    def last_part():
        cols = pl.ds(pl.multiple_of((fd // 2) * 640, 128), 640)

        def tile(i, _):
            pl.when(i % 2 == 0)(functools.partial(at, 'd', i // 2))
            finish_q(jnp.maximum(i - 1, 0))
            rows = pl.ds(pl.multiple_of(jnp.minimum(i, T // TA - 1) * TA, TA), TA)
            accq[rows, :] += dot(xa[rows, cols], wdq[cols, :])
            return 0
        lax.fori_loop(0, T // TA + 1, tile, 0)

    with jax.named_scope('norm'):
        lax.fori_loop(0, T // TA, norm_tile, 0)
    for n in ('dq', 'dkv'):
        local(n).wait()
    with jax.named_scope('own'):
        lax.fori_loop(0, 4, own_part, 0)
    with jax.named_scope('kv'):
        lax.fori_loop(0, 6, kv_part, 0)
    with jax.named_scope('qx'):
        lax.fori_loop(0, 4, functools.partial(q_part, True), 0)
    with jax.named_scope('qy'):
        lax.fori_loop(0, 4, functools.partial(q_part, False), 0)
    with jax.named_scope('last'):
        last_part()
    outs = [pltpu.make_async_copy(cbuf, c_hbm, csem.at[0]), pltpu.make_async_copy(rT, r_hbm, csem.at[1])]
    for o in outs:
        o.start()

    keep = lax.broadcasted_iota(jnp.int32, (S, S), 0) <= lax.broadcasted_iota(jnp.int32, (S, S), 1)
    lane = lax.broadcasted_iota(jnp.int32, (S, 128), 1)
    co, si = cosT_ref[...], sinT_ref[...]
    for h in range(HG):
        zr = 128 * h + (96 if h % 2 == 0 else 32)
        qT[zr:zr + 32, :] = jnp.zeros((32, TC), BF16)

    def load_group(g):
        uc = pl.ds(pl.multiple_of(g * (HG * 96), 128), HG * 96)
        wqT[...] = wuq[:, uc].T
        for j in range(HG // 2):
            t0 = wukv[:, pl.ds(pl.multiple_of(g * (HG * 128) + 256 * j, 128), 128)]
            t1 = wukv[:, pl.ds(pl.multiple_of(g * (HG * 128) + 256 * j + 128, 128), 128)]
            wk[:, 128 * j:128 * j + 128] = jnp.concatenate([t0[:, :64], t1[:, :64]], axis=1)
            wvT[128 * j:128 * j + 128, :] = jnp.concatenate([t0[:, 64:], t1[:, 64:]], axis=1).T

    def out_copy(i):
        g, tc = i // NCH, i % NCH
        return pltpu.make_async_copy(obuf.at[i % 2], attn_hbm.at[pl.ds(pl.multiple_of(tc * TC, TC), TC), pl.ds(pl.multiple_of(g * (HG * 64), 128), HG * 64)], osem.at[i % 2])

    def step(i, _):
        g, tc = i // NCH, i % NCH
        tok = pl.multiple_of(tc * TC, TC)
        at('s', i)

        @pl.when(tc == 0)
        def _():
            with jax.named_scope('load_group'):
                load_group(g)

        @pl.when(i >= 2)
        def _():
            out_copy(i - 2).wait()

        slot = i % 2
        for n in range(TC // 256):
            q = dot(wqT[...], cqT[:, pl.ds(tok + 256 * n, 256)])
            cols = slice(256 * n, 256 * n + 256)
            for h in range(HG):
                nope = q[96 * h:96 * h + 64]
                lo, hi = q[96 * h + 64:96 * h + 80], q[96 * h + 80:96 * h + 96]
                b = 128 * h
                qn, qp = (b, b + 64) if h % 2 == 0 else (b + 64, b)
                qT[qn:qn + 64, cols] = nope.astype(BF16)
                qT[qp:qp + 16, cols] = (lo * co - hi * si).astype(BF16)
                qT[qp + 16:qp + 32, cols] = (hi * co + lo * si).astype(BF16)
        kbuf[...] = dot(cbuf[pl.ds(tok, TC), :], wk[...]).astype(BF16)
        vT[...] = dot(wvT[...], cT[:, pl.ds(tok, TC)]).astype(BF16)

        for p in range(TC // S):
            row = p * S
            r = rbuf[pl.ds(tok + row, S), :]
            z32, z64 = jnp.zeros((S, 32), BF16), jnp.zeros((S, 64), BF16)
            r_hi = jnp.concatenate([z64, r, z32], axis=1)
            r_lo = jnp.concatenate([r, z32, z64], axis=1)
            for j in range(HG // 2):
                k2 = kbuf[row:row + S, 128 * j:128 * j + 128]
                both = []
                for par in range(2):
                    h = 2 * j + par
                    k = jnp.where(lane < 64, k2, r_hi) if par == 0 else jnp.where(lane < 64, r_lo, k2)
                    both.append(attn_unit(k, qT[128 * h:128 * h + 128, row:row + S], vT[64 * h:64 * h + 64, row:row + S], keep))
                obuf[slot, row:row + S, 128 * j:128 * j + 128] = jnp.concatenate(both, axis=0).astype(BF16).T
        out_copy(i).start()
        return 0

    lax.fori_loop(0, STEPS, step, 0)
    with jax.named_scope('fin_O'):
        comm(SCHED['end'])
    with jax.named_scope('tail_out'):
        for i in (STEPS - 2, STEPS - 1):
            out_copy(i).wait()
        for o in outs:
            o.wait()
    with jax.named_scope('tail_sends'):
        for j, gb in enumerate((g1b, gqb, gkvb)):
            pltpu.make_async_copy(gb.at[pl.ds(0, 7)], gb.at[pl.ds(0, 7)], gss.at[j]).wait()
        for p in PIECES:
            take(p[0], units(p[0], 'sent'), ssem.at[PIDX[p[0]]])


def front(x, gains, ws, cos, sin):
    anyspace, vm = pl.BlockSpec(memory_space=pl.ANY), pl.BlockSpec(memory_space=pltpu.VMEM)
    V = pltpu.VMEM
    dma = pltpu.SemaphoreType.DMA
    tab = [cos, sin, np.tile(cos.T, (1, 2)), np.tile(sin.T, (1, 2))]
    return pl.pallas_call(
        front_kernel, name='front',
        in_specs=[anyspace] + [vm] * 3 + [anyspace] * 5 + [vm] * 4,
        out_specs=[anyspace] * 4,
        out_shape=[jax.ShapeDtypeStruct((T, H * VD), BF16), jax.ShapeDtypeStruct((H * VD, D), BF16), jax.ShapeDtypeStruct((T, KR), BF16), jax.ShapeDtypeStruct((T // S, RD, S), BF16)],
        scratch_shapes=[
            V((T, D), BF16), V((D, QR), BF16), V((D, KR + RD), BF16), V((QR, H * 96), BF16), V((KR, H * 128), BF16), V((320, D), BF16),
            V((8, 1, 320), BF16), V((8, 1, 96), BF16), V((8, 1, 32), BF16), V((T, QR), F32), V((T, KR + RD), F32), V((T, 128), F32),
            V((QR, T), BF16), V((T, KR), BF16), V((KR, T), BF16), V((T, RD), BF16), V((T // S, RD, S), BF16),
            V((HG * 96, QR), BF16), V((KR, HG * 64), BF16), V((HG * 64, KR), BF16), V((HG * 128, TC), BF16), V((TC, HG * 64), BF16), V((HG * 64, TC), BF16), V((2, TC, HG * 64), BF16),
            dma((len(PIECES),)), dma((len(PIECES) - 2, 7)), dma((2, 11)), dma((len(PIECES),)), dma((3,)), dma((3,)), dma((T // TA,)), dma((3,)), dma((2,)),
        ],
        compiler_params=pltpu.CompilerParams(collective_id=0, has_side_effects=True, vmem_limit_bytes=63 << 20),
    )(x, *gains, *ws, *(jnp.asarray(t) for t in tab))


def out_kernel(o_ref, w_ref, x_ref, c_ref, r_ref, y_ref, c_out, r_out):
    for n in range(0, y_ref.shape[1], 256):
        cols = slice(n, n + 256)
        y_ref[:, cols] = (x_ref[:, cols].astype(F32) + dot(o_ref[...], w_ref[:, cols])).astype(BF16)
    c_out[...] = c_ref[...]
    r_out[...] = r_ref[...]


def outp(o, w, x, c, r, tm=1024, tn=1280):
    nt = D // tn
    cr = T // ((T // tm) * nt)
    step = lambda j, i: j * (T // tm) + i
    return pl.pallas_call(
        out_kernel, grid=(nt, T // tm), name='outp',
        in_specs=[pl.BlockSpec((tm, D), lambda j, i: (i, 0)), pl.BlockSpec((D, tn), lambda j, i: (0, j)), pl.BlockSpec((tm, tn), lambda j, i: (i, j)),
                  pl.BlockSpec((cr, KR), lambda j, i: (step(j, i), 0)), pl.BlockSpec((cr // S, RD, S), lambda j, i: (step(j, i), 0, 0))],
        out_specs=[pl.BlockSpec((tm, tn), lambda j, i: (i, j)), pl.BlockSpec((cr, KR), lambda j, i: (step(j, i), 0)), pl.BlockSpec((cr // S, RD, S), lambda j, i: (step(j, i), 0, 0))],
        out_shape=[jax.ShapeDtypeStruct((T, D), BF16), jax.ShapeDtypeStruct((T, KR), BF16), jax.ShapeDtypeStruct((T // S, RD, S), BF16)],
        compiler_params=pltpu.CompilerParams(vmem_limit_bytes=62 << 20),
    )(o, w, x, c, r)


def tables():
    half = RD // 2
    freq = np.float32(10000.0) ** (np.float32(-2.0) * np.arange(half, dtype=np.float32) / np.float32(RD))
    ang = np.arange(S, dtype=np.float32)[:, None] * freq[None, :].astype(np.float32)
    return np.cos(ang).astype(np.float32), np.sin(ang).astype(np.float32)


def solution(mesh):
    batch, row, mat = P(('dp', 'fsdp')), P('fsdp'), P('fsdp', None)

    def local(tok, g1, wdq, gq, wuq, wkv, gkv, wukv, wo):
        cos, sin = tables()
        x = tok.reshape(T, D)
        o, w, c, r = front(x, (g1[None], gq[None], gkv[None]), (wdq, wkv, wuq, wukv, wo), cos, sin)
        y, c, r = outp(o, w, x, c, r)
        return y.reshape(tok.shape), c.reshape(-1, S, KR), jnp.swapaxes(r, 1, 2)

    return jax.shard_map(local, mesh=mesh, in_specs=(batch, row, mat, row, mat, mat, row, mat, mat),
                         out_specs=(batch,) * 3, check_vma=False)
```

```python
import functools
import numpy as np
import jax
import jax.numpy as jnp
from jax import lax
from jax.experimental import pallas as pl
from jax.experimental.pallas import tpu as pltpu
from jax.sharding import PartitionSpec as P

F32, BF16 = jnp.float32, jnp.bfloat16
MESH = pl.DeviceIdType.MESH
EPS = 1e-6
T, D, QR, KR, RD, H, ND, VD = 2048, 2560, 768, 256, 32, 40, 64, 64
S = 128
SC = (ND + RD) ** -0.5 * 1.4426950408889634
HG, TC = 8, 512
NCH = T // TC
STEPS = (H // HG) * NCH
TA = 256


def dot(a, b):
    return jnp.dot(a, b, preferred_element_type=F32)


def rms(v):
    return lax.rsqrt(jnp.mean(v * v, axis=-1, keepdims=True) + EPS)


def attn_unit(k, qT, vT, keep):
    s = dot(k, qT) * SC
    s = jnp.where(keep, s, -1e30)
    m = jnp.max(s, axis=0, keepdims=True)
    e = jnp.exp2(s - m)
    p = (e * (1.0 / jnp.sum(e, axis=0, keepdims=True))).astype(BF16)
    return dot(vT, p)


PIECES = (
    ('dq', 'dq', False, 320, 0, 768, 112),
    ('dkv', 'dkv', False, 320, 0, 288, 128),
    ('uq0', 'uq', False, 96, 0, 1536, 32),
    ('ukv0', 'ukv', True, 32, 0, 2048, 768),
    ('uq1', 'uq', False, 96, 1536, 1536, 32),
    ('ukv1', 'ukv', True, 32, 2048, 2048, 768),
    ('uq2', 'uq', False, 96, 3072, 768, 16),
    ('ukv2', 'ukv', True, 32, 4096, 1024, 256),
    ('o0', 'o', False, 320, 0, 512, 128),
    ('o1', 'o', False, 320, 512, 512, 128),
    ('o2', 'o', False, 320, 1024, 512, 96),
    ('o3', 'o', False, 320, 1536, 512, 80),
    ('o4', 'o', False, 320, 2048, 512, 64),
)
PIDX = {p[0]: i for i, p in enumerate(PIECES)}
SPLIT = ('S1a', 'S1b', 'S2a', 'S2b', 'S3a', 'S3b')
KINDS = ('XE', 'YE', 'XS', 'YS', 'S0', 'Z1', 'Z2', 'DY', 'DX', 'Z3', 'S1', 'S2', 'S3') + SPLIT
RSEM = {'XE': 0, 'YE': 0, 'XS': 1, 'YS': 1, 'Z1': 2, 'Z2': 3, 'DY': 4, 'DX': 5, 'Z3': 5, 'S0': 6, 'S1': 6, 'S2': 6, 'S3': 6}
RSEM_SPLIT = dict(RSEM, Z3=7, S1a=8, S1b=8, S2a=9, S2b=9, S3a=10, S3b=10)
SPLIT_ARRS = ('dq', 'dkv')
GROUPS = {'K': ('dkv',), 'D': ('dq',), 'U0': ('uq0', 'ukv0'), 'U1': ('uq1', 'ukv1'), 'U2': ('uq2', 'ukv2'),
          'O0': ('o0',), 'O1': ('o1',), 'O2': ('o2',), 'O3': ('o3',), 'O4': ('o4',)}
STAGES = {
    'st0': ((), ('XE', 'YE', 'XS', 'YS', 'S0')),
    'st1': (('XYE',), ('Z1', 'Z2', 'DY')),
    'st2': (('XYS',), ('DX',)),
    'st4x': (('Z1',), ('S1',)),
    'st3': (('DY',), ('Z3',)),
    'st4y': (('Z2',), ('S2',)),
    'st5': (('DXZ',), ('S3',)),
    'fin': (('SS',), ()),
    'st2d': (('XYS',), ('DX', 'S1a', 'S2a')),
    'st4xd': (('Z1',), ('S1b',)),
    'st4yd': (('Z2',), ('S2b',)),
    'st5a': (('DX',), ('S3a',)),
    'st5b': (('Z3',), ('S3b',)),
    'find': ((), ()),
}
SCHED = {
    'stats0': (('st0', 'K'), ('st0', 'D')),
    'norm1': (('st1', 'K'),),
    'norm2': (('st2d', 'K'),),
    'part0': (('recv', 'K', 'S0'), ('recv', 'D', 'S0')),
    'part2': (('st4xd', 'K'), ('st1', 'D')),
    'k0': (('st0', 'U0'), ('recv', 'K', 'S1a+S1b')),
    'k1': (('st2d', 'D'),),
    'k2': (('st3', 'K'), ('st4yd', 'K'), ('st5a', 'K'), ('recv', 'K', 'S2a+S2b'), ('st4xd', 'D')),
    'k4': (('st3', 'D'), ('st5b', 'K'), ('st4yd', 'D'), ('st1', 'U0'), ('recv', 'K', 'S3a+S3b'), ('st0', 'U1')),
    'k5': (('st2', 'U0'),),
    'q0': (('st5a', 'D'), ('recv', 'D', 'S1a+S1b')),
    'q1': (('st5b', 'D'),),
    'q4': (('st4x', 'U0'), ('st3', 'U0'), ('recv', 'D', 'S2a+S2b')),
    'q5': (('st1', 'U1'),),
    'q7': (('st4y', 'U0'), ('st0', 'U2')),
    'd0': (('st2', 'U1'), ('recv', 'D', 'S3a+S3b')),
    'd2': (('st5', 'U0'), ('st0', 'O0'), ('st0', 'O1')),
    'd4': (('fin', 'U0'), ('st1', 'U2')),
    's0': (('st4x', 'U1'), ('st3', 'U1')),
    's1': (('st4y', 'U1'), ('st2', 'U2')),
    's2': (('st4x', 'U2'), ('st1', 'O0'), ('st0', 'O2')),
    's3': (('st5', 'U1'), ('st2', 'O0')),
    's4': (('st1', 'O1'), ('fin', 'U1')),
    's5': (('st3', 'U2'), ('st4y', 'U2'), ('st4x', 'O0'), ('st2', 'O1')),
    's6': (('st3', 'O0'), ('st4y', 'O0')),
    's7': (('st4x', 'O1'), ('st1', 'O2')),
    's8': (('st2', 'O2'),),
    's9': (('st5', 'U2'), ('st3', 'O1'), ('st4y', 'O1'), ('st0', 'O3'), ('st0', 'O4')),
    's10': (('fin', 'U2'), ('st5', 'O0')),
    's11': (('fin', 'O0'), ('st4x', 'O2'), ('st3', 'O2'), ('st1', 'O3')),
    's12': (('st4y', 'O2'),),
    's13': (('st5', 'O1'), ('st2', 'O3')),
    's14': (('fin', 'O1'), ('st5', 'O2'), ('st1', 'O4')),
    's15': (('fin', 'O2'), ('st4x', 'O3')),
    's16': (('st3', 'O3'), ('st4y', 'O3'), ('st2', 'O4')),
    's17': (('st4x', 'O4'), ('st3', 'O4'), ('st4y', 'O4')),
    's18': (('st5', 'O3'),),
    's19': (('fin', 'O3'), ('st5', 'O4')),
    'end': (('fin', 'O4'),),
    'stats1': (),
}
SWAPPED = ('dq', 'uq0', 'ukv0', 'uq1', 'ukv1', 'uq2', 'ukv2', 'o0', 'o1')


def front_kernel(x_hbm, g1_s, gq_s, gkv_s, dq_s, dkv_s, uq_s, ukv_s, o_s, cos_ref, sin_ref, cosT_ref, sinT_ref,
                 attn_hbm, wo_hbm, c_hbm, r_hbm,
                 xa, wdq, wdkv, wuq, wukv, ostage, g1b, gqb, gkvb, accq, acck, inv, cqT, cbuf, cT, rbuf, rT,
                 wqT, wk, wvT, qT, kbuf, vT, obuf,
                 ssem, rsem, dsem, lsem, gss, grs, xsem, osem, csem):
    z, f = lax.axis_index('dp'), lax.axis_index('fsdp')
    core, xx, yy = f % 2, (f // 2) % 2, f // 4

    def idx(dx, dy, dc):
        return ((yy + dy) % 2) * 4 + ((xx + dx) % 2) * 2 + (core + dc) % 2

    fx, fy, fd = idx(1, 0, 0), idx(0, 1, 0), idx(1, 1, 0)
    dev = {'X': (z, fx), 'Y': (z, fy), 'Z': (1 - z, f), 'S': (z, idx(0, 0, 1))}
    plane = [idx(dx, dy, dc) for dx in range(2) for dy in range(2) for dc in range(2) if dx + dy + dc]
    src = {'dq': dq_s, 'dkv': dkv_s, 'uq': uq_s, 'ukv': ukv_s, 'o': ostage}
    buf = {'dq': wdq, 'dkv': wdkv, 'uq': wuq, 'ukv': wukv, 'o': wo_hbm}

    def region(piece, shard, part, base):
        name, arr, bycol, rows, c0, nc, e = piece
        n = nc if bycol else rows
        off, size = {'E': (z * (n - e), e), 'S': (e, n - 2 * e), 'A': (0, n), 'B': (z * e, n - e), 'M': ((1 - z) * (n - e), e)}[part]
        if bycol:
            row = shard * rows if base else 0
            return pl.ds(pl.multiple_of(row, 16), rows), pl.ds(pl.multiple_of(c0 + off, 128), size)
        row = (shard * rows if base else 0) + off
        return pl.ds(pl.multiple_of(row, 16), size), pl.ds(c0, nc)

    def copy(name, kind):
        piece = PIECES[PIDX[name]]
        arr = piece[1]
        shard = {'X': f, 'Y': f}.get(kind[0]) if kind in ('XE', 'YE', 'XS', 'YS') else None
        if kind in ('XE', 'YE', 'XS', 'YS', 'S0'):
            part = 'A' if kind == 'S0' else kind[1]
            r0, c0 = region(piece, f, part, False)
            r1, c1 = region(piece, f, part, True)
            s_ref, d_ref = src[arr].at[r0, c0], buf[arr].at[r1, c1]
            to = dev[kind[0]]
        else:
            shard, part, to = {'Z1': (fx, 'E', 'Z'), 'Z2': (fy, 'E', 'Z'), 'Z3': (fd, 'E', 'Z'), 'DY': (fx, 'E', 'Y'),
                               'DX': (fy, 'S', 'X'), 'S1': (fx, 'A', 'S'), 'S2': (fy, 'A', 'S'), 'S3': (fd, 'A', 'S'),
                               'S1a': (fx, 'B', 'S'), 'S1b': (fx, 'M', 'S'), 'S2a': (fy, 'B', 'S'), 'S2b': (fy, 'M', 'S'),
                               'S3a': (fd, 'B', 'S'), 'S3b': (fd, 'M', 'S')}[kind]
            if name in SWAPPED and kind in ('DX', 'DY'):
                shard, to = {'DX': (fx, 'Y'), 'DY': (fy, 'X')}[kind]
            to = dev[to]
            r1, c1 = region(piece, shard, part, True)
            s_ref = d_ref = buf[arr].at[r1, c1]
        return pltpu.make_async_remote_copy(src_ref=s_ref, dst_ref=d_ref, send_sem=ssem.at[PIDX[name]], recv_sem=rsem_of(name, kind),
                                            device_id=to, device_id_type=MESH)

    def rsem_of(name, kind):
        if PIECES[PIDX[name]][1] in SPLIT_ARRS:
            return dsem.at[PIDX[name], RSEM_SPLIT[kind]]
        return rsem.at[PIDX[name] - 2, RSEM[kind]]

    def take(name, n, sem, rows_too=True):
        _, arr, bycol, rows, c0, nc, e = PIECES[PIDX[name]]
        ref = buf[arr]
        if bycol:
            k = max(1, -(-n // nc))
            assert n % k == 0
            part = ref.at[pl.ds(0, rows * k), pl.ds(c0, n // k)]
        else:
            part = ref.at[pl.ds(0, n), pl.ds(c0, nc)]
        pltpu.make_async_copy(part, part, sem).wait()

    def units(name, what):
        _, arr, bycol, rows, c0, nc, e = PIECES[PIDX[name]]
        n = nc if bycol else rows
        return {'XYE': 2 * e, 'XYS': 2 * (n - 2 * e), 'Z1': e, 'Z2': e, 'DY': e, 'DX': n - 2 * e, 'Z3': e, 'DXZ': n - e, 'SS': 4 * n,
                'S0': n, 'S1': n, 'S2': n, 'S3': n, 'sent': 7 * n}[what]

    FIRST = {'XYE': 'XE', 'XYS': 'XS', 'DXZ': 'DX', 'SS': 'S0'}

    def local(name):
        piece = PIECES[PIDX[name]]
        r0, c0 = region(piece, f, 'A', False)
        r1, c1 = region(piece, f, 'A', True)
        return pltpu.make_async_copy(src[piece[1]].at[r0, c0], buf[piece[1]].at[r1, c1], lsem.at[PIDX[name]])

    def start(names, *kinds):
        for k in kinds:
            for n in names:
                copy(n, k).start()

    def recv(names, *kinds):
        for k in kinds:
            for n in names:
                k = {'S1a+S1b': 'S1', 'S2a+S2b': 'S2', 'S3a+S3b': 'S3'}.get(k, k)
                first = k + 'a' if k in ('S1', 'S2', 'S3') else FIRST.get(k, k)
                take(n, units(n, k), rsem_of(n, first))

    def comm(todo):
        for op in todo:
            stage, piece = op[0], op[1]
            names = GROUPS[piece]
            if stage == 'recv':
                recv(names, op[2])
                continue
            if stage == 'st0' and piece == 'O0':
                stage_o.wait()
            waits, starts = STAGES[stage]
            recv(names, *waits)
            start(names, *starts)
            if stage == 'st0':
                for n in names:
                    local(n).start()
            if stage in ('fin', 'find'):
                for n in names:
                    if piece not in ('K', 'D'):
                        local(n).wait()

    def at(seg, i):
        marks = sorted((int(n[len(seg):]), n) for n in SCHED if n.startswith(seg) and n[len(seg):].isdigit() and SCHED[n])

        def tree(ms):
            if len(ms) == 1:
                @pl.when(i == ms[0][0])
                def _():
                    with jax.named_scope('comm_' + ms[0][1]):
                        comm(SCHED[ms[0][1]])
            elif ms:
                h = len(ms) // 2
                lax.cond(i < ms[h][0], lambda: tree(ms[:h]), lambda: tree(ms[h:]))
        tree(marks)

    for i in range(T // TA):
        pltpu.make_async_copy(x_hbm.at[pl.ds(i * TA, TA)], xa.at[pl.ds(i * TA, TA)], xsem.at[i]).start()
    stage_o = pltpu.make_async_copy(o_s, ostage, osem.at[2])
    stage_o.start()

    def stat_tile(i, _):
        pltpu.make_async_copy(x_hbm.at[pl.ds(i * TA, TA)], xa.at[pl.ds(i * TA, TA)], xsem.at[i]).wait()
        for h in range(TA // 64):
            rows = pl.ds(pl.multiple_of(i * TA + h * 64, 64), 64)
            inv[rows, :] = jnp.broadcast_to(rms(xa[rows, :].astype(F32)), (64, 128))
        return 0

    barrier = pltpu.get_barrier_semaphore()
    for p in plane:
        pl.semaphore_signal(barrier, inc=1, device_id=(z, p), device_id_type=MESH)
    pl.semaphore_signal(barrier, inc=1, device_id=dev['Z'], device_id_type=MESH)
    with jax.named_scope('barrier'):
        pl.semaphore_wait(barrier, 8)

    for j, (gs, gb) in enumerate(((g1_s, g1b), (gq_s, gqb), (gkv_s, gkvb))):
        for p in plane:
            pltpu.make_async_remote_copy(src_ref=gs, dst_ref=gb.at[f], send_sem=gss.at[j], recv_sem=grs.at[j],
                                         device_id=(z, p), device_id_type=MESH).start()
        pltpu.make_async_copy(gs, gb.at[f], grs.at[j]).start()
    comm(SCHED['stats0'])

    with jax.named_scope('stats_b'):
        lax.fori_loop(0, T // TA, stat_tile, 0)
    comm(SCHED['stats1'])
    with jax.named_scope('gains'):
        for j, gb in enumerate((g1b, gqb, gkvb)):
            pltpu.make_async_copy(gb, gb, grs.at[j]).wait()

    def row_of(gb):
        return jnp.concatenate([gb[i].astype(F32) for i in range(8)], axis=-1)

    g1, gq, gkv = row_of(g1b), row_of(gqb), row_of(gkvb)

    def norm_tile(i, _):
        pl.when(i % 2 == 0)(functools.partial(at, 'norm', i // 2))
        for h in range(TA // 64):
            rows = pl.ds(pl.multiple_of(i * TA + h * 64, 64), 64)
            scale = inv[rows, :]
            for j in range(D // 128):
                cols = slice(128 * j, 128 * j + 128)
                xa[rows, cols] = (xa[rows, cols].astype(F32) * scale * g1[:, cols]).astype(BF16)
        return 0

    def quarter_cols(dy, dx):
        quarter = ((yy + dy) % 2) * 2 + (xx + dx) % 2
        return pl.ds(pl.multiple_of(quarter * 640, 128), 640)

    def own_part(i, _):
        at('part', i)
        cols, rows = quarter_cols(0, 0), pl.ds(pl.multiple_of(i * 512, 512), 512)
        a = xa[rows, cols]
        accq[rows, :] = dot(a, wdq[cols, :])
        acck[rows, :] = dot(a, wdkv[cols, :])
        return 0

    def kv_part(i, _):
        at('k', i)
        q = i // 2 + 1
        cols, rows = quarter_cols(q // 2, q % 2), pl.ds(pl.multiple_of((i % 2) * 1024, 1024), 1024)
        acck[rows, :] += dot(xa[rows, cols], wdkv[cols, :])
        return 0

    def q_part(x_not_y, i, _):
        at('q', i if x_not_y else i + 4)
        if x_not_y:
            finish_kv(2 * i)
            finish_kv(2 * i + 1)
        cols, rows = quarter_cols(0, 1) if x_not_y else quarter_cols(1, 0), pl.ds(pl.multiple_of(i * 512, 512), 512)
        accq[rows, :] += dot(xa[rows, cols], wdq[cols, :])
        return 0

    cos2 = jnp.concatenate([cos_ref[...]] * (TA // S), axis=0)
    sin2 = jnp.concatenate([sin_ref[...]] * (TA // S), axis=0)

    def finish_kv(i):
        rows = pl.ds(pl.multiple_of(i * TA, TA), TA)
        kd = acck[rows, :]
        kc = kd[:, :KR]
        c = (kc * rms(kc) * gkv).astype(BF16)
        cbuf[rows, :] = c
        cT[:, rows] = c.T
        lo, hi = kd[:, KR:KR + 16], kd[:, KR + 16:]
        r = jnp.concatenate([lo * cos2 - hi * sin2, hi * cos2 + lo * sin2], axis=-1).astype(BF16)
        rbuf[rows, :] = r
        for h in range(TA // S):
            rT[i * (TA // S) + h] = r[h * S:h * S + S].T

    def finish_q(i):
        rows = pl.ds(pl.multiple_of(i * TA, TA), TA)
        qd = accq[rows, :]
        cqT[:, rows] = (qd * rms(qd) * gq).astype(BF16).T

    def last_part():
        cols = pl.ds(pl.multiple_of((fd // 2) * 640, 128), 640)

        def tile(i, _):
            pl.when(i % 2 == 0)(functools.partial(at, 'd', i // 2))
            finish_q(jnp.maximum(i - 1, 0))
            rows = pl.ds(pl.multiple_of(jnp.minimum(i, T // TA - 1) * TA, TA), TA)
            accq[rows, :] += dot(xa[rows, cols], wdq[cols, :])
            return 0
        lax.fori_loop(0, T // TA + 1, tile, 0)

    with jax.named_scope('norm'):
        lax.fori_loop(0, T // TA, norm_tile, 0)
    for n in ('dq', 'dkv'):
        local(n).wait()
    with jax.named_scope('own'):
        lax.fori_loop(0, 4, own_part, 0)
    with jax.named_scope('kv'):
        lax.fori_loop(0, 6, kv_part, 0)
    with jax.named_scope('qx'):
        lax.fori_loop(0, 4, functools.partial(q_part, True), 0)
    with jax.named_scope('qy'):
        lax.fori_loop(0, 4, functools.partial(q_part, False), 0)
    with jax.named_scope('last'):
        last_part()
    outs = [pltpu.make_async_copy(cbuf, c_hbm, csem.at[0]), pltpu.make_async_copy(rT, r_hbm, csem.at[1])]
    for o in outs:
        o.start()

    keep = lax.broadcasted_iota(jnp.int32, (S, S), 0) <= lax.broadcasted_iota(jnp.int32, (S, S), 1)
    lane = lax.broadcasted_iota(jnp.int32, (S, 128), 1)
    co, si = cosT_ref[...], sinT_ref[...]
    for h in range(HG):
        zr = 128 * h + (96 if h % 2 == 0 else 32)
        qT[zr:zr + 32, :] = jnp.zeros((32, TC), BF16)

    def prepare(g, k, slot):
        col = 256 * jnp.minimum(k, 2)
        wqT[slot, pl.ds(pl.multiple_of(col, 256), 256), :] = wuq[:, pl.ds(pl.multiple_of(g * (HG * 96) + col, 128), 256)].T
        t0 = wukv[:, pl.ds(pl.multiple_of(g * (HG * 128) + 256 * k, 128), 128)]
        t1 = wukv[:, pl.ds(pl.multiple_of(g * (HG * 128) + 256 * k + 128, 128), 128)]
        lanes = pl.ds(pl.multiple_of(128 * k, 128), 128)
        wk[slot, :, lanes] = jnp.concatenate([t0[:, :64], t1[:, :64]], axis=1)
        wvT[slot, lanes, :] = jnp.concatenate([t0[:, 64:], t1[:, 64:]], axis=1).T

    def out_copy(i):
        g, tc = i // NCH, i % NCH
        return pltpu.make_async_copy(obuf.at[i % 2], attn_hbm.at[pl.ds(pl.multiple_of(tc * TC, TC), TC), pl.ds(pl.multiple_of(g * (HG * 64), 128), HG * 64)], osem.at[i % 2])

    def step(i, _):
        g, tc = i // NCH, i % NCH
        tok = pl.multiple_of(tc * TC, TC)
        at('s', i)

        @pl.when(i == 0)
        def _():
            with jax.named_scope('prepare'):
                for k in range(4):
                    prepare(0, k, 0)

        here = g % 2
        @pl.when(i >= 2)
        def _():
            out_copy(i - 2).wait()

        slot = i % 2
        for n in range(TC // 256):
            q = dot(wqT[here], cqT[:, pl.ds(tok + 256 * n, 256)])
            cols = slice(256 * n, 256 * n + 256)
            for h in range(HG):
                nope = q[96 * h:96 * h + 64]
                lo, hi = q[96 * h + 64:96 * h + 80], q[96 * h + 80:96 * h + 96]
                b = 128 * h
                qn, qp = (b, b + 64) if h % 2 == 0 else (b + 64, b)
                qT[qn:qn + 64, cols] = nope.astype(BF16)
                qT[qp:qp + 16, cols] = (lo * co - hi * si).astype(BF16)
                qT[qp + 16:qp + 32, cols] = (hi * co + lo * si).astype(BF16)
        kbuf[...] = dot(cbuf[pl.ds(tok, TC), :], wk[here]).astype(BF16)
        vT[...] = dot(wvT[here], cT[:, pl.ds(tok, TC)]).astype(BF16)
        prepare(jnp.minimum(g + 1, H // HG - 1), tc, 1 - here)

        for p in range(TC // S):
            row = p * S
            r = rbuf[pl.ds(tok + row, S), :]
            z32, z64 = jnp.zeros((S, 32), BF16), jnp.zeros((S, 64), BF16)
            r_hi = jnp.concatenate([z64, r, z32], axis=1)
            r_lo = jnp.concatenate([r, z32, z64], axis=1)
            for j in range(HG // 2):
                k2 = kbuf[row:row + S, 128 * j:128 * j + 128]
                both = []
                for par in range(2):
                    h = 2 * j + par
                    k = jnp.where(lane < 64, k2, r_hi) if par == 0 else jnp.where(lane < 64, r_lo, k2)
                    both.append(attn_unit(k, qT[128 * h:128 * h + 128, row:row + S], vT[64 * h:64 * h + 64, row:row + S], keep))
                obuf[slot, row:row + S, 128 * j:128 * j + 128] = jnp.concatenate(both, axis=0).astype(BF16).T
        out_copy(i).start()
        return 0

    lax.fori_loop(0, STEPS, step, 0)
    with jax.named_scope('fin_O'):
        comm(SCHED['end'])
    with jax.named_scope('tail_out'):
        for i in (STEPS - 2, STEPS - 1):
            out_copy(i).wait()
        for o in outs:
            o.wait()
    with jax.named_scope('tail_sends'):
        for j, gb in enumerate((g1b, gqb, gkvb)):
            pltpu.make_async_copy(gb.at[pl.ds(0, 7)], gb.at[pl.ds(0, 7)], gss.at[j]).wait()
        for p in PIECES:
            take(p[0], units(p[0], 'sent'), ssem.at[PIDX[p[0]]])


def front(x, gains, ws, cos, sin):
    anyspace, vm = pl.BlockSpec(memory_space=pl.ANY), pl.BlockSpec(memory_space=pltpu.VMEM)
    V = pltpu.VMEM
    dma = pltpu.SemaphoreType.DMA
    tab = [cos, sin, np.tile(cos.T, (1, 2)), np.tile(sin.T, (1, 2))]
    return pl.pallas_call(
        front_kernel, name='front',
        in_specs=[anyspace] + [vm] * 3 + [anyspace] * 5 + [vm] * 4,
        out_specs=[anyspace] * 4,
        out_shape=[jax.ShapeDtypeStruct((T, H * VD), BF16), jax.ShapeDtypeStruct((H * VD, D), BF16), jax.ShapeDtypeStruct((T, KR), BF16), jax.ShapeDtypeStruct((T // S, RD, S), BF16)],
        scratch_shapes=[
            V((T, D), BF16), V((D, QR), BF16), V((D, KR + RD), BF16), V((QR, H * 96), BF16), V((KR, H * 128), BF16), V((320, D), BF16),
            V((8, 1, 320), BF16), V((8, 1, 96), BF16), V((8, 1, 32), BF16), V((T, QR), F32), V((T, KR + RD), F32), V((T, 128), F32),
            V((QR, T), BF16), V((T, KR), BF16), V((KR, T), BF16), V((T, RD), BF16), V((T // S, RD, S), BF16),
            V((2, HG * 96, QR), BF16), V((2, KR, HG * 64), BF16), V((2, HG * 64, KR), BF16), V((HG * 128, TC), BF16), V((TC, HG * 64), BF16), V((HG * 64, TC), BF16), V((2, TC, HG * 64), BF16),
            dma((len(PIECES),)), dma((len(PIECES) - 2, 7)), dma((2, 11)), dma((len(PIECES),)), dma((3,)), dma((3,)), dma((T // TA,)), dma((3,)), dma((2,)),
        ],
        compiler_params=pltpu.CompilerParams(collective_id=0, has_side_effects=True, vmem_limit_bytes=63 << 20),
    )(x, *gains, *ws, *(jnp.asarray(t) for t in tab))


def out_kernel(o_ref, w_ref, x_ref, c_ref, r_ref, y_ref, c_out, r_out):
    for n in range(0, y_ref.shape[1], 256):
        cols = slice(n, n + 256)
        y_ref[:, cols] = (x_ref[:, cols].astype(F32) + dot(o_ref[...], w_ref[:, cols])).astype(BF16)
    c_out[...] = c_ref[...]
    r_out[...] = r_ref[...]


def outp(o, w, x, c, r, tm=1024, tn=1280):
    nt = D // tn
    cr = T // ((T // tm) * nt)
    step = lambda j, i: j * (T // tm) + i
    return pl.pallas_call(
        out_kernel, grid=(nt, T // tm), name='outp',
        in_specs=[pl.BlockSpec((tm, D), lambda j, i: (i, 0)), pl.BlockSpec((D, tn), lambda j, i: (0, j)), pl.BlockSpec((tm, tn), lambda j, i: (i, j)),
                  pl.BlockSpec((cr, KR), lambda j, i: (step(j, i), 0)), pl.BlockSpec((cr // S, RD, S), lambda j, i: (step(j, i), 0, 0))],
        out_specs=[pl.BlockSpec((tm, tn), lambda j, i: (i, j)), pl.BlockSpec((cr, KR), lambda j, i: (step(j, i), 0)), pl.BlockSpec((cr // S, RD, S), lambda j, i: (step(j, i), 0, 0))],
        out_shape=[jax.ShapeDtypeStruct((T, D), BF16), jax.ShapeDtypeStruct((T, KR), BF16), jax.ShapeDtypeStruct((T // S, RD, S), BF16)],
        compiler_params=pltpu.CompilerParams(vmem_limit_bytes=62 << 20),
    )(o, w, x, c, r)


def tables():
    half = RD // 2
    freq = np.float32(10000.0) ** (np.float32(-2.0) * np.arange(half, dtype=np.float32) / np.float32(RD))
    ang = np.arange(S, dtype=np.float32)[:, None] * freq[None, :].astype(np.float32)
    return np.cos(ang).astype(np.float32), np.sin(ang).astype(np.float32)


def solution(mesh):
    batch, row, mat = P(('dp', 'fsdp')), P('fsdp'), P('fsdp', None)

    def local(tok, g1, wdq, gq, wuq, wkv, gkv, wukv, wo):
        cos, sin = tables()
        x = tok.reshape(T, D)
        o, w, c, r = front(x, (g1[None], gq[None], gkv[None]), (wdq, wkv, wuq, wukv, wo), cos, sin)
        y, c, r = outp(o, w, x, c, r)
        return y.reshape(tok.shape), c.reshape(-1, S, KR), jnp.swapaxes(r, 1, 2)

    return jax.shard_map(local, mesh=mesh, in_specs=(batch, row, mat, row, mat, mat, row, mat, mat),
                         out_specs=(batch,) * 3, check_vma=False)
```

```python
import functools
import numpy as np
import jax
import jax.numpy as jnp
from jax import lax
from jax.experimental import pallas as pl
from jax.experimental.pallas import tpu as pltpu
from jax.sharding import PartitionSpec as P

F32, BF16 = jnp.float32, jnp.bfloat16
MESH = pl.DeviceIdType.MESH
EPS = 1e-6
T, D, QR, KR, RD, H, ND, VD = 2048, 2560, 768, 256, 32, 40, 64, 64
S = 128
SC = (ND + RD) ** -0.5 * 1.4426950408889634
HG, TC = 8, 512
NCH = T // TC
STEPS = (H // HG) * NCH
TA = 256


def dot(a, b):
    return jnp.dot(a, b, preferred_element_type=F32)


def rms(v):
    return lax.rsqrt(jnp.mean(v * v, axis=-1, keepdims=True) + EPS)


def attn_unit(k, qT, vT, keep):
    s = dot(k, qT) * SC
    s = jnp.where(keep, s, -1e30)
    m = jnp.max(s, axis=0, keepdims=True)
    e = jnp.exp2(s - m)
    p = (e * (1.0 / jnp.sum(e, axis=0, keepdims=True))).astype(BF16)
    return dot(vT, p)


PIECES = (
    ('dq', 'dq', False, 320, 0, 768, 112),
    ('dkv', 'dkv', False, 320, 0, 288, 128),
    ('uq0', 'uq', False, 96, 0, 1536, 32),
    ('ukv0', 'ukv', True, 32, 0, 2048, 768),
    ('uq1', 'uq', False, 96, 1536, 1536, 32),
    ('ukv1', 'ukv', True, 32, 2048, 2048, 768),
    ('uq2', 'uq', False, 96, 3072, 768, 16),
    ('ukv2', 'ukv', True, 32, 4096, 1024, 256),
    ('o0', 'o', False, 320, 0, 512, 128),
    ('o1', 'o', False, 320, 512, 512, 128),
    ('o2', 'o', False, 320, 1024, 512, 96),
    ('o3', 'o', False, 320, 1536, 512, 80),
    ('o4', 'o', False, 320, 2048, 512, 64),
)
PIDX = {p[0]: i for i, p in enumerate(PIECES)}
SPLIT = ('S1a', 'S1b', 'S2a', 'S2b', 'S3a', 'S3b')
KINDS = ('XE', 'YE', 'XS', 'YS', 'S0', 'Z1', 'Z2', 'DY', 'DX', 'Z3', 'S1', 'S2', 'S3') + SPLIT
RSEM = {'XE': 0, 'YE': 0, 'XS': 1, 'YS': 1, 'Z1': 2, 'Z2': 3, 'DY': 4, 'DX': 5, 'Z3': 5, 'S0': 6, 'S1': 6, 'S2': 6, 'S3': 6}
RSEM_SPLIT = dict(RSEM, Z3=7, S1a=8, S1b=8, S2a=9, S2b=9, S3a=10, S3b=10)
SPLIT_ARRS = ('dq', 'dkv')
GROUPS = {'K': ('dkv',), 'D': ('dq',), 'U0': ('uq0', 'ukv0'), 'U1': ('uq1', 'ukv1'), 'U2': ('uq2', 'ukv2'),
          'O0': ('o0',), 'O1': ('o1',), 'O2': ('o2',), 'O3': ('o3',), 'O4': ('o4',)}
STAGES = {
    'st0': ((), ('XE', 'YE', 'XS', 'YS', 'S0')),
    'st1': (('XYE',), ('Z1', 'Z2', 'DY')),
    'st2': (('XYS',), ('DX',)),
    'st4x': (('Z1',), ('S1',)),
    'st3': (('DY',), ('Z3',)),
    'st4y': (('Z2',), ('S2',)),
    'st5': (('DXZ',), ('S3',)),
    'fin': (('SS',), ()),
    'st2d': (('XYS',), ('DX', 'S1a', 'S2a')),
    'st4xd': (('Z1',), ('S1b',)),
    'st4yd': (('Z2',), ('S2b',)),
    'st5a': (('DX',), ('S3a',)),
    'st5b': (('Z3',), ('S3b',)),
    'find': ((), ()),
}
SCHED = {
    'stats0': (('st0', 'K'), ('st0', 'D')),
    'norm1': (('st1', 'K'),),
    'norm2': (('st2d', 'K'),),
    'part0': (('recv', 'K', 'S0'), ('recv', 'D', 'S0')),
    'part2': (('st4xd', 'K'), ('st1', 'D')),
    'k0': (('st0', 'U0'), ('recv', 'K', 'S1a+S1b')),
    'k1': (('st2d', 'D'),),
    'k2': (('st3', 'K'), ('st4yd', 'K'), ('st5a', 'K'), ('recv', 'K', 'S2a+S2b'), ('st4xd', 'D')),
    'k4': (('st3', 'D'), ('st5b', 'K'), ('st4yd', 'D'), ('st1', 'U0'), ('recv', 'K', 'S3a+S3b'), ('st0', 'U1')),
    'k5': (('st2', 'U0'),),
    'q0': (('st5a', 'D'), ('recv', 'D', 'S1a+S1b')),
    'q1': (('st5b', 'D'),),
    'q4': (('st4x', 'U0'), ('st3', 'U0'), ('recv', 'D', 'S2a+S2b')),
    'q5': (('st1', 'U1'),),
    'q7': (('st4y', 'U0'), ('st0', 'U2')),
    'd0': (('st2', 'U1'), ('recv', 'D', 'S3a+S3b')),
    'd2': (('st5', 'U0'), ('st0', 'O0'), ('st0', 'O1')),
    'd4': (('fin', 'U0'), ('st1', 'U2')),
    's0': (('st4x', 'U1'), ('st3', 'U1')),
    's1': (('st4y', 'U1'), ('st2', 'U2')),
    's2': (('st4x', 'U2'), ('st1', 'O0'), ('st0', 'O2')),
    's3': (('st5', 'U1'), ('st2', 'O0')),
    's4': (('st1', 'O1'), ('fin', 'U1')),
    's5': (('st3', 'U2'), ('st4y', 'U2'), ('st4x', 'O0'), ('st2', 'O1')),
    's6': (('st3', 'O0'), ('st4y', 'O0')),
    's7': (('st4x', 'O1'), ('st1', 'O2')),
    's8': (('st2', 'O2'),),
    's9': (('st5', 'U2'), ('st3', 'O1'), ('st4y', 'O1'), ('st0', 'O3'), ('st0', 'O4')),
    's10': (('fin', 'U2'), ('st5', 'O0')),
    's11': (('fin', 'O0'), ('st4x', 'O2'), ('st3', 'O2'), ('st1', 'O3')),
    's12': (('st4y', 'O2'),),
    's13': (('st5', 'O1'), ('st2', 'O3')),
    's14': (('fin', 'O1'), ('st5', 'O2'), ('st1', 'O4')),
    's15': (('fin', 'O2'), ('st4x', 'O3')),
    's16': (('st3', 'O3'), ('st4y', 'O3'), ('st2', 'O4')),
    's17': (('st4x', 'O4'), ('st3', 'O4'), ('st4y', 'O4')),
    's18': (('st5', 'O3'),),
    's19': (('fin', 'O3'), ('st5', 'O4')),
    'end': (('fin', 'O4'),),
    'stats1': (),
}
SWAPPED = ('dq', 'uq0', 'ukv0', 'uq1', 'ukv1', 'uq2', 'ukv2', 'o0', 'o1')


def front_kernel(x_hbm, g1_s, gq_s, gkv_s, dq_s, dkv_t, uq_s, ukv_s, o_s, cos_ref, sin_ref, cosT_ref, sinT_ref,
                 attn_hbm, wo_hbm, c_hbm, r_hbm,
                 xa, wdq, wdkv, wuq, wukv, ostage, g1b, gqb, gkvb, accq, acck, inv, cqT, cbuf, cT, rbuf, rT,
                 wqT, wk, wvT, qT, kbuf, vT, obuf,
                 dkv_in, dkv_s,
                 ssem, rsem, dsem, lsem, gss, grs, xsem, osem, csem):
    z, f = lax.axis_index('dp'), lax.axis_index('fsdp')
    core, xx, yy = f % 2, (f // 2) % 2, f // 4

    def idx(dx, dy, dc):
        return ((yy + dy) % 2) * 4 + ((xx + dx) % 2) * 2 + (core + dc) % 2

    fx, fy, fd = idx(1, 0, 0), idx(0, 1, 0), idx(1, 1, 0)
    dev = {'X': (z, fx), 'Y': (z, fy), 'Z': (1 - z, f), 'S': (z, idx(0, 0, 1))}
    plane = [idx(dx, dy, dc) for dx in range(2) for dy in range(2) for dc in range(2) if dx + dy + dc]
    src = {'dq': dq_s, 'dkv': dkv_s, 'uq': uq_s, 'ukv': ukv_s, 'o': ostage}
    buf = {'dq': wdq, 'dkv': wdkv, 'uq': wuq, 'ukv': wukv, 'o': wo_hbm}

    def region(piece, shard, part, base):
        name, arr, bycol, rows, c0, nc, e = piece
        n = nc if bycol else rows
        off, size = {'E': (z * (n - e), e), 'S': (e, n - 2 * e), 'A': (0, n), 'B': (z * e, n - e), 'M': ((1 - z) * (n - e), e)}[part]
        if bycol:
            row = shard * rows if base else 0
            return pl.ds(pl.multiple_of(row, 16), rows), pl.ds(pl.multiple_of(c0 + off, 128), size)
        row = (shard * rows if base else 0) + off
        return pl.ds(pl.multiple_of(row, 16), size), pl.ds(c0, nc)

    def copy(name, kind):
        piece = PIECES[PIDX[name]]
        arr = piece[1]
        shard = {'X': f, 'Y': f}.get(kind[0]) if kind in ('XE', 'YE', 'XS', 'YS') else None
        if kind in ('XE', 'YE', 'XS', 'YS', 'S0'):
            part = 'A' if kind == 'S0' else kind[1]
            r0, c0 = region(piece, f, part, False)
            r1, c1 = region(piece, f, part, True)
            s_ref, d_ref = src[arr].at[r0, c0], buf[arr].at[r1, c1]
            to = dev[kind[0]]
        else:
            shard, part, to = {'Z1': (fx, 'E', 'Z'), 'Z2': (fy, 'E', 'Z'), 'Z3': (fd, 'E', 'Z'), 'DY': (fx, 'E', 'Y'),
                               'DX': (fy, 'S', 'X'), 'S1': (fx, 'A', 'S'), 'S2': (fy, 'A', 'S'), 'S3': (fd, 'A', 'S'),
                               'S1a': (fx, 'B', 'S'), 'S1b': (fx, 'M', 'S'), 'S2a': (fy, 'B', 'S'), 'S2b': (fy, 'M', 'S'),
                               'S3a': (fd, 'B', 'S'), 'S3b': (fd, 'M', 'S')}[kind]
            if name in SWAPPED and kind in ('DX', 'DY'):
                shard, to = {'DX': (fx, 'Y'), 'DY': (fy, 'X')}[kind]
            to = dev[to]
            r1, c1 = region(piece, shard, part, True)
            s_ref = d_ref = buf[arr].at[r1, c1]
        return pltpu.make_async_remote_copy(src_ref=s_ref, dst_ref=d_ref, send_sem=ssem.at[PIDX[name]], recv_sem=rsem_of(name, kind),
                                            device_id=to, device_id_type=MESH)

    def rsem_of(name, kind):
        if PIECES[PIDX[name]][1] in SPLIT_ARRS:
            return dsem.at[PIDX[name], RSEM_SPLIT[kind]]
        return rsem.at[PIDX[name] - 2, RSEM[kind]]

    def take(name, n, sem, rows_too=True):
        _, arr, bycol, rows, c0, nc, e = PIECES[PIDX[name]]
        ref = buf[arr]
        if bycol:
            k = max(1, -(-n // nc))
            assert n % k == 0
            part = ref.at[pl.ds(0, rows * k), pl.ds(c0, n // k)]
        else:
            part = ref.at[pl.ds(0, n), pl.ds(c0, nc)]
        pltpu.make_async_copy(part, part, sem).wait()

    def units(name, what):
        _, arr, bycol, rows, c0, nc, e = PIECES[PIDX[name]]
        n = nc if bycol else rows
        return {'XYE': 2 * e, 'XYS': 2 * (n - 2 * e), 'Z1': e, 'Z2': e, 'DY': e, 'DX': n - 2 * e, 'Z3': e, 'DXZ': n - e, 'SS': 4 * n,
                'S0': n, 'S1': n, 'S2': n, 'S3': n, 'sent': 7 * n}[what]

    FIRST = {'XYE': 'XE', 'XYS': 'XS', 'DXZ': 'DX', 'SS': 'S0'}

    def local(name):
        piece = PIECES[PIDX[name]]
        r0, c0 = region(piece, f, 'A', False)
        r1, c1 = region(piece, f, 'A', True)
        return pltpu.make_async_copy(src[piece[1]].at[r0, c0], buf[piece[1]].at[r1, c1], lsem.at[PIDX[name]])

    def start(names, *kinds):
        for k in kinds:
            for n in names:
                copy(n, k).start()

    def recv(names, *kinds):
        for k in kinds:
            for n in names:
                k = {'S1a+S1b': 'S1', 'S2a+S2b': 'S2', 'S3a+S3b': 'S3'}.get(k, k)
                first = k + 'a' if k in ('S1', 'S2', 'S3') else FIRST.get(k, k)
                take(n, units(n, k), rsem_of(n, first))

    def comm(todo):
        for op in todo:
            stage, piece = op[0], op[1]
            names = GROUPS[piece]
            if stage == 'recv':
                recv(names, op[2])
                continue
            if stage == 'st0' and piece == 'O0':
                stage_o.wait()
            waits, starts = STAGES[stage]
            recv(names, *waits)
            start(names, *starts)
            if stage == 'st0':
                for n in names:
                    local(n).start()
            if stage in ('fin', 'find'):
                for n in names:
                    if piece not in ('K', 'D'):
                        local(n).wait()

    def at(seg, i):
        marks = sorted((int(n[len(seg):]), n) for n in SCHED if n.startswith(seg) and n[len(seg):].isdigit() and SCHED[n])

        def tree(ms):
            if len(ms) == 1:
                @pl.when(i == ms[0][0])
                def _():
                    with jax.named_scope('comm_' + ms[0][1]):
                        comm(SCHED[ms[0][1]])
            elif ms:
                h = len(ms) // 2
                lax.cond(i < ms[h][0], lambda: tree(ms[:h]), lambda: tree(ms[h:]))
        tree(marks)

    for i in range(T // TA):
        pltpu.make_async_copy(x_hbm.at[pl.ds(i * TA, TA)], xa.at[pl.ds(i * TA, TA)], xsem.at[i]).start()
    stage_o = pltpu.make_async_copy(o_s, ostage, osem.at[2])
    stage_o.start()

    def stat_tile(i, _):
        pltpu.make_async_copy(x_hbm.at[pl.ds(i * TA, TA)], xa.at[pl.ds(i * TA, TA)], xsem.at[i]).wait()
        for h in range(TA // 64):
            rows = pl.ds(pl.multiple_of(i * TA + h * 64, 64), 64)
            inv[rows, :] = jnp.broadcast_to(rms(xa[rows, :].astype(F32)), (64, 128))
        return 0

    turn = pltpu.make_async_copy(dkv_t, dkv_in, csem.at[2])
    turn.start()
    barrier = pltpu.get_barrier_semaphore()
    for p in plane:
        pl.semaphore_signal(barrier, inc=1, device_id=(z, p), device_id_type=MESH)
    pl.semaphore_signal(barrier, inc=1, device_id=dev['Z'], device_id_type=MESH)
    turn.wait()
    dkv_s[...] = dkv_in[...].T
    with jax.named_scope('barrier'):
        pl.semaphore_wait(barrier, 8)

    for j, (gs, gb) in enumerate(((g1_s, g1b), (gq_s, gqb), (gkv_s, gkvb))):
        for p in plane:
            pltpu.make_async_remote_copy(src_ref=gs, dst_ref=gb.at[f], send_sem=gss.at[j], recv_sem=grs.at[j],
                                         device_id=(z, p), device_id_type=MESH).start()
        pltpu.make_async_copy(gs, gb.at[f], grs.at[j]).start()
    comm(SCHED['stats0'])

    with jax.named_scope('stats_b'):
        lax.fori_loop(0, T // TA, stat_tile, 0)
    comm(SCHED['stats1'])
    with jax.named_scope('gains'):
        for j, gb in enumerate((g1b, gqb, gkvb)):
            pltpu.make_async_copy(gb, gb, grs.at[j]).wait()

    def row_of(gb):
        return jnp.concatenate([gb[i].astype(F32) for i in range(8)], axis=-1)

    g1, gq, gkv = row_of(g1b), row_of(gqb), row_of(gkvb)

    def norm_tile(i, _):
        pl.when(i % 2 == 0)(functools.partial(at, 'norm', i // 2))
        for h in range(TA // 64):
            rows = pl.ds(pl.multiple_of(i * TA + h * 64, 64), 64)
            scale = inv[rows, :]
            for j in range(D // 128):
                cols = slice(128 * j, 128 * j + 128)
                xa[rows, cols] = (xa[rows, cols].astype(F32) * scale * g1[:, cols]).astype(BF16)
        return 0

    def quarter_cols(dy, dx):
        quarter = ((yy + dy) % 2) * 2 + (xx + dx) % 2
        return pl.ds(pl.multiple_of(quarter * 640, 128), 640)

    def own_part(i, _):
        at('part', i)
        cols, rows = quarter_cols(0, 0), pl.ds(pl.multiple_of(i * 512, 512), 512)
        a = xa[rows, cols]
        accq[rows, :] = dot(a, wdq[cols, :])
        acck[rows, :] = dot(a, wdkv[cols, :])
        return 0

    def kv_part(i, _):
        at('k', i)
        q = i // 2 + 1
        cols, rows = quarter_cols(q // 2, q % 2), pl.ds(pl.multiple_of((i % 2) * 1024, 1024), 1024)
        acck[rows, :] += dot(xa[rows, cols], wdkv[cols, :])
        return 0

    def q_part(x_not_y, i, _):
        at('q', i if x_not_y else i + 4)
        if x_not_y:
            finish_kv(2 * i)
            finish_kv(2 * i + 1)
        cols, rows = quarter_cols(0, 1) if x_not_y else quarter_cols(1, 0), pl.ds(pl.multiple_of(i * 512, 512), 512)
        accq[rows, :] += dot(xa[rows, cols], wdq[cols, :])
        return 0

    cos2 = jnp.concatenate([cos_ref[...]] * (TA // S), axis=0)
    sin2 = jnp.concatenate([sin_ref[...]] * (TA // S), axis=0)

    def finish_kv(i):
        rows = pl.ds(pl.multiple_of(i * TA, TA), TA)
        kd = acck[rows, :]
        kc = kd[:, :KR]
        c = (kc * rms(kc) * gkv).astype(BF16)
        cbuf[rows, :] = c
        cT[:, rows] = c.T
        lo, hi = kd[:, KR:KR + 16], kd[:, KR + 16:]
        r = jnp.concatenate([lo * cos2 - hi * sin2, hi * cos2 + lo * sin2], axis=-1).astype(BF16)
        rbuf[rows, :] = r
        for h in range(TA // S):
            rT[i * (TA // S) + h] = r[h * S:h * S + S].T

    def finish_q(i):
        rows = pl.ds(pl.multiple_of(i * TA, TA), TA)
        qd = accq[rows, :]
        cqT[:, rows] = (qd * rms(qd) * gq).astype(BF16).T

    def last_part():
        cols = pl.ds(pl.multiple_of((fd // 2) * 640, 128), 640)

        def tile(i, _):
            pl.when(i % 2 == 0)(functools.partial(at, 'd', i // 2))
            finish_q(jnp.maximum(i - 1, 0))
            rows = pl.ds(pl.multiple_of(jnp.minimum(i, T // TA - 1) * TA, TA), TA)
            accq[rows, :] += dot(xa[rows, cols], wdq[cols, :])
            return 0
        lax.fori_loop(0, T // TA + 1, tile, 0)

    with jax.named_scope('norm'):
        lax.fori_loop(0, T // TA, norm_tile, 0)
    for n in ('dq', 'dkv'):
        local(n).wait()
    with jax.named_scope('own'):
        lax.fori_loop(0, 4, own_part, 0)
    with jax.named_scope('kv'):
        lax.fori_loop(0, 6, kv_part, 0)
    with jax.named_scope('qx'):
        lax.fori_loop(0, 4, functools.partial(q_part, True), 0)
    with jax.named_scope('qy'):
        lax.fori_loop(0, 4, functools.partial(q_part, False), 0)
    with jax.named_scope('last'):
        last_part()
    outs = [pltpu.make_async_copy(cbuf, c_hbm, csem.at[0]), pltpu.make_async_copy(rT, r_hbm, csem.at[1])]
    for o in outs:
        o.start()

    keep = lax.broadcasted_iota(jnp.int32, (S, S), 0) <= lax.broadcasted_iota(jnp.int32, (S, S), 1)
    lane = lax.broadcasted_iota(jnp.int32, (S, 128), 1)
    co, si = cosT_ref[...], sinT_ref[...]
    for h in range(HG):
        zr = 128 * h + (96 if h % 2 == 0 else 32)
        qT[zr:zr + 32, :] = jnp.zeros((32, TC), BF16)

    def prepare(g, k, slot):
        col = 256 * jnp.minimum(k, 2)
        wqT[slot, pl.ds(pl.multiple_of(col, 256), 256), :] = wuq[:, pl.ds(pl.multiple_of(g * (HG * 96) + col, 128), 256)].T
        t0 = wukv[:, pl.ds(pl.multiple_of(g * (HG * 128) + 256 * k, 128), 128)]
        t1 = wukv[:, pl.ds(pl.multiple_of(g * (HG * 128) + 256 * k + 128, 128), 128)]
        lanes = pl.ds(pl.multiple_of(128 * k, 128), 128)
        wk[slot, :, lanes] = jnp.concatenate([t0[:, :64], t1[:, :64]], axis=1)
        wvT[slot, lanes, :] = jnp.concatenate([t0[:, 64:], t1[:, 64:]], axis=1).T

    def out_copy(i):
        g, tc = i // NCH, i % NCH
        return pltpu.make_async_copy(obuf.at[i % 2], attn_hbm.at[pl.ds(pl.multiple_of(tc * TC, TC), TC), pl.ds(pl.multiple_of(g * (HG * 64), 128), HG * 64)], osem.at[i % 2])

    def step(i, _):
        g, tc = i // NCH, i % NCH
        tok = pl.multiple_of(tc * TC, TC)
        at('s', i)

        @pl.when(i == 0)
        def _():
            with jax.named_scope('prepare'):
                for k in range(4):
                    prepare(0, k, 0)

        here = g % 2
        @pl.when(i >= 2)
        def _():
            out_copy(i - 2).wait()

        slot = i % 2
        for n in range(TC // 256):
            q = dot(wqT[here], cqT[:, pl.ds(tok + 256 * n, 256)])
            cols = slice(256 * n, 256 * n + 256)
            for h in range(HG):
                nope = q[96 * h:96 * h + 64]
                lo, hi = q[96 * h + 64:96 * h + 80], q[96 * h + 80:96 * h + 96]
                b = 128 * h
                qn, qp = (b, b + 64) if h % 2 == 0 else (b + 64, b)
                qT[qn:qn + 64, cols] = nope.astype(BF16)
                qT[qp:qp + 16, cols] = (lo * co - hi * si).astype(BF16)
                qT[qp + 16:qp + 32, cols] = (hi * co + lo * si).astype(BF16)
        kbuf[...] = dot(cbuf[pl.ds(tok, TC), :], wk[here]).astype(BF16)
        vT[...] = dot(wvT[here], cT[:, pl.ds(tok, TC)]).astype(BF16)
        prepare(jnp.minimum(g + 1, H // HG - 1), tc, 1 - here)

        for p in range(TC // S):
            row = p * S
            r = rbuf[pl.ds(tok + row, S), :]
            z32, z64 = jnp.zeros((S, 32), BF16), jnp.zeros((S, 64), BF16)
            r_hi = jnp.concatenate([z64, r, z32], axis=1)
            r_lo = jnp.concatenate([r, z32, z64], axis=1)
            for j in range(HG // 2):
                k2 = kbuf[row:row + S, 128 * j:128 * j + 128]
                both = []
                for par in range(2):
                    h = 2 * j + par
                    k = jnp.where(lane < 64, k2, r_hi) if par == 0 else jnp.where(lane < 64, r_lo, k2)
                    both.append(attn_unit(k, qT[128 * h:128 * h + 128, row:row + S], vT[64 * h:64 * h + 64, row:row + S], keep))
                obuf[slot, row:row + S, 128 * j:128 * j + 128] = jnp.concatenate(both, axis=0).astype(BF16).T
        out_copy(i).start()
        return 0

    lax.fori_loop(0, STEPS, step, 0)
    with jax.named_scope('fin_O'):
        comm(SCHED['end'])
    with jax.named_scope('tail_out'):
        for i in (STEPS - 2, STEPS - 1):
            out_copy(i).wait()
        for o in outs:
            o.wait()
    with jax.named_scope('tail_sends'):
        for j, gb in enumerate((g1b, gqb, gkvb)):
            pltpu.make_async_copy(gb.at[pl.ds(0, 7)], gb.at[pl.ds(0, 7)], gss.at[j]).wait()
        for p in PIECES:
            take(p[0], units(p[0], 'sent'), ssem.at[PIDX[p[0]]])


def front(x, gains, ws, cos, sin):
    anyspace, vm = pl.BlockSpec(memory_space=pl.ANY), pl.BlockSpec(memory_space=pltpu.VMEM)
    V = pltpu.VMEM
    dma = pltpu.SemaphoreType.DMA
    tab = [cos, sin, np.tile(cos.T, (1, 2)), np.tile(sin.T, (1, 2))]
    return pl.pallas_call(
        front_kernel, name='front',
        in_specs=[anyspace] + [vm] * 3 + [anyspace] * 5 + [vm] * 4,
        out_specs=[anyspace] * 4,
        out_shape=[jax.ShapeDtypeStruct((T, H * VD), BF16), jax.ShapeDtypeStruct((H * VD, D), BF16), jax.ShapeDtypeStruct((T, KR), BF16), jax.ShapeDtypeStruct((T // S, RD, S), BF16)],
        scratch_shapes=[
            V((T, D), BF16), V((D, QR), BF16), V((D, KR + RD), BF16), V((QR, H * 96), BF16), V((KR, H * 128), BF16), V((320, D), BF16),
            V((8, 1, 320), BF16), V((8, 1, 96), BF16), V((8, 1, 32), BF16), V((T, QR), F32), V((T, KR + RD), F32), V((T, 128), F32),
            V((QR, T), BF16), V((T, KR), BF16), V((KR, T), BF16), V((T, RD), BF16), V((T // S, RD, S), BF16),
            V((2, HG * 96, QR), BF16), V((2, KR, HG * 64), BF16), V((2, HG * 64, KR), BF16), V((HG * 128, TC), BF16), V((TC, HG * 64), BF16), V((HG * 64, TC), BF16), V((2, TC, HG * 64), BF16),
            V((KR + RD, 320), BF16), V((320, KR + RD), BF16),
            dma((len(PIECES),)), dma((len(PIECES) - 2, 7)), dma((2, 11)), dma((len(PIECES),)), dma((3,)), dma((3,)), dma((T // TA,)), dma((3,)), dma((3,)),
        ],
        compiler_params=pltpu.CompilerParams(collective_id=0, has_side_effects=True, vmem_limit_bytes=63 << 20),
    )(x, *gains, *ws, *(jnp.asarray(t) for t in tab))


def out_kernel(o_ref, w_ref, x_ref, c_ref, r_ref, y_ref, c_out, r_out):
    for n in range(0, y_ref.shape[1], 256):
        cols = slice(n, n + 256)
        y_ref[:, cols] = (x_ref[:, cols].astype(F32) + dot(o_ref[...], w_ref[:, cols])).astype(BF16)
    c_out[...] = c_ref[...]
    r_out[...] = r_ref[...]


def outp(o, w, x, c, r, tm=1024, tn=1280):
    nt = D // tn
    cr = T // ((T // tm) * nt)
    step = lambda j, i: j * (T // tm) + i
    return pl.pallas_call(
        out_kernel, grid=(nt, T // tm), name='outp',
        in_specs=[pl.BlockSpec((tm, D), lambda j, i: (i, 0)), pl.BlockSpec((D, tn), lambda j, i: (0, j)), pl.BlockSpec((tm, tn), lambda j, i: (i, j)),
                  pl.BlockSpec((cr, KR), lambda j, i: (step(j, i), 0)), pl.BlockSpec((cr // S, RD, S), lambda j, i: (step(j, i), 0, 0))],
        out_specs=[pl.BlockSpec((tm, tn), lambda j, i: (i, j)), pl.BlockSpec((cr, KR), lambda j, i: (step(j, i), 0)), pl.BlockSpec((cr // S, RD, S), lambda j, i: (step(j, i), 0, 0))],
        out_shape=[jax.ShapeDtypeStruct((T, D), BF16), jax.ShapeDtypeStruct((T, KR), BF16), jax.ShapeDtypeStruct((T // S, RD, S), BF16)],
        compiler_params=pltpu.CompilerParams(vmem_limit_bytes=62 << 20),
    )(o, w, x, c, r)


def tables():
    half = RD // 2
    freq = np.float32(10000.0) ** (np.float32(-2.0) * np.arange(half, dtype=np.float32) / np.float32(RD))
    ang = np.arange(S, dtype=np.float32)[:, None] * freq[None, :].astype(np.float32)
    return np.cos(ang).astype(np.float32), np.sin(ang).astype(np.float32)


def solution(mesh):
    batch, row, mat = P(('dp', 'fsdp')), P('fsdp'), P('fsdp', None)

    def local(tok, g1, wdq, gq, wuq, wkv, gkv, wukv, wo):
        cos, sin = tables()
        x = tok.reshape(T, D)
        o, w, c, r = front(x, (g1[None], gq[None], gkv[None]), (wdq, wkv.T, wuq, wukv, wo), cos, sin)
        y, c, r = outp(o, w, x, c, r)
        return y.reshape(tok.shape), c.reshape(-1, S, KR), jnp.swapaxes(r, 1, 2)

    return jax.shard_map(local, mesh=mesh, in_specs=(batch, row, mat, row, mat, mat, row, mat, mat),
                         out_specs=(batch,) * 3, check_vma=False)
```

```python
import functools
import numpy as np
import jax
import jax.numpy as jnp
from jax import lax
from jax.experimental import pallas as pl
from jax.experimental.pallas import tpu as pltpu
from jax.sharding import PartitionSpec as P

F32, BF16 = jnp.float32, jnp.bfloat16
MESH = pl.DeviceIdType.MESH
EPS = 1e-6
T, D, QR, KR, RD, H, ND, VD = 2048, 2560, 768, 256, 32, 40, 64, 64
S = 128
SC = (ND + RD) ** -0.5 * 1.4426950408889634
HG, TC = 8, 512
NCH = T // TC
STEPS = (H // HG) * NCH
TA = 256


def dot(a, b):
    return jnp.dot(a, b, preferred_element_type=F32)


def rms(v):
    return lax.rsqrt(jnp.mean(v * v, axis=-1, keepdims=True) + EPS)


def attn_unit(k, qT, vT, keep):
    s = dot(k, qT) * SC
    s = jnp.where(keep, s, -1e30)
    m = jnp.max(s, axis=0, keepdims=True)
    e = jnp.exp2(s - m)
    p = (e * (1.0 / jnp.sum(e, axis=0, keepdims=True))).astype(BF16)
    return dot(vT, p)


PIECES = (
    ('dq', 'dq', False, 320, 0, 768, 112),
    ('dkv', 'dkv', False, 320, 0, 288, 128),
    ('uq0', 'uq', False, 96, 0, 1536, 32),
    ('ukv0', 'ukv', True, 32, 0, 2048, 768),
    ('uq1', 'uq', False, 96, 1536, 1536, 32),
    ('ukv1', 'ukv', True, 32, 2048, 2048, 768),
    ('uq2', 'uq', False, 96, 3072, 768, 16),
    ('ukv2', 'ukv', True, 32, 4096, 1024, 256),
    ('o0', 'o', False, 320, 0, 512, 128),
    ('o1', 'o', False, 320, 512, 512, 128),
    ('o2', 'o', False, 320, 1024, 512, 96),
    ('o3', 'o', False, 320, 1536, 512, 80),
    ('o4', 'o', False, 320, 2048, 512, 64),
)
PIDX = {p[0]: i for i, p in enumerate(PIECES)}
SPLIT = ('S1a', 'S1b', 'S2a', 'S2b', 'S3a', 'S3b')
KINDS = ('XE', 'YE', 'XS', 'YS', 'S0', 'Z1', 'Z2', 'DY', 'DX', 'Z3', 'S1', 'S2', 'S3') + SPLIT
RSEM = {'XE': 0, 'YE': 0, 'XS': 1, 'YS': 1, 'Z1': 2, 'Z2': 3, 'DY': 4, 'DX': 5, 'Z3': 5, 'S0': 6, 'S1': 6, 'S2': 6, 'S3': 6}
RSEM_SPLIT = dict(RSEM, Z3=7, S1a=8, S1b=8, S2a=9, S2b=9, S3a=10, S3b=10)
SPLIT_ARRS = ('dq', 'dkv')
GROUPS = {'K': ('dkv',), 'D': ('dq',), 'U0': ('uq0', 'ukv0'), 'U1': ('uq1', 'ukv1'), 'U2': ('uq2', 'ukv2'),
          'O0': ('o0',), 'O1': ('o1',), 'O2': ('o2',), 'O3': ('o3',), 'O4': ('o4',)}
STAGES = {
    'st0': ((), ('XE', 'YE', 'XS', 'YS', 'S0')),
    'st1': (('XYE',), ('Z1', 'Z2', 'DY')),
    'st2': (('XYS',), ('DX',)),
    'st4x': (('Z1',), ('S1',)),
    'st3': (('DY',), ('Z3',)),
    'st4y': (('Z2',), ('S2',)),
    'st5': (('DXZ',), ('S3',)),
    'fin': (('SS',), ()),
    'st2d': (('XYS',), ('DX', 'S1a', 'S2a')),
    'st4xd': (('Z1',), ('S1b',)),
    'st4yd': (('Z2',), ('S2b',)),
    'st5a': (('DX',), ('S3a',)),
    'st5b': (('Z3',), ('S3b',)),
    'find': ((), ()),
}
SCHED = {
    'stats0': (('st0', 'K'), ('st0', 'D')),
    'norm1': (('st1', 'K'),),
    'norm2': (('st2d', 'K'),),
    'part0': (('recv', 'K', 'S0'), ('recv', 'D', 'S0')),
    'part2': (('st4xd', 'K'), ('st1', 'D')),
    'k0': (('st0', 'U0'), ('recv', 'K', 'S1a+S1b')),
    'k1': (('st2d', 'D'),),
    'k2': (('st3', 'K'), ('st4yd', 'K'), ('st5a', 'K'), ('recv', 'K', 'S2a+S2b'), ('st4xd', 'D')),
    'k4': (('st3', 'D'), ('st5b', 'K'), ('st4yd', 'D'), ('st1', 'U0'), ('recv', 'K', 'S3a+S3b'), ('st0', 'U1')),
    'k5': (('st2', 'U0'),),
    'q0': (('st5a', 'D'), ('recv', 'D', 'S1a+S1b')),
    'q1': (('st5b', 'D'),),
    'q4': (('st4x', 'U0'), ('st3', 'U0'), ('recv', 'D', 'S2a+S2b')),
    'q5': (('st1', 'U1'),),
    'q7': (('st4y', 'U0'), ('st0', 'U2')),
    'd0': (('st2', 'U1'), ('recv', 'D', 'S3a+S3b')),
    'd2': (('st5', 'U0'), ('st0', 'O0'), ('st0', 'O1')),
    'd4': (('fin', 'U0'), ('st1', 'U2')),
    's0': (('st4x', 'U1'), ('st3', 'U1')),
    's1': (('st4y', 'U1'), ('st2', 'U2')),
    's2': (('st4x', 'U2'), ('st1', 'O0'), ('st0', 'O2')),
    's3': (('st5', 'U1'), ('st2', 'O0')),
    's4': (('st1', 'O1'), ('fin', 'U1')),
    's5': (('st3', 'U2'), ('st4y', 'U2'), ('st4x', 'O0'), ('st2', 'O1')),
    's6': (('st3', 'O0'), ('st4y', 'O0')),
    's7': (('st4x', 'O1'), ('st1', 'O2')),
    's8': (('st2', 'O2'),),
    's9': (('st5', 'U2'), ('st3', 'O1'), ('st4y', 'O1'), ('st0', 'O3'), ('st0', 'O4')),
    's10': (('fin', 'U2'), ('st5', 'O0')),
    's11': (('fin', 'O0'), ('st4x', 'O2'), ('st3', 'O2'), ('st1', 'O3')),
    's12': (('st4y', 'O2'),),
    's13': (('st5', 'O1'), ('st2', 'O3')),
    's14': (('fin', 'O1'), ('st5', 'O2'), ('st1', 'O4')),
    's15': (('fin', 'O2'), ('st4x', 'O3')),
    's16': (('st3', 'O3'), ('st4y', 'O3'), ('st2', 'O4')),
    's17': (('st4x', 'O4'), ('st3', 'O4'), ('st4y', 'O4')),
    's18': (('st5', 'O3'),),
    's19': (('fin', 'O3'), ('st5', 'O4')),
    'end': (('fin', 'O4'),),
    'stats1': (),
}
SWAPPED = ('dq', 'uq0', 'ukv0', 'uq1', 'ukv1', 'uq2', 'ukv2', 'o0', 'o1')


def front_kernel(x_hbm, g1_s, gq_s, gkv_s, dq_s, dkv_t, uq_s, ukv_s, o_s, cos_ref, sin_ref, cosT_ref, sinT_ref,
                 attn_hbm, wo_hbm, c_hbm, r_hbm,
                 xa, wdq, wdkv, wuq, wukv, ostage, g1b, gqb, gkvb, accq, acck, inv, cqT, cbuf, cT, rbuf, rT,
                 wqT, wk, wvT, qT, kbuf, vT, obuf,
                 dkv_in, dkv_s,
                 ssem, rsem, dsem, lsem, gss, grs, xsem, osem, csem):
    z, f = lax.axis_index('dp'), lax.axis_index('fsdp')
    core, xx, yy = f % 2, (f // 2) % 2, f // 4

    def idx(dx, dy, dc):
        return ((yy + dy) % 2) * 4 + ((xx + dx) % 2) * 2 + (core + dc) % 2

    fx, fy, fd = idx(1, 0, 0), idx(0, 1, 0), idx(1, 1, 0)
    dev = {'X': (z, fx), 'Y': (z, fy), 'Z': (1 - z, f), 'S': (z, idx(0, 0, 1))}
    plane = [idx(dx, dy, dc) for dx in range(2) for dy in range(2) for dc in range(2) if dx + dy + dc]
    src = {'dq': dq_s, 'dkv': dkv_s, 'uq': uq_s, 'ukv': ukv_s, 'o': ostage}
    buf = {'dq': wdq, 'dkv': wdkv, 'uq': wuq, 'ukv': wukv, 'o': wo_hbm}

    def region(piece, shard, part, base):
        name, arr, bycol, rows, c0, nc, e = piece
        n = nc if bycol else rows
        off, size = {'E': (z * (n - e), e), 'S': (e, n - 2 * e), 'A': (0, n), 'B': (z * e, n - e), 'M': ((1 - z) * (n - e), e)}[part]
        if bycol:
            row = shard * rows if base else 0
            return pl.ds(pl.multiple_of(row, 16), rows), pl.ds(pl.multiple_of(c0 + off, 128), size)
        row = (shard * rows if base else 0) + off
        return pl.ds(pl.multiple_of(row, 16), size), pl.ds(c0, nc)

    def copy(name, kind):
        piece = PIECES[PIDX[name]]
        arr = piece[1]
        shard = {'X': f, 'Y': f}.get(kind[0]) if kind in ('XE', 'YE', 'XS', 'YS') else None
        if kind in ('XE', 'YE', 'XS', 'YS', 'S0'):
            part = 'A' if kind == 'S0' else kind[1]
            r0, c0 = region(piece, f, part, False)
            r1, c1 = region(piece, f, part, True)
            s_ref, d_ref = src[arr].at[r0, c0], buf[arr].at[r1, c1]
            to = dev[kind[0]]
        else:
            shard, part, to = {'Z1': (fx, 'E', 'Z'), 'Z2': (fy, 'E', 'Z'), 'Z3': (fd, 'E', 'Z'), 'DY': (fx, 'E', 'Y'),
                               'DX': (fy, 'S', 'X'), 'S1': (fx, 'A', 'S'), 'S2': (fy, 'A', 'S'), 'S3': (fd, 'A', 'S'),
                               'S1a': (fx, 'B', 'S'), 'S1b': (fx, 'M', 'S'), 'S2a': (fy, 'B', 'S'), 'S2b': (fy, 'M', 'S'),
                               'S3a': (fd, 'B', 'S'), 'S3b': (fd, 'M', 'S')}[kind]
            if name in SWAPPED and kind in ('DX', 'DY'):
                shard, to = {'DX': (fx, 'Y'), 'DY': (fy, 'X')}[kind]
            to = dev[to]
            r1, c1 = region(piece, shard, part, True)
            s_ref = d_ref = buf[arr].at[r1, c1]
        return pltpu.make_async_remote_copy(src_ref=s_ref, dst_ref=d_ref, send_sem=ssem.at[PIDX[name]], recv_sem=rsem_of(name, kind),
                                            device_id=to, device_id_type=MESH)

    def rsem_of(name, kind):
        if PIECES[PIDX[name]][1] in SPLIT_ARRS:
            return dsem.at[PIDX[name], RSEM_SPLIT[kind]]
        return rsem.at[PIDX[name] - 2, RSEM[kind]]

    def take(name, n, sem, rows_too=True):
        _, arr, bycol, rows, c0, nc, e = PIECES[PIDX[name]]
        ref = buf[arr]
        if bycol:
            k = max(1, -(-n // nc))
            assert n % k == 0
            part = ref.at[pl.ds(0, rows * k), pl.ds(c0, n // k)]
        else:
            part = ref.at[pl.ds(0, n), pl.ds(c0, nc)]
        pltpu.make_async_copy(part, part, sem).wait()

    def units(name, what):
        _, arr, bycol, rows, c0, nc, e = PIECES[PIDX[name]]
        n = nc if bycol else rows
        return {'XYE': 2 * e, 'XYS': 2 * (n - 2 * e), 'Z1': e, 'Z2': e, 'DY': e, 'DX': n - 2 * e, 'Z3': e, 'DXZ': n - e, 'SS': 4 * n,
                'S0': n, 'S1': n, 'S2': n, 'S3': n, 'sent': 7 * n}[what]

    FIRST = {'XYE': 'XE', 'XYS': 'XS', 'DXZ': 'DX', 'SS': 'S0'}

    def local(name):
        piece = PIECES[PIDX[name]]
        r0, c0 = region(piece, f, 'A', False)
        r1, c1 = region(piece, f, 'A', True)
        return pltpu.make_async_copy(src[piece[1]].at[r0, c0], buf[piece[1]].at[r1, c1], lsem.at[PIDX[name]])

    def start(names, *kinds):
        for k in kinds:
            for n in names:
                copy(n, k).start()

    def recv(names, *kinds):
        for k in kinds:
            for n in names:
                k = {'S1a+S1b': 'S1', 'S2a+S2b': 'S2', 'S3a+S3b': 'S3'}.get(k, k)
                first = k + 'a' if k in ('S1', 'S2', 'S3') else FIRST.get(k, k)
                take(n, units(n, k), rsem_of(n, first))

    def comm(todo):
        for op in todo:
            stage, piece = op[0], op[1]
            names = GROUPS[piece]
            if stage == 'recv':
                recv(names, op[2])
                continue
            if stage == 'st0' and piece == 'O0':
                stage_o.wait()
            waits, starts = STAGES[stage]
            recv(names, *waits)
            start(names, *starts)
            if stage == 'st0':
                for n in names:
                    local(n).start()
            if stage in ('fin', 'find'):
                for n in names:
                    if piece not in ('K', 'D'):
                        local(n).wait()

    def at(seg, i):
        marks = sorted((int(n[len(seg):]), n) for n in SCHED if n.startswith(seg) and n[len(seg):].isdigit() and SCHED[n])

        def tree(ms):
            if len(ms) == 1:
                @pl.when(i == ms[0][0])
                def _():
                    with jax.named_scope('comm_' + ms[0][1]):
                        comm(SCHED[ms[0][1]])
            elif ms:
                h = len(ms) // 2
                lax.cond(i < ms[h][0], lambda: tree(ms[:h]), lambda: tree(ms[h:]))
        tree(marks)

    barrier = pltpu.get_barrier_semaphore()
    for p in plane:
        pl.semaphore_signal(barrier, inc=1, device_id=(z, p), device_id_type=MESH)
    pl.semaphore_signal(barrier, inc=1, device_id=dev['Z'], device_id_type=MESH)
    turn = pltpu.make_async_copy(dkv_t, dkv_in, csem.at[2])
    turn.start()
    stage_o = pltpu.make_async_copy(o_s, ostage, osem.at[2])

    def load_x(lo, hi):
        for i in range(lo, hi):
            pltpu.make_async_copy(x_hbm.at[pl.ds(i * TA, TA)], xa.at[pl.ds(i * TA, TA)], xsem.at[i]).start()

    load_x(0, 1)

    def stat_tile(i, _):
        pltpu.make_async_copy(x_hbm.at[pl.ds(i * TA, TA)], xa.at[pl.ds(i * TA, TA)], xsem.at[i]).wait()
        for h in range(TA // 64):
            rows = pl.ds(pl.multiple_of(i * TA + h * 64, 64), 64)
            inv[rows, :] = jnp.broadcast_to(rms(xa[rows, :].astype(F32)), (64, 128))
        return 0

    turn.wait()
    load_x(1, T // TA)
    dkv_s[...] = dkv_in[...].T
    with jax.named_scope('barrier'):
        pl.semaphore_wait(barrier, 8)

    for j, (gs, gb) in enumerate(((g1_s, g1b), (gq_s, gqb), (gkv_s, gkvb))):
        for p in plane:
            pltpu.make_async_remote_copy(src_ref=gs, dst_ref=gb.at[f], send_sem=gss.at[j], recv_sem=grs.at[j],
                                         device_id=(z, p), device_id_type=MESH).start()
        pltpu.make_async_copy(gs, gb.at[f], grs.at[j]).start()
    comm(SCHED['stats0'])

    stage_o.start()
    with jax.named_scope('stats_b'):
        lax.fori_loop(0, T // TA, stat_tile, 0)
    comm(SCHED['stats1'])
    with jax.named_scope('gains'):
        for j, gb in enumerate((g1b, gqb, gkvb)):
            pltpu.make_async_copy(gb, gb, grs.at[j]).wait()

    def row_of(gb):
        return jnp.concatenate([gb[i].astype(F32) for i in range(8)], axis=-1)

    g1, gq, gkv = row_of(g1b), row_of(gqb), row_of(gkvb)

    def norm_tile(i, _):
        pl.when(i % 2 == 0)(functools.partial(at, 'norm', i // 2))
        for h in range(TA // 64):
            rows = pl.ds(pl.multiple_of(i * TA + h * 64, 64), 64)
            scale = inv[rows, :]
            for j in range(D // 128):
                cols = slice(128 * j, 128 * j + 128)
                xa[rows, cols] = (xa[rows, cols].astype(F32) * scale * g1[:, cols]).astype(BF16)
        return 0

    def quarter_cols(dy, dx):
        quarter = ((yy + dy) % 2) * 2 + (xx + dx) % 2
        return pl.ds(pl.multiple_of(quarter * 640, 128), 640)

    def own_part(i, _):
        at('part', i)
        cols, rows = quarter_cols(0, 0), pl.ds(pl.multiple_of(i * 512, 512), 512)
        a = xa[rows, cols]
        accq[rows, :] = dot(a, wdq[cols, :])
        acck[rows, :] = dot(a, wdkv[cols, :])
        return 0

    def kv_part(i, _):
        at('k', i)
        q = i // 2 + 1
        cols, rows = quarter_cols(q // 2, q % 2), pl.ds(pl.multiple_of((i % 2) * 1024, 1024), 1024)
        acck[rows, :] += dot(xa[rows, cols], wdkv[cols, :])
        return 0

    def q_part(x_not_y, i, _):
        at('q', i if x_not_y else i + 4)
        if x_not_y:
            finish_kv(2 * i)
            finish_kv(2 * i + 1)
        cols, rows = quarter_cols(0, 1) if x_not_y else quarter_cols(1, 0), pl.ds(pl.multiple_of(i * 512, 512), 512)
        accq[rows, :] += dot(xa[rows, cols], wdq[cols, :])
        return 0

    cos2 = jnp.concatenate([cos_ref[...]] * (TA // S), axis=0)
    sin2 = jnp.concatenate([sin_ref[...]] * (TA // S), axis=0)

    def finish_kv(i):
        rows = pl.ds(pl.multiple_of(i * TA, TA), TA)
        kd = acck[rows, :]
        kc = kd[:, :KR]
        c = (kc * rms(kc) * gkv).astype(BF16)
        cbuf[rows, :] = c
        cT[:, rows] = c.T
        lo, hi = kd[:, KR:KR + 16], kd[:, KR + 16:]
        r = jnp.concatenate([lo * cos2 - hi * sin2, hi * cos2 + lo * sin2], axis=-1).astype(BF16)
        rbuf[rows, :] = r
        for h in range(TA // S):
            rT[i * (TA // S) + h] = r[h * S:h * S + S].T

    def finish_q(i):
        rows = pl.ds(pl.multiple_of(i * TA, TA), TA)
        qd = accq[rows, :]
        cqT[:, rows] = (qd * rms(qd) * gq).astype(BF16).T

    def last_part():
        cols = pl.ds(pl.multiple_of((fd // 2) * 640, 128), 640)

        def tile(i, _):
            pl.when(i % 2 == 0)(functools.partial(at, 'd', i // 2))
            finish_q(jnp.maximum(i - 1, 0))
            rows = pl.ds(pl.multiple_of(jnp.minimum(i, T // TA - 1) * TA, TA), TA)
            accq[rows, :] += dot(xa[rows, cols], wdq[cols, :])
            return 0
        lax.fori_loop(0, T // TA + 1, tile, 0)

    with jax.named_scope('norm'):
        lax.fori_loop(0, T // TA, norm_tile, 0)
    for n in ('dq', 'dkv'):
        local(n).wait()
    with jax.named_scope('own'):
        lax.fori_loop(0, 4, own_part, 0)
    with jax.named_scope('kv'):
        lax.fori_loop(0, 6, kv_part, 0)
    with jax.named_scope('qx'):
        lax.fori_loop(0, 4, functools.partial(q_part, True), 0)
    with jax.named_scope('qy'):
        lax.fori_loop(0, 4, functools.partial(q_part, False), 0)
    with jax.named_scope('last'):
        last_part()
    outs = [pltpu.make_async_copy(cbuf, c_hbm, csem.at[0]), pltpu.make_async_copy(rT, r_hbm, csem.at[1])]
    for o in outs:
        o.start()

    keep = lax.broadcasted_iota(jnp.int32, (S, S), 0) <= lax.broadcasted_iota(jnp.int32, (S, S), 1)
    lane = lax.broadcasted_iota(jnp.int32, (S, 128), 1)
    co, si = cosT_ref[...], sinT_ref[...]
    for h in range(HG):
        zr = 128 * h + (96 if h % 2 == 0 else 32)
        qT[zr:zr + 32, :] = jnp.zeros((32, TC), BF16)

    def prepare(g, k, slot):
        col = 256 * jnp.minimum(k, 2)
        wqT[slot, pl.ds(pl.multiple_of(col, 256), 256), :] = wuq[:, pl.ds(pl.multiple_of(g * (HG * 96) + col, 128), 256)].T
        t0 = wukv[:, pl.ds(pl.multiple_of(g * (HG * 128) + 256 * k, 128), 128)]
        t1 = wukv[:, pl.ds(pl.multiple_of(g * (HG * 128) + 256 * k + 128, 128), 128)]
        lanes = pl.ds(pl.multiple_of(128 * k, 128), 128)
        wk[slot, :, lanes] = jnp.concatenate([t0[:, :64], t1[:, :64]], axis=1)
        wvT[slot, lanes, :] = jnp.concatenate([t0[:, 64:], t1[:, 64:]], axis=1).T

    def out_copy(i):
        g, tc = i // NCH, i % NCH
        return pltpu.make_async_copy(obuf.at[i % 2], attn_hbm.at[pl.ds(pl.multiple_of(tc * TC, TC), TC), pl.ds(pl.multiple_of(g * (HG * 64), 128), HG * 64)], osem.at[i % 2])

    def step(i, _):
        g, tc = i // NCH, i % NCH
        tok = pl.multiple_of(tc * TC, TC)
        at('s', i)

        @pl.when(i == 0)
        def _():
            with jax.named_scope('prepare'):
                for k in range(4):
                    prepare(0, k, 0)

        here = g % 2
        @pl.when(i >= 2)
        def _():
            out_copy(i - 2).wait()

        slot = i % 2
        for n in range(TC // 256):
            q = dot(wqT[here], cqT[:, pl.ds(tok + 256 * n, 256)])
            cols = slice(256 * n, 256 * n + 256)
            for h in range(HG):
                nope = q[96 * h:96 * h + 64]
                lo, hi = q[96 * h + 64:96 * h + 80], q[96 * h + 80:96 * h + 96]
                b = 128 * h
                qn, qp = (b, b + 64) if h % 2 == 0 else (b + 64, b)
                qT[qn:qn + 64, cols] = nope.astype(BF16)
                qT[qp:qp + 16, cols] = (lo * co - hi * si).astype(BF16)
                qT[qp + 16:qp + 32, cols] = (hi * co + lo * si).astype(BF16)
        kbuf[...] = dot(cbuf[pl.ds(tok, TC), :], wk[here]).astype(BF16)
        vT[...] = dot(wvT[here], cT[:, pl.ds(tok, TC)]).astype(BF16)
        prepare(jnp.minimum(g + 1, H // HG - 1), tc, 1 - here)

        for p in range(TC // S):
            row = p * S
            r = rbuf[pl.ds(tok + row, S), :]
            z32, z64 = jnp.zeros((S, 32), BF16), jnp.zeros((S, 64), BF16)
            r_hi = jnp.concatenate([z64, r, z32], axis=1)
            r_lo = jnp.concatenate([r, z32, z64], axis=1)
            for j in range(HG // 2):
                k2 = kbuf[row:row + S, 128 * j:128 * j + 128]
                both = []
                for par in range(2):
                    h = 2 * j + par
                    k = jnp.where(lane < 64, k2, r_hi) if par == 0 else jnp.where(lane < 64, r_lo, k2)
                    both.append(attn_unit(k, qT[128 * h:128 * h + 128, row:row + S], vT[64 * h:64 * h + 64, row:row + S], keep))
                obuf[slot, row:row + S, 128 * j:128 * j + 128] = jnp.concatenate(both, axis=0).astype(BF16).T
        out_copy(i).start()
        return 0

    lax.fori_loop(0, STEPS, step, 0)
    with jax.named_scope('fin_O'):
        comm(SCHED['end'])
    with jax.named_scope('tail_out'):
        for i in (STEPS - 2, STEPS - 1):
            out_copy(i).wait()
        for o in outs:
            o.wait()
    with jax.named_scope('tail_sends'):
        for j, gb in enumerate((g1b, gqb, gkvb)):
            pltpu.make_async_copy(gb.at[pl.ds(0, 7)], gb.at[pl.ds(0, 7)], gss.at[j]).wait()
        for p in PIECES:
            take(p[0], units(p[0], 'sent'), ssem.at[PIDX[p[0]]])


def front(x, gains, ws, cos, sin):
    anyspace, vm = pl.BlockSpec(memory_space=pl.ANY), pl.BlockSpec(memory_space=pltpu.VMEM)
    V = pltpu.VMEM
    dma = pltpu.SemaphoreType.DMA
    tab = [cos, sin, np.tile(cos.T, (1, 2)), np.tile(sin.T, (1, 2))]
    return pl.pallas_call(
        front_kernel, name='front',
        in_specs=[anyspace] + [vm] * 3 + [anyspace] * 5 + [vm] * 4,
        out_specs=[anyspace] * 4,
        out_shape=[jax.ShapeDtypeStruct((T, H * VD), BF16), jax.ShapeDtypeStruct((H * VD, D), BF16), jax.ShapeDtypeStruct((T, KR), BF16), jax.ShapeDtypeStruct((T // S, RD, S), BF16)],
        scratch_shapes=[
            V((T, D), BF16), V((D, QR), BF16), V((D, KR + RD), BF16), V((QR, H * 96), BF16), V((KR, H * 128), BF16), V((320, D), BF16),
            V((8, 1, 320), BF16), V((8, 1, 96), BF16), V((8, 1, 32), BF16), V((T, QR), F32), V((T, KR + RD), F32), V((T, 128), F32),
            V((QR, T), BF16), V((T, KR), BF16), V((KR, T), BF16), V((T, RD), BF16), V((T // S, RD, S), BF16),
            V((2, HG * 96, QR), BF16), V((2, KR, HG * 64), BF16), V((2, HG * 64, KR), BF16), V((HG * 128, TC), BF16), V((TC, HG * 64), BF16), V((HG * 64, TC), BF16), V((2, TC, HG * 64), BF16),
            V((KR + RD, 320), BF16), V((320, KR + RD), BF16),
            dma((len(PIECES),)), dma((len(PIECES) - 2, 7)), dma((2, 11)), dma((len(PIECES),)), dma((3,)), dma((3,)), dma((T // TA,)), dma((3,)), dma((3,)),
        ],
        compiler_params=pltpu.CompilerParams(collective_id=0, has_side_effects=True, vmem_limit_bytes=63 << 20),
    )(x, *gains, *ws, *(jnp.asarray(t) for t in tab))


def out_kernel(o_ref, w_ref, x_ref, c_ref, r_ref, y_ref, c_out, r_out):
    for n in range(0, y_ref.shape[1], 256):
        cols = slice(n, n + 256)
        y_ref[:, cols] = (x_ref[:, cols].astype(F32) + dot(o_ref[...], w_ref[:, cols])).astype(BF16)
    c_out[...] = c_ref[...]
    r_out[...] = r_ref[...]


def outp(o, w, x, c, r, tm=1024, tn=1280):
    nt = D // tn
    cr = T // ((T // tm) * nt)
    step = lambda j, i: j * (T // tm) + i
    return pl.pallas_call(
        out_kernel, grid=(nt, T // tm), name='outp',
        in_specs=[pl.BlockSpec((tm, D), lambda j, i: (i, 0)), pl.BlockSpec((D, tn), lambda j, i: (0, j)), pl.BlockSpec((tm, tn), lambda j, i: (i, j)),
                  pl.BlockSpec((cr, KR), lambda j, i: (step(j, i), 0)), pl.BlockSpec((cr // S, RD, S), lambda j, i: (step(j, i), 0, 0))],
        out_specs=[pl.BlockSpec((tm, tn), lambda j, i: (i, j)), pl.BlockSpec((cr, KR), lambda j, i: (step(j, i), 0)), pl.BlockSpec((cr // S, RD, S), lambda j, i: (step(j, i), 0, 0))],
        out_shape=[jax.ShapeDtypeStruct((T, D), BF16), jax.ShapeDtypeStruct((T, KR), BF16), jax.ShapeDtypeStruct((T // S, RD, S), BF16)],
        compiler_params=pltpu.CompilerParams(vmem_limit_bytes=62 << 20),
    )(o, w, x, c, r)


def tables():
    half = RD // 2
    freq = np.float32(10000.0) ** (np.float32(-2.0) * np.arange(half, dtype=np.float32) / np.float32(RD))
    ang = np.arange(S, dtype=np.float32)[:, None] * freq[None, :].astype(np.float32)
    return np.cos(ang).astype(np.float32), np.sin(ang).astype(np.float32)


def solution(mesh):
    batch, row, mat = P(('dp', 'fsdp')), P('fsdp'), P('fsdp', None)

    def local(tok, g1, wdq, gq, wuq, wkv, gkv, wukv, wo):
        cos, sin = tables()
        x = tok.reshape(T, D)
        o, w, c, r = front(x, (g1[None], gq[None], gkv[None]), (wdq, wkv.T, wuq, wukv, wo), cos, sin)
        y, c, r = outp(o, w, x, c, r)
        return y.reshape(tok.shape), c.reshape(-1, S, KR), jnp.swapaxes(r, 1, 2)

    return jax.shard_map(local, mesh=mesh, in_specs=(batch, row, mat, row, mat, mat, row, mat, mat),
                         out_specs=(batch,) * 3, check_vma=False)
```

```python
import functools
import numpy as np
import jax
import jax.numpy as jnp
from jax import lax
from jax.experimental import pallas as pl
from jax.experimental.pallas import tpu as pltpu
from jax.sharding import PartitionSpec as P

F32, BF16 = jnp.float32, jnp.bfloat16
MESH = pl.DeviceIdType.MESH
EPS = 1e-6
T, D, QR, KR, RD, H, ND, VD = 2048, 2560, 768, 256, 32, 40, 64, 64
S = 128
SC = (ND + RD) ** -0.5 * 1.4426950408889634
HG, TC = 8, 512
NCH = T // TC
STEPS = (H // HG) * NCH
TA = 256


def dot(a, b):
    return jnp.dot(a, b, preferred_element_type=F32)


def rms(v):
    return lax.rsqrt(jnp.mean(v * v, axis=-1, keepdims=True) + EPS)


def attn_unit(k, qT, vT, keep):
    s = dot(k, qT) * SC
    s = jnp.where(keep, s, -1e30)
    m = jnp.max(s, axis=0, keepdims=True)
    e = jnp.exp2(s - m)
    p = (e * (1.0 / jnp.sum(e, axis=0, keepdims=True))).astype(BF16)
    return dot(vT, p)


PIECES = (
    ('dq', 'dq', False, 320, 0, 768, 112),
    ('dkv', 'dkv', False, 320, 0, 288, 112),
    ('uq0', 'uq', False, 96, 0, 768, 32),
    ('ukv0', 'ukv', True, 32, 0, 1024, 128),
    ('uq1', 'uq', False, 96, 768, 1536, 32),
    ('ukv1', 'ukv', True, 32, 1024, 2048, 768),
    ('uq2', 'uq', False, 96, 2304, 1536, 32),
    ('ukv2', 'ukv', True, 32, 3072, 2048, 768),
    ('o0', 'o', False, 320, 0, 512, 128),
    ('o1', 'o', False, 320, 512, 512, 112),
    ('o2', 'o', False, 320, 1024, 512, 80),
    ('o3', 'o', False, 320, 1536, 512, 64),
    ('o4', 'o', False, 320, 2048, 512, 96),
)
PIDX = {p[0]: i for i, p in enumerate(PIECES)}
SPLIT = ('S1a', 'S1b', 'S2a', 'S2b', 'S3a', 'S3b')
KINDS = ('XE', 'YE', 'XS', 'YS', 'S0', 'Z1', 'Z2', 'DY', 'DX', 'Z3', 'S1', 'S2', 'S3') + SPLIT
RSEM = {'XE': 0, 'YE': 0, 'XS': 1, 'YS': 1, 'Z1': 2, 'Z2': 3, 'DY': 4, 'DX': 5, 'Z3': 5, 'S0': 6, 'S1': 6, 'S2': 6, 'S3': 6}
RSEM_SPLIT = dict(RSEM, Z3=7, S1a=8, S1b=8, S2a=9, S2b=9, S3a=10, S3b=10)
SPLIT_ARRS = ('dq', 'dkv')
GROUPS = {'K': ('dkv',), 'D': ('dq',), 'U0': ('uq0', 'ukv0'), 'U1': ('uq1', 'ukv1'), 'U2': ('uq2', 'ukv2'),
          'O0': ('o0',), 'O1': ('o1',), 'O2': ('o2',), 'O3': ('o3',), 'O4': ('o4',)}
STAGES = {
    'st0': ((), ('XE', 'YE', 'XS', 'YS', 'S0')),
    'st1': (('XYE',), ('Z1', 'Z2', 'DY')),
    'st2': (('XYS',), ('DX',)),
    'st4x': (('Z1',), ('S1',)),
    'st3': (('DY',), ('Z3',)),
    'st4y': (('Z2',), ('S2',)),
    'st5': (('DXZ',), ('S3',)),
    'fin': (('SS',), ()),
    'st2d': (('XYS',), ('DX', 'S1a', 'S2a')),
    'st4xd': (('Z1',), ('S1b',)),
    'st4yd': (('Z2',), ('S2b',)),
    'st5a': (('DX',), ('S3a',)),
    'st5b': (('Z3',), ('S3b',)),
    'find': ((), ()),
}
SCHED = {
    'stats0': (('st0', 'K'), ('st0', 'D')),
    'norm1': (('st1', 'K'),),
    'norm3': (('st2d', 'K'),),
    'part0': (('recv', 'K', 'S0'), ('recv', 'D', 'S0')),
    'part1': (('st0', 'U0'),),
    'part2': (('st4xd', 'K'), ('st1', 'D')),
    'k0': (('recv', 'K', 'S1a+S1b'),),
    'k1': (('st2d', 'D'),),
    'k2': (('st0', 'U1'), ('st3', 'K'), ('st4yd', 'K'), ('st5a', 'K'), ('recv', 'K', 'S2a+S2b'), ('st4xd', 'D'), ('st1', 'U0')),
    'k3': (('st2', 'U0'),),
    'q0': (('recv', 'D', 'S1a+S1b'),),
    'q3': (('st5b', 'K'), ('st3', 'D'), ('st4yd', 'D'), ('st5a', 'D')),
    'k4': (('st4x', 'U0'), ('recv', 'K', 'S3a+S3b')),
    'q4': (('st1', 'U1'), ('recv', 'D', 'S2a+S2b')),
    'q5': (('st0', 'U2'),),
    'q6': (('st0', 'O0'), ('st5b', 'D')),
    'q7': (('st3', 'U0'), ('st4y', 'U0'), ('st2', 'U1')),
    'd0': (('recv', 'D', 'S3a+S3b'),),
    'd1': (('st4x', 'U1'),),
    'd2': (('st3', 'U1'),),
    'd4': (('st4y', 'U1'),),
    's0': (('st1', 'U2'), ('st5', 'U0'), ('fin', 'U0')),
    's1': (('st2', 'U2'), ('st0', 'O1')),
    's2': (('st4x', 'U2'), ('st1', 'O0'), ('st2', 'O0')),
    's3': (('st5', 'U1'),),
    's4': (('st3', 'U2'), ('st4y', 'U2'), ('st0', 'O2'), ('fin', 'U1')),
    's5': (('st4x', 'O0'), ('st1', 'O1')),
    's6': (('st2', 'O1'),),
    's7': (('st5', 'U2'), ('st3', 'O0'), ('st4y', 'O0'), ('st1', 'O2')),
    's8': (('st4x', 'O1'), ('st0', 'O3'), ('st0', 'O4'), ('fin', 'U2')),
    's9': (('st2', 'O2'),),
    's10': (('st3', 'O1'), ('st4y', 'O1')),
    's11': (('st5', 'O0'), ('st4x', 'O2'), ('st3', 'O2'), ('st1', 'O3')),
    's12': (('fin', 'O0'), ('st4y', 'O2')),
    's13': (('st5', 'O1'), ('st2', 'O3')),
    's14': (('fin', 'O1'), ('st1', 'O4')),
    's15': (('st4x', 'O3'), ('st2', 'O4')),
    's16': (('st5', 'O2'), ('st3', 'O3'), ('st4y', 'O3'), ('st4x', 'O4')),
    's17': (('fin', 'O2'), ('st3', 'O4'), ('st4y', 'O4')),
    's18': (('st5', 'O3'),),
    's19': (('fin', 'O3'), ('st5', 'O4')),
    'end': (('fin', 'O4'),),
    'stats1': (),
}
SWAPPED = ('uq0', 'ukv0', 'uq1', 'ukv1', 'uq2', 'ukv2', 'o0')


def front_kernel(x_hbm, g1_s, gq_s, gkv_s, dq_s, dkv_t, uq_s, ukv_s, o_s, cos_ref, sin_ref, cosT_ref, sinT_ref,
                 attn_hbm, wo_hbm, c_hbm, r_hbm,
                 xa, wdq, wdkv, wuq, wukv, ostage, g1b, gqb, gkvb, accq, acck, inv, cqT, cbuf, cT, rbuf, rT,
                 wqT, wk, wvT, qT, kbuf, vT, obuf,
                 dkv_in, dkv_s,
                 ssem, rsem, dsem, lsem, gss, grs, xsem, osem, csem):
    z, f = lax.axis_index('dp'), lax.axis_index('fsdp')
    core, xx, yy = f % 2, (f // 2) % 2, f // 4

    def idx(dx, dy, dc):
        return ((yy + dy) % 2) * 4 + ((xx + dx) % 2) * 2 + (core + dc) % 2

    fx, fy, fd = idx(1, 0, 0), idx(0, 1, 0), idx(1, 1, 0)
    dev = {'X': (z, fx), 'Y': (z, fy), 'Z': (1 - z, f), 'S': (z, idx(0, 0, 1))}
    plane = [idx(dx, dy, dc) for dx in range(2) for dy in range(2) for dc in range(2) if dx + dy + dc]
    src = {'dq': dq_s, 'dkv': dkv_s, 'uq': uq_s, 'ukv': ukv_s, 'o': ostage}
    buf = {'dq': wdq, 'dkv': wdkv, 'uq': wuq, 'ukv': wukv, 'o': wo_hbm}

    def region(piece, shard, part, base):
        name, arr, bycol, rows, c0, nc, e = piece
        n = nc if bycol else rows
        off, size = {'E': (z * (n - e), e), 'S': (e, n - 2 * e), 'A': (0, n), 'B': (z * e, n - e), 'M': ((1 - z) * (n - e), e)}[part]
        if bycol:
            row = shard * rows if base else 0
            return pl.ds(pl.multiple_of(row, 16), rows), pl.ds(pl.multiple_of(c0 + off, 128), size)
        row = (shard * rows if base else 0) + off
        return pl.ds(pl.multiple_of(row, 16), size), pl.ds(c0, nc)

    def copy(name, kind):
        piece = PIECES[PIDX[name]]
        arr = piece[1]
        shard = {'X': f, 'Y': f}.get(kind[0]) if kind in ('XE', 'YE', 'XS', 'YS') else None
        if kind in ('XE', 'YE', 'XS', 'YS', 'S0'):
            part = 'A' if kind == 'S0' else kind[1]
            r0, c0 = region(piece, f, part, False)
            r1, c1 = region(piece, f, part, True)
            s_ref, d_ref = src[arr].at[r0, c0], buf[arr].at[r1, c1]
            to = dev[kind[0]]
        else:
            shard, part, to = {'Z1': (fx, 'E', 'Z'), 'Z2': (fy, 'E', 'Z'), 'Z3': (fd, 'E', 'Z'), 'DY': (fx, 'E', 'Y'),
                               'DX': (fy, 'S', 'X'), 'S1': (fx, 'A', 'S'), 'S2': (fy, 'A', 'S'), 'S3': (fd, 'A', 'S'),
                               'S1a': (fx, 'B', 'S'), 'S1b': (fx, 'M', 'S'), 'S2a': (fy, 'B', 'S'), 'S2b': (fy, 'M', 'S'),
                               'S3a': (fd, 'B', 'S'), 'S3b': (fd, 'M', 'S')}[kind]
            if name in SWAPPED and kind in ('DX', 'DY'):
                shard, to = {'DX': (fx, 'Y'), 'DY': (fy, 'X')}[kind]
            to = dev[to]
            r1, c1 = region(piece, shard, part, True)
            s_ref = d_ref = buf[arr].at[r1, c1]
        return pltpu.make_async_remote_copy(src_ref=s_ref, dst_ref=d_ref, send_sem=ssem.at[PIDX[name]], recv_sem=rsem_of(name, kind),
                                            device_id=to, device_id_type=MESH)

    def rsem_of(name, kind):
        if PIECES[PIDX[name]][1] in SPLIT_ARRS:
            return dsem.at[PIDX[name], RSEM_SPLIT[kind]]
        return rsem.at[PIDX[name] - 2, RSEM[kind]]

    def take(name, n, sem, rows_too=True):
        _, arr, bycol, rows, c0, nc, e = PIECES[PIDX[name]]
        ref = buf[arr]
        if bycol:
            k = max(1, -(-n // nc))
            assert n % k == 0
            part = ref.at[pl.ds(0, rows * k), pl.ds(c0, n // k)]
        else:
            part = ref.at[pl.ds(0, n), pl.ds(c0, nc)]
        pltpu.make_async_copy(part, part, sem).wait()

    def units(name, what):
        _, arr, bycol, rows, c0, nc, e = PIECES[PIDX[name]]
        n = nc if bycol else rows
        return {'XYE': 2 * e, 'XYS': 2 * (n - 2 * e), 'Z1': e, 'Z2': e, 'DY': e, 'DX': n - 2 * e, 'Z3': e, 'DXZ': n - e, 'SS': 4 * n,
                'S0': n, 'S1': n, 'S2': n, 'S3': n, 'sent': 7 * n}[what]

    FIRST = {'XYE': 'XE', 'XYS': 'XS', 'DXZ': 'DX', 'SS': 'S0'}

    def local(name):
        piece = PIECES[PIDX[name]]
        r0, c0 = region(piece, f, 'A', False)
        r1, c1 = region(piece, f, 'A', True)
        return pltpu.make_async_copy(src[piece[1]].at[r0, c0], buf[piece[1]].at[r1, c1], lsem.at[PIDX[name]])

    def start(names, *kinds):
        for k in kinds:
            for n in names:
                copy(n, k).start()

    def recv(names, *kinds):
        for k in kinds:
            for n in names:
                k = {'S1a+S1b': 'S1', 'S2a+S2b': 'S2', 'S3a+S3b': 'S3'}.get(k, k)
                first = k + 'a' if k in ('S1', 'S2', 'S3') else FIRST.get(k, k)
                take(n, units(n, k), rsem_of(n, first))

    def comm(todo):
        for op in todo:
            stage, piece = op[0], op[1]
            names = GROUPS[piece]
            if stage == 'recv':
                recv(names, op[2])
                continue
            if stage == 'st0' and piece == 'O0':
                stage_o.wait()
            waits, starts = STAGES[stage]
            recv(names, *waits)
            start(names, *starts)
            if stage == 'st0':
                for n in names:
                    local(n).start()
            if stage in ('fin', 'find'):
                for n in names:
                    if piece not in ('K', 'D'):
                        local(n).wait()

    def at(seg, i):
        marks = sorted((int(n[len(seg):]), n) for n in SCHED if n.startswith(seg) and n[len(seg):].isdigit() and SCHED[n])

        def tree(ms):
            if len(ms) == 1:
                @pl.when(i == ms[0][0])
                def _():
                    with jax.named_scope('comm_' + ms[0][1]):
                        comm(SCHED[ms[0][1]])
            elif ms:
                h = len(ms) // 2
                lax.cond(i < ms[h][0], lambda: tree(ms[:h]), lambda: tree(ms[h:]))
        tree(marks)

    barrier = pltpu.get_barrier_semaphore()
    for p in plane:
        pl.semaphore_signal(barrier, inc=1, device_id=(z, p), device_id_type=MESH)
    pl.semaphore_signal(barrier, inc=1, device_id=dev['Z'], device_id_type=MESH)
    turn = pltpu.make_async_copy(dkv_t, dkv_in, csem.at[2])
    turn.start()
    stage_o = pltpu.make_async_copy(o_s, ostage, osem.at[2])

    def load_x(lo, hi):
        for i in range(lo, hi):
            pltpu.make_async_copy(x_hbm.at[pl.ds(i * TA, TA)], xa.at[pl.ds(i * TA, TA)], xsem.at[i]).start()

    load_x(0, 1)

    def stat_tile(i, _):
        pltpu.make_async_copy(x_hbm.at[pl.ds(i * TA, TA)], xa.at[pl.ds(i * TA, TA)], xsem.at[i]).wait()
        for h in range(TA // 64):
            rows = pl.ds(pl.multiple_of(i * TA + h * 64, 64), 64)
            inv[rows, :] = jnp.broadcast_to(rms(xa[rows, :].astype(F32)), (64, 128))
        return 0

    turn.wait()
    load_x(1, T // TA)
    dkv_s[...] = dkv_in[...].T
    with jax.named_scope('barrier'):
        pl.semaphore_wait(barrier, 8)

    for j, (gs, gb) in enumerate(((g1_s, g1b), (gq_s, gqb), (gkv_s, gkvb))):
        for p in plane:
            pltpu.make_async_remote_copy(src_ref=gs, dst_ref=gb.at[f], send_sem=gss.at[j], recv_sem=grs.at[j],
                                         device_id=(z, p), device_id_type=MESH).start()
        pltpu.make_async_copy(gs, gb.at[f], grs.at[j]).start()
    comm(SCHED['stats0'])

    stage_o.start()
    with jax.named_scope('stats_b'):
        lax.fori_loop(0, T // TA, stat_tile, 0)
    comm(SCHED['stats1'])
    with jax.named_scope('gains'):
        for j, gb in enumerate((g1b, gqb, gkvb)):
            pltpu.make_async_copy(gb, gb, grs.at[j]).wait()

    def row_of(gb):
        return jnp.concatenate([gb[i].astype(F32) for i in range(8)], axis=-1)

    g1, gq, gkv = row_of(g1b), row_of(gqb), row_of(gkvb)

    def norm_tile(i, _):
        pl.when(i % 2 == 0)(functools.partial(at, 'norm', i // 2))
        for h in range(TA // 64):
            rows = pl.ds(pl.multiple_of(i * TA + h * 64, 64), 64)
            scale = inv[rows, :]
            for j in range(D // 128):
                cols = slice(128 * j, 128 * j + 128)
                xa[rows, cols] = (xa[rows, cols].astype(F32) * scale * g1[:, cols]).astype(BF16)
        return 0

    def quarter_cols(dy, dx):
        quarter = ((yy + dy) % 2) * 2 + (xx + dx) % 2
        return pl.ds(pl.multiple_of(quarter * 640, 128), 640)

    def own_part(i, _):
        at('part', i)
        cols, rows = quarter_cols(0, 0), pl.ds(pl.multiple_of(i * 512, 512), 512)
        a = xa[rows, cols]
        accq[rows, :] = dot(a, wdq[cols, :])
        acck[rows, :] = dot(a, wdkv[cols, :])
        return 0

    def kv_part(i, _):
        at('k', i)
        q = i // 2 + 1
        cols, rows = quarter_cols(q // 2, q % 2), pl.ds(pl.multiple_of((i % 2) * 1024, 1024), 1024)
        acck[rows, :] += dot(xa[rows, cols], wdkv[cols, :])
        return 0

    def q_part(x_not_y, i, _):
        at('q', i if x_not_y else i + 4)
        if not x_not_y:
            finish_kv(2 * i)
            finish_kv(2 * i + 1)
        cols, rows = quarter_cols(0, 1) if x_not_y else quarter_cols(1, 0), pl.ds(pl.multiple_of(i * 512, 512), 512)
        accq[rows, :] += dot(xa[rows, cols], wdq[cols, :])
        return 0

    cos2 = jnp.concatenate([cos_ref[...]] * (TA // S), axis=0)
    sin2 = jnp.concatenate([sin_ref[...]] * (TA // S), axis=0)

    def finish_kv(i):
        rows = pl.ds(pl.multiple_of(i * TA, TA), TA)
        kd = acck[rows, :]
        kc = kd[:, :KR]
        c = (kc * rms(kc) * gkv).astype(BF16)
        cbuf[rows, :] = c
        cT[:, rows] = c.T
        lo, hi = kd[:, KR:KR + 16], kd[:, KR + 16:]
        r = jnp.concatenate([lo * cos2 - hi * sin2, hi * cos2 + lo * sin2], axis=-1).astype(BF16)
        rbuf[rows, :] = r
        for h in range(TA // S):
            rT[i * (TA // S) + h] = r[h * S:h * S + S].T

    def finish_q(i):
        rows = pl.ds(pl.multiple_of(i * TA, TA), TA)
        qd = accq[rows, :]
        cqT[:, rows] = (qd * rms(qd) * gq).astype(BF16).T

    def last_part():
        cols = pl.ds(pl.multiple_of((fd // 2) * 640, 128), 640)

        def tile(i, _):
            pl.when(i % 2 == 0)(functools.partial(at, 'd', i // 2))
            finish_q(jnp.maximum(i - 1, 0))
            rows = pl.ds(pl.multiple_of(jnp.minimum(i, T // TA - 1) * TA, TA), TA)
            accq[rows, :] += dot(xa[rows, cols], wdq[cols, :])
            return 0
        lax.fori_loop(0, T // TA + 1, tile, 0)

    with jax.named_scope('norm'):
        lax.fori_loop(0, T // TA, norm_tile, 0)
    for n in ('dq', 'dkv'):
        local(n).wait()
    with jax.named_scope('own'):
        lax.fori_loop(0, 4, own_part, 0)
    with jax.named_scope('kv'):
        lax.fori_loop(0, 4, kv_part, 0)
    with jax.named_scope('qx'):
        lax.fori_loop(0, 4, functools.partial(q_part, True), 0)
    with jax.named_scope('kd'):
        lax.fori_loop(4, 6, kv_part, 0)
    with jax.named_scope('qy'):
        lax.fori_loop(0, 4, functools.partial(q_part, False), 0)
    with jax.named_scope('last'):
        last_part()
    outs = [pltpu.make_async_copy(cbuf, c_hbm, csem.at[0]), pltpu.make_async_copy(rT, r_hbm, csem.at[1])]
    for o in outs:
        o.start()

    keep = lax.broadcasted_iota(jnp.int32, (S, S), 0) <= lax.broadcasted_iota(jnp.int32, (S, S), 1)
    lane = lax.broadcasted_iota(jnp.int32, (S, 128), 1)
    co, si = cosT_ref[...], sinT_ref[...]
    for h in range(HG):
        zr = 128 * h + (96 if h % 2 == 0 else 32)
        qT[zr:zr + 32, :] = jnp.zeros((32, TC), BF16)

    def prepare(g, k, slot):
        col = 256 * jnp.minimum(k, 2)
        wqT[slot, pl.ds(pl.multiple_of(col, 256), 256), :] = wuq[:, pl.ds(pl.multiple_of(g * (HG * 96) + col, 128), 256)].T
        t0 = wukv[:, pl.ds(pl.multiple_of(g * (HG * 128) + 256 * k, 128), 128)]
        t1 = wukv[:, pl.ds(pl.multiple_of(g * (HG * 128) + 256 * k + 128, 128), 128)]
        lanes = pl.ds(pl.multiple_of(128 * k, 128), 128)
        wk[slot, :, lanes] = jnp.concatenate([t0[:, :64], t1[:, :64]], axis=1)
        wvT[slot, lanes, :] = jnp.concatenate([t0[:, 64:], t1[:, 64:]], axis=1).T

    def out_copy(i):
        g, tc = i // NCH, i % NCH
        return pltpu.make_async_copy(obuf.at[i % 2], attn_hbm.at[pl.ds(pl.multiple_of(tc * TC, TC), TC), pl.ds(pl.multiple_of(g * (HG * 64), 128), HG * 64)], osem.at[i % 2])

    def step(i, _):
        g, tc = i // NCH, i % NCH
        tok = pl.multiple_of(tc * TC, TC)
        at('s', i)

        @pl.when(i * (4 - i) == 0)
        def _():
            with jax.named_scope('prepare'):
                for k in range(4):
                    prepare(g, k, g % 2)

        here = g % 2
        @pl.when(i >= 2)
        def _():
            out_copy(i - 2).wait()

        slot = i % 2
        for n in range(TC // 256):
            q = dot(wqT[here], cqT[:, pl.ds(tok + 256 * n, 256)])
            cols = slice(256 * n, 256 * n + 256)
            for h in range(HG):
                nope = q[96 * h:96 * h + 64]
                lo, hi = q[96 * h + 64:96 * h + 80], q[96 * h + 80:96 * h + 96]
                b = 128 * h
                qn, qp = (b, b + 64) if h % 2 == 0 else (b + 64, b)
                qT[qn:qn + 64, cols] = nope.astype(BF16)
                qT[qp:qp + 16, cols] = (lo * co - hi * si).astype(BF16)
                qT[qp + 16:qp + 32, cols] = (hi * co + lo * si).astype(BF16)
        kbuf[...] = dot(cbuf[pl.ds(tok, TC), :], wk[here]).astype(BF16)
        vT[...] = dot(wvT[here], cT[:, pl.ds(tok, TC)]).astype(BF16)
        prepare(jnp.minimum(g + jnp.minimum(g, 1), H // HG - 1), tc, 1 - here)

        for p in range(TC // S):
            row = p * S
            r = rbuf[pl.ds(tok + row, S), :]
            z32, z64 = jnp.zeros((S, 32), BF16), jnp.zeros((S, 64), BF16)
            r_hi = jnp.concatenate([z64, r, z32], axis=1)
            r_lo = jnp.concatenate([r, z32, z64], axis=1)
            for j in range(HG // 2):
                k2 = kbuf[row:row + S, 128 * j:128 * j + 128]
                both = []
                for par in range(2):
                    h = 2 * j + par
                    k = jnp.where(lane < 64, k2, r_hi) if par == 0 else jnp.where(lane < 64, r_lo, k2)
                    both.append(attn_unit(k, qT[128 * h:128 * h + 128, row:row + S], vT[64 * h:64 * h + 64, row:row + S], keep))
                obuf[slot, row:row + S, 128 * j:128 * j + 128] = jnp.concatenate(both, axis=0).astype(BF16).T
        out_copy(i).start()
        return 0

    lax.fori_loop(0, STEPS, step, 0)
    with jax.named_scope('fin_O'):
        comm(SCHED['end'])
    with jax.named_scope('tail_out'):
        for i in (STEPS - 2, STEPS - 1):
            out_copy(i).wait()
        for o in outs:
            o.wait()
    with jax.named_scope('tail_sends'):
        for j, gb in enumerate((g1b, gqb, gkvb)):
            pltpu.make_async_copy(gb.at[pl.ds(0, 7)], gb.at[pl.ds(0, 7)], gss.at[j]).wait()
        for p in PIECES:
            take(p[0], units(p[0], 'sent'), ssem.at[PIDX[p[0]]])


def front(x, gains, ws, cos, sin):
    anyspace, vm = pl.BlockSpec(memory_space=pl.ANY), pl.BlockSpec(memory_space=pltpu.VMEM)
    V = pltpu.VMEM
    dma = pltpu.SemaphoreType.DMA
    tab = [cos, sin, np.tile(cos.T, (1, 2)), np.tile(sin.T, (1, 2))]
    return pl.pallas_call(
        front_kernel, name='front',
        in_specs=[anyspace] + [vm] * 3 + [anyspace] * 5 + [vm] * 4,
        out_specs=[anyspace] * 4,
        out_shape=[jax.ShapeDtypeStruct((T, H * VD), BF16), jax.ShapeDtypeStruct((H * VD, D), BF16), jax.ShapeDtypeStruct((T, KR), BF16), jax.ShapeDtypeStruct((T // S, RD, S), BF16)],
        scratch_shapes=[
            V((T, D), BF16), V((D, QR), BF16), V((D, KR + RD), BF16), V((QR, H * 96), BF16), V((KR, H * 128), BF16), V((320, D), BF16),
            V((8, 1, 320), BF16), V((8, 1, 96), BF16), V((8, 1, 32), BF16), V((T, QR), F32), V((T, KR + RD), F32), V((T, 128), F32),
            V((QR, T), BF16), V((T, KR), BF16), V((KR, T), BF16), V((T, RD), BF16), V((T // S, RD, S), BF16),
            V((2, HG * 96, QR), BF16), V((2, KR, HG * 64), BF16), V((2, HG * 64, KR), BF16), V((HG * 128, TC), BF16), V((TC, HG * 64), BF16), V((HG * 64, TC), BF16), V((2, TC, HG * 64), BF16),
            V((KR + RD, 320), BF16), V((320, KR + RD), BF16),
            dma((len(PIECES),)), dma((len(PIECES) - 2, 7)), dma((2, 11)), dma((len(PIECES),)), dma((3,)), dma((3,)), dma((T // TA,)), dma((3,)), dma((3,)),
        ],
        compiler_params=pltpu.CompilerParams(collective_id=0, has_side_effects=True, vmem_limit_bytes=63 << 20),
    )(x, *gains, *ws, *(jnp.asarray(t) for t in tab))


def out_kernel(o_ref, w_ref, x_ref, c_ref, r_ref, y_ref, c_out, r_out):
    for n in range(0, y_ref.shape[1], 256):
        cols = slice(n, n + 256)
        y_ref[:, cols] = (x_ref[:, cols].astype(F32) + dot(o_ref[...], w_ref[:, cols])).astype(BF16)
    c_out[...] = c_ref[...]
    r_out[...] = r_ref[...]


def outp(o, w, x, c, r, tm=1024, tn=1280):
    nt = D // tn
    cr = T // ((T // tm) * nt)
    step = lambda j, i: j * (T // tm) + i
    return pl.pallas_call(
        out_kernel, grid=(nt, T // tm), name='outp',
        in_specs=[pl.BlockSpec((tm, D), lambda j, i: (i, 0)), pl.BlockSpec((D, tn), lambda j, i: (0, j)), pl.BlockSpec((tm, tn), lambda j, i: (i, j)),
                  pl.BlockSpec((cr, KR), lambda j, i: (step(j, i), 0)), pl.BlockSpec((cr // S, RD, S), lambda j, i: (step(j, i), 0, 0))],
        out_specs=[pl.BlockSpec((tm, tn), lambda j, i: (i, j)), pl.BlockSpec((cr, KR), lambda j, i: (step(j, i), 0)), pl.BlockSpec((cr // S, RD, S), lambda j, i: (step(j, i), 0, 0))],
        out_shape=[jax.ShapeDtypeStruct((T, D), BF16), jax.ShapeDtypeStruct((T, KR), BF16), jax.ShapeDtypeStruct((T // S, RD, S), BF16)],
        compiler_params=pltpu.CompilerParams(vmem_limit_bytes=62 << 20),
    )(o, w, x, c, r)


def tables():
    half = RD // 2
    freq = np.float32(10000.0) ** (np.float32(-2.0) * np.arange(half, dtype=np.float32) / np.float32(RD))
    ang = np.arange(S, dtype=np.float32)[:, None] * freq[None, :].astype(np.float32)
    return np.cos(ang).astype(np.float32), np.sin(ang).astype(np.float32)


def solution(mesh):
    batch, row, mat = P(('dp', 'fsdp')), P('fsdp'), P('fsdp', None)

    def local(tok, g1, wdq, gq, wuq, wkv, gkv, wukv, wo):
        cos, sin = tables()
        x = tok.reshape(T, D)
        o, w, c, r = front(x, (g1[None], gq[None], gkv[None]), (wdq, wkv.T, wuq, wukv, wo), cos, sin)
        y, c, r = outp(o, w, x, c, r)
        return y.reshape(tok.shape), c.reshape(-1, S, KR), jnp.swapaxes(r, 1, 2)

    return jax.shard_map(local, mesh=mesh, in_specs=(batch, row, mat, row, mat, mat, row, mat, mat),
                         out_specs=(batch,) * 3, check_vma=False)
```

```python
import functools
import numpy as np
import jax
import jax.numpy as jnp
from jax import lax
from jax.experimental import pallas as pl
from jax.experimental.pallas import tpu as pltpu
from jax.sharding import PartitionSpec as P

F32, BF16 = jnp.float32, jnp.bfloat16
MESH = pl.DeviceIdType.MESH
EPS = 1e-6
T, D, QR, KR, RD, H, ND, VD = 2048, 2560, 768, 256, 32, 40, 64, 64
S = 128
SC = (ND + RD) ** -0.5 * 1.4426950408889634
HG, TC = 8, 512
NCH = T // TC
STEPS = (H // HG) * NCH
TA = 256


def dot(a, b):
    return jnp.dot(a, b, preferred_element_type=F32)


def rms(v):
    return lax.rsqrt(jnp.mean(v * v, axis=-1, keepdims=True) + EPS)


def attn_unit(k, qT, vT, keep):
    s = dot(k, qT) * SC
    s = jnp.where(keep, s, -1e30)
    m = jnp.max(s, axis=0, keepdims=True)
    e = jnp.exp2(s - m)
    p = (e * (1.0 / jnp.sum(e, axis=0, keepdims=True))).astype(BF16)
    return dot(vT, p)


PIECES = (
    ('dq', 'dq', False, 320, 0, 768, 112),
    ('dkv', 'dkv', False, 320, 0, 288, 112),
    ('uq0', 'uq', False, 96, 0, 768, 32),
    ('ukv0', 'ukv', True, 32, 0, 1024, 128),
    ('uq1', 'uq', False, 96, 768, 1536, 32),
    ('ukv1', 'ukv', True, 32, 1024, 2048, 768),
    ('uq2', 'uq', False, 96, 2304, 1536, 32),
    ('ukv2', 'ukv', True, 32, 3072, 2048, 768),
    ('o0', 'o', False, 320, 0, 512, 128),
    ('o1', 'o', False, 320, 512, 512, 112),
    ('o2', 'o', False, 320, 1024, 512, 80),
    ('o3', 'o', False, 320, 1536, 512, 64),
    ('o4', 'o', False, 320, 2048, 512, 96),
)
PIDX = {p[0]: i for i, p in enumerate(PIECES)}
SPLIT = ('S1a', 'S1b', 'S2a', 'S2b', 'S3a', 'S3b')
KINDS = ('XE', 'YE', 'XS', 'YS', 'S0', 'Z1', 'Z2', 'DY', 'DX', 'Z3', 'S1', 'S2', 'S3') + SPLIT
RSEM = {'XE': 0, 'YE': 0, 'XS': 1, 'YS': 1, 'Z1': 2, 'Z2': 3, 'DY': 4, 'DX': 5, 'Z3': 5, 'S0': 6, 'S1': 6, 'S2': 6, 'S3': 6}
RSEM_SPLIT = dict(RSEM, Z3=7, S1a=8, S1b=8, S2a=9, S2b=9, S3a=10, S3b=10)
SPLIT_ARRS = ('dq', 'dkv')
GROUPS = {'K': ('dkv',), 'D': ('dq',), 'U0': ('uq0', 'ukv0'), 'U1': ('uq1', 'ukv1'), 'U2': ('uq2', 'ukv2'),
          'O0': ('o0',), 'O1': ('o1',), 'O2': ('o2',), 'O3': ('o3',), 'O4': ('o4',)}
STAGES = {
    'st0': ((), ('XE', 'YE', 'XS', 'YS', 'S0')),
    'st1': (('XYE',), ('Z1', 'Z2', 'DY')),
    'st2': (('XYS',), ('DX',)),
    'st4x': (('Z1',), ('S1',)),
    'st3': (('DY',), ('Z3',)),
    'st4y': (('Z2',), ('S2',)),
    'st5': (('DXZ',), ('S3',)),
    'fin': (('SS',), ()),
    'st2d': (('XYS',), ('DX', 'S1a', 'S2a')),
    'st4xd': (('Z1',), ('S1b',)),
    'st4yd': (('Z2',), ('S2b',)),
    'st5a': (('DX',), ('S3a',)),
    'st5b': (('Z3',), ('S3b',)),
    'find': ((), ()),
}
SCHED = {
    'stats0': (('st0', 'K'), ('st0', 'D')),
    'norm1': (('st1', 'K'),),
    'norm3': (('st2d', 'K'),),
    'part0': (('recv', 'K', 'S0'), ('recv', 'D', 'S0')),
    'part1': (('st0', 'U0'),),
    'part2': (('st4xd', 'K'), ('st1', 'D')),
    'k0': (('recv', 'K', 'S1a+S1b'),),
    'k1': (('st2d', 'D'),),
    'k2': (('st0', 'U1'), ('st3', 'K'), ('st4yd', 'K'), ('st5a', 'K'), ('recv', 'K', 'S2a+S2b'), ('st4xd', 'D'), ('st1', 'U0')),
    'k3': (('st2', 'U0'),),
    'q0': (('recv', 'D', 'S1a+S1b'),),
    'q3': (('st5b', 'K'), ('st3', 'D'), ('st4yd', 'D'), ('st5a', 'D')),
    'k4': (('st4x', 'U0'), ('recv', 'K', 'S3a+S3b')),
    'q4': (('st1', 'U1'), ('recv', 'D', 'S2a+S2b')),
    'q5': (('st0', 'U2'),),
    'q6': (('st0', 'O0'), ('st5b', 'D')),
    'q7': (('st3', 'U0'), ('st4y', 'U0'), ('st2', 'U1')),
    'd0': (('recv', 'D', 'S3a+S3b'),),
    'd1': (('st4x', 'U1'),),
    'd2': (('st3', 'U1'),),
    'd4': (('st4y', 'U1'),),
    's0': (('st1', 'U2'), ('st5', 'U0'), ('fin', 'U0')),
    's1': (('st2', 'U2'), ('st0', 'O1')),
    's2': (('st4x', 'U2'), ('st1', 'O0'), ('st2', 'O0')),
    's3': (('st5', 'U1'),),
    's4': (('st3', 'U2'), ('st4y', 'U2'), ('st0', 'O2'), ('fin', 'U1')),
    's5': (('st4x', 'O0'), ('st1', 'O1')),
    's6': (('st2', 'O1'),),
    's7': (('st5', 'U2'), ('st3', 'O0'), ('st4y', 'O0'), ('st1', 'O2')),
    's8': (('st4x', 'O1'), ('st0', 'O3'), ('st0', 'O4'), ('fin', 'U2')),
    's9': (('st2', 'O2'),),
    's10': (('st3', 'O1'), ('st4y', 'O1')),
    's11': (('st5', 'O0'), ('st4x', 'O2'), ('st3', 'O2'), ('st1', 'O3')),
    's12': (('fin', 'O0'), ('st4y', 'O2')),
    's13': (('st5', 'O1'), ('st2', 'O3')),
    's14': (('fin', 'O1'), ('st1', 'O4')),
    's15': (('st4x', 'O3'), ('st2', 'O4')),
    's16': (('st5', 'O2'), ('st3', 'O3'), ('st4y', 'O3'), ('st4x', 'O4')),
    's17': (('fin', 'O2'), ('st3', 'O4'), ('st4y', 'O4')),
    's18': (('st5', 'O3'),),
    's19': (('fin', 'O3'), ('st5', 'O4')),
    'end': (('fin', 'O4'),),
    'stats1': (),
}
SWAPPED = ('uq0', 'ukv0', 'uq1', 'ukv1', 'uq2', 'ukv2', 'o0')


def front_kernel(x_hbm, g1_s, gq_s, gkv_s, dq_s, dkv_t, uq_s, ukv_s, o_s, cos_ref, sin_ref, cosT_ref, sinT_ref,
                 attn_hbm, wo_hbm, c_hbm, r_hbm,
                 xa, wdq, wdkv, wuq, wukv, ostage, g1b, gqb, gkvb, accq, acck, inv, cqT, cbuf, cT, rbuf, rT,
                 wqT, wk, wvT, qT, kbuf, vT, obuf,
                 dkv_in, dkv_s, g1sem, g1r0, g1r1, g1r2, g1r3, g1r4, g1r5, g1r6, g1r7,
                 ssem, rsem, dsem, lsem, gss, grs, xsem, osem, csem):
    z, f = lax.axis_index('dp'), lax.axis_index('fsdp')
    g1r = (g1r0, g1r1, g1r2, g1r3, g1r4, g1r5, g1r6, g1r7)
    core, xx, yy = f % 2, (f // 2) % 2, f // 4

    def idx(dx, dy, dc):
        return ((yy + dy) % 2) * 4 + ((xx + dx) % 2) * 2 + (core + dc) % 2

    fx, fy, fd = idx(1, 0, 0), idx(0, 1, 0), idx(1, 1, 0)
    dev = {'X': (z, fx), 'Y': (z, fy), 'Z': (1 - z, f), 'S': (z, idx(0, 0, 1))}
    plane = [idx(dx, dy, dc) for dx in range(2) for dy in range(2) for dc in range(2) if dx + dy + dc]
    src = {'dq': dq_s, 'dkv': dkv_s, 'uq': uq_s, 'ukv': ukv_s, 'o': ostage}
    buf = {'dq': wdq, 'dkv': wdkv, 'uq': wuq, 'ukv': wukv, 'o': wo_hbm}

    def region(piece, shard, part, base):
        name, arr, bycol, rows, c0, nc, e = piece
        n = nc if bycol else rows
        off, size = {'E': (z * (n - e), e), 'S': (e, n - 2 * e), 'A': (0, n), 'B': (z * e, n - e), 'M': ((1 - z) * (n - e), e)}[part]
        if bycol:
            row = shard * rows if base else 0
            return pl.ds(pl.multiple_of(row, 16), rows), pl.ds(pl.multiple_of(c0 + off, 128), size)
        row = (shard * rows if base else 0) + off
        return pl.ds(pl.multiple_of(row, 16), size), pl.ds(c0, nc)

    def copy(name, kind):
        piece = PIECES[PIDX[name]]
        arr = piece[1]
        shard = {'X': f, 'Y': f}.get(kind[0]) if kind in ('XE', 'YE', 'XS', 'YS') else None
        if kind in ('XE', 'YE', 'XS', 'YS', 'S0'):
            part = 'A' if kind == 'S0' else kind[1]
            r0, c0 = region(piece, f, part, False)
            r1, c1 = region(piece, f, part, True)
            s_ref, d_ref = src[arr].at[r0, c0], buf[arr].at[r1, c1]
            to = dev[kind[0]]
        else:
            shard, part, to = {'Z1': (fx, 'E', 'Z'), 'Z2': (fy, 'E', 'Z'), 'Z3': (fd, 'E', 'Z'), 'DY': (fx, 'E', 'Y'),
                               'DX': (fy, 'S', 'X'), 'S1': (fx, 'A', 'S'), 'S2': (fy, 'A', 'S'), 'S3': (fd, 'A', 'S'),
                               'S1a': (fx, 'B', 'S'), 'S1b': (fx, 'M', 'S'), 'S2a': (fy, 'B', 'S'), 'S2b': (fy, 'M', 'S'),
                               'S3a': (fd, 'B', 'S'), 'S3b': (fd, 'M', 'S')}[kind]
            if name in SWAPPED and kind in ('DX', 'DY'):
                shard, to = {'DX': (fx, 'Y'), 'DY': (fy, 'X')}[kind]
            to = dev[to]
            r1, c1 = region(piece, shard, part, True)
            s_ref = d_ref = buf[arr].at[r1, c1]
        return pltpu.make_async_remote_copy(src_ref=s_ref, dst_ref=d_ref, send_sem=ssem.at[PIDX[name]], recv_sem=rsem_of(name, kind),
                                            device_id=to, device_id_type=MESH)

    def rsem_of(name, kind):
        if PIECES[PIDX[name]][1] in SPLIT_ARRS:
            return dsem.at[PIDX[name], RSEM_SPLIT[kind]]
        return rsem.at[PIDX[name] - 2, RSEM[kind]]

    def take(name, n, sem, rows_too=True):
        _, arr, bycol, rows, c0, nc, e = PIECES[PIDX[name]]
        ref = buf[arr]
        if bycol:
            k = max(1, -(-n // nc))
            assert n % k == 0
            part = ref.at[pl.ds(0, rows * k), pl.ds(c0, n // k)]
        else:
            part = ref.at[pl.ds(0, n), pl.ds(c0, nc)]
        pltpu.make_async_copy(part, part, sem).wait()

    def units(name, what):
        _, arr, bycol, rows, c0, nc, e = PIECES[PIDX[name]]
        n = nc if bycol else rows
        return {'XYE': 2 * e, 'XYS': 2 * (n - 2 * e), 'Z1': e, 'Z2': e, 'DY': e, 'DX': n - 2 * e, 'Z3': e, 'DXZ': n - e, 'SS': 4 * n,
                'S0': n, 'S1': n, 'S2': n, 'S3': n, 'sent': 7 * n}[what]

    FIRST = {'XYE': 'XE', 'XYS': 'XS', 'DXZ': 'DX', 'SS': 'S0'}

    def local(name):
        piece = PIECES[PIDX[name]]
        r0, c0 = region(piece, f, 'A', False)
        r1, c1 = region(piece, f, 'A', True)
        return pltpu.make_async_copy(src[piece[1]].at[r0, c0], buf[piece[1]].at[r1, c1], lsem.at[PIDX[name]])

    def start(names, *kinds):
        for k in kinds:
            for n in names:
                copy(n, k).start()

    def recv(names, *kinds):
        for k in kinds:
            for n in names:
                k = {'S1a+S1b': 'S1', 'S2a+S2b': 'S2', 'S3a+S3b': 'S3'}.get(k, k)
                first = k + 'a' if k in ('S1', 'S2', 'S3') else FIRST.get(k, k)
                take(n, units(n, k), rsem_of(n, first))

    def comm(todo):
        for op in todo:
            stage, piece = op[0], op[1]
            names = GROUPS[piece]
            if stage == 'recv':
                recv(names, op[2])
                continue
            if stage == 'st0' and piece == 'O0':
                stage_o.wait()
            waits, starts = STAGES[stage]
            recv(names, *waits)
            start(names, *starts)
            if stage == 'st0':
                for n in names:
                    local(n).start()
            if stage in ('fin', 'find'):
                for n in names:
                    if piece not in ('K', 'D'):
                        local(n).wait()

    def at(seg, i):
        marks = sorted((int(n[len(seg):]), n) for n in SCHED if n.startswith(seg) and n[len(seg):].isdigit() and SCHED[n])

        def tree(ms):
            if len(ms) == 1:
                @pl.when(i == ms[0][0])
                def _():
                    with jax.named_scope('comm_' + ms[0][1]):
                        comm(SCHED[ms[0][1]])
            elif ms:
                h = len(ms) // 2
                lax.cond(i < ms[h][0], lambda: tree(ms[:h]), lambda: tree(ms[h:]))
        tree(marks)

    barrier = pltpu.get_barrier_semaphore()
    for p in plane:
        pl.semaphore_signal(barrier, inc=1, device_id=(z, p), device_id_type=MESH)
    pl.semaphore_signal(barrier, inc=1, device_id=dev['Z'], device_id_type=MESH)
    turn = pltpu.make_async_copy(dkv_t, dkv_in, csem.at[2])
    turn.start()
    stage_o = pltpu.make_async_copy(o_s, ostage, osem.at[2])

    def load_x(lo, hi):
        for i in range(lo, hi):
            pltpu.make_async_copy(x_hbm.at[pl.ds(i * TA, TA)], xa.at[pl.ds(i * TA, TA)], xsem.at[i]).start()

    load_x(0, 1)

    def stat_tile(i, _):
        pltpu.make_async_copy(x_hbm.at[pl.ds(i * TA, TA)], xa.at[pl.ds(i * TA, TA)], xsem.at[i]).wait()
        for h in range(TA // 64):
            rows = pl.ds(pl.multiple_of(i * TA + h * 64, 64), 64)
            inv[rows, :] = jnp.broadcast_to(rms(xa[rows, :].astype(F32)), (64, 128))
        return 0

    turn.wait()
    load_x(1, T // TA)
    dkv_s[...] = dkv_in[...].T
    with jax.named_scope('barrier'):
        pl.semaphore_wait(barrier, 8)

    def g1_copies():
        for r, p in enumerate(plane):
            yield pltpu.make_async_remote_copy(src_ref=g1_s, dst_ref=g1r[r + 1], send_sem=g1sem.at[0, r], recv_sem=g1sem.at[1, r],
                                               device_id=(z, p), device_id_type=MESH)
        yield pltpu.make_async_copy(g1_s, g1r[0], g1sem.at[0, 7])

    for g in g1_copies():
        g.start()
    for j, (gs, gb) in enumerate(((gq_s, gqb), (gkv_s, gkvb))):
        for p in plane:
            pltpu.make_async_remote_copy(src_ref=gs, dst_ref=gb.at[f], send_sem=gss.at[j], recv_sem=grs.at[j],
                                         device_id=(z, p), device_id_type=MESH).start()
        pltpu.make_async_copy(gs, gb.at[f], grs.at[j]).start()
    comm(SCHED['stats0'])

    stage_o.start()
    with jax.named_scope('stats_b'):
        lax.fori_loop(0, T // TA, stat_tile, 0)
    comm(SCHED['stats1'])
    with jax.named_scope('gains'):
        for g in g1_copies():
            g.wait()
        for j, gb in enumerate((gqb, gkvb)):
            pltpu.make_async_copy(gb, gb, grs.at[j]).wait()
        for r, p in enumerate([f] + plane):
            g1b[p] = g1r[r][...].astype(F32).reshape(1, 320)

    def row_of(gb):
        return jnp.concatenate([gb[i].astype(F32) for i in range(8)], axis=-1)

    g1, gq, gkv = row_of(g1b), row_of(gqb), row_of(gkvb)

    def norm_tile(i, _):
        pl.when(i % 2 == 0)(functools.partial(at, 'norm', i // 2))
        for h in range(TA // 64):
            rows = pl.ds(pl.multiple_of(i * TA + h * 64, 64), 64)
            scale = inv[rows, :]
            for j in range(D // 128):
                cols = slice(128 * j, 128 * j + 128)
                xa[rows, cols] = (xa[rows, cols].astype(F32) * scale * g1[:, cols]).astype(BF16)
        return 0

    def quarter_cols(dy, dx):
        quarter = ((yy + dy) % 2) * 2 + (xx + dx) % 2
        return pl.ds(pl.multiple_of(quarter * 640, 128), 640)

    def own_part(i, _):
        at('part', i)
        cols, rows = quarter_cols(0, 0), pl.ds(pl.multiple_of(i * 512, 512), 512)
        a = xa[rows, cols]
        accq[rows, :] = dot(a, wdq[cols, :])
        acck[rows, :] = dot(a, wdkv[cols, :])
        return 0

    def kv_part(i, _):
        at('k', i)
        q = i // 2 + 1
        cols, rows = quarter_cols(q // 2, q % 2), pl.ds(pl.multiple_of((i % 2) * 1024, 1024), 1024)
        acck[rows, :] += dot(xa[rows, cols], wdkv[cols, :])
        return 0

    def q_part(x_not_y, i, _):
        at('q', i if x_not_y else i + 4)
        if not x_not_y:
            finish_kv(2 * i)
            finish_kv(2 * i + 1)
        cols, rows = quarter_cols(0, 1) if x_not_y else quarter_cols(1, 0), pl.ds(pl.multiple_of(i * 512, 512), 512)
        accq[rows, :] += dot(xa[rows, cols], wdq[cols, :])
        return 0

    cos2 = jnp.concatenate([cos_ref[...]] * (TA // S), axis=0)
    sin2 = jnp.concatenate([sin_ref[...]] * (TA // S), axis=0)

    def finish_kv(i):
        rows = pl.ds(pl.multiple_of(i * TA, TA), TA)
        kd = acck[rows, :]
        kc = kd[:, :KR]
        c = (kc * rms(kc) * gkv).astype(BF16)
        cbuf[rows, :] = c
        cT[:, rows] = c.T
        lo, hi = kd[:, KR:KR + 16], kd[:, KR + 16:]
        r = jnp.concatenate([lo * cos2 - hi * sin2, hi * cos2 + lo * sin2], axis=-1).astype(BF16)
        rbuf[rows, :] = r
        for h in range(TA // S):
            rT[i * (TA // S) + h] = r[h * S:h * S + S].T

    def finish_q(i):
        rows = pl.ds(pl.multiple_of(i * TA, TA), TA)
        qd = accq[rows, :]
        cqT[:, rows] = (qd * rms(qd) * gq).astype(BF16).T

    def last_part():
        cols = pl.ds(pl.multiple_of((fd // 2) * 640, 128), 640)

        def tile(i, _):
            pl.when(i % 2 == 0)(functools.partial(at, 'd', i // 2))
            finish_q(jnp.maximum(i - 1, 0))
            rows = pl.ds(pl.multiple_of(jnp.minimum(i, T // TA - 1) * TA, TA), TA)
            accq[rows, :] += dot(xa[rows, cols], wdq[cols, :])
            return 0
        lax.fori_loop(0, T // TA + 1, tile, 0)

    with jax.named_scope('norm'):
        lax.fori_loop(0, T // TA, norm_tile, 0)
    for n in ('dq', 'dkv'):
        local(n).wait()
    with jax.named_scope('own'):
        lax.fori_loop(0, 4, own_part, 0)
    with jax.named_scope('kv'):
        lax.fori_loop(0, 4, kv_part, 0)
    with jax.named_scope('qx'):
        lax.fori_loop(0, 4, functools.partial(q_part, True), 0)
    with jax.named_scope('kd'):
        lax.fori_loop(4, 6, kv_part, 0)
    with jax.named_scope('qy'):
        lax.fori_loop(0, 4, functools.partial(q_part, False), 0)
    with jax.named_scope('last'):
        last_part()
    outs = [pltpu.make_async_copy(cbuf, c_hbm, csem.at[0]), pltpu.make_async_copy(rT, r_hbm, csem.at[1])]
    for o in outs:
        o.start()

    keep = lax.broadcasted_iota(jnp.int32, (S, S), 0) <= lax.broadcasted_iota(jnp.int32, (S, S), 1)
    lane = lax.broadcasted_iota(jnp.int32, (S, 128), 1)
    co, si = cosT_ref[...], sinT_ref[...]
    for h in range(HG):
        zr = 128 * h + (96 if h % 2 == 0 else 32)
        qT[zr:zr + 32, :] = jnp.zeros((32, TC), BF16)

    def prepare(g, k, slot):
        col = 256 * jnp.minimum(k, 2)
        wqT[slot, pl.ds(pl.multiple_of(col, 256), 256), :] = wuq[:, pl.ds(pl.multiple_of(g * (HG * 96) + col, 128), 256)].T
        t0 = wukv[:, pl.ds(pl.multiple_of(g * (HG * 128) + 256 * k, 128), 128)]
        t1 = wukv[:, pl.ds(pl.multiple_of(g * (HG * 128) + 256 * k + 128, 128), 128)]
        lanes = pl.ds(pl.multiple_of(128 * k, 128), 128)
        wk[slot, :, lanes] = jnp.concatenate([t0[:, :64], t1[:, :64]], axis=1)
        wvT[slot, lanes, :] = jnp.concatenate([t0[:, 64:], t1[:, 64:]], axis=1).T

    def out_copy(i):
        g, tc = i // NCH, i % NCH
        return pltpu.make_async_copy(obuf.at[i % 2], attn_hbm.at[pl.ds(pl.multiple_of(tc * TC, TC), TC), pl.ds(pl.multiple_of(g * (HG * 64), 128), HG * 64)], osem.at[i % 2])

    def step(i, _):
        g, tc = i // NCH, i % NCH
        tok = pl.multiple_of(tc * TC, TC)
        at('s', i)

        @pl.when(i * (4 - i) == 0)
        def _():
            with jax.named_scope('prepare'):
                for k in range(4):
                    prepare(g, k, g % 2)

        here = g % 2
        @pl.when(i >= 2)
        def _():
            out_copy(i - 2).wait()

        slot = i % 2
        for n in range(TC // 256):
            q = dot(wqT[here], cqT[:, pl.ds(tok + 256 * n, 256)])
            cols = slice(256 * n, 256 * n + 256)
            for h in range(HG):
                nope = q[96 * h:96 * h + 64]
                lo, hi = q[96 * h + 64:96 * h + 80], q[96 * h + 80:96 * h + 96]
                b = 128 * h
                qn, qp = (b, b + 64) if h % 2 == 0 else (b + 64, b)
                qT[qn:qn + 64, cols] = nope.astype(BF16)
                qT[qp:qp + 16, cols] = (lo * co - hi * si).astype(BF16)
                qT[qp + 16:qp + 32, cols] = (hi * co + lo * si).astype(BF16)
        kbuf[...] = dot(cbuf[pl.ds(tok, TC), :], wk[here]).astype(BF16)
        vT[...] = dot(wvT[here], cT[:, pl.ds(tok, TC)]).astype(BF16)
        prepare(jnp.minimum(g + jnp.minimum(g, 1), H // HG - 1), tc, 1 - here)

        for p in range(TC // S):
            row = p * S
            r = rbuf[pl.ds(tok + row, S), :]
            z32, z64 = jnp.zeros((S, 32), BF16), jnp.zeros((S, 64), BF16)
            r_hi = jnp.concatenate([z64, r, z32], axis=1)
            r_lo = jnp.concatenate([r, z32, z64], axis=1)
            for j in range(HG // 2):
                k2 = kbuf[row:row + S, 128 * j:128 * j + 128]
                both = []
                for par in range(2):
                    h = 2 * j + par
                    k = jnp.where(lane < 64, k2, r_hi) if par == 0 else jnp.where(lane < 64, r_lo, k2)
                    both.append(attn_unit(k, qT[128 * h:128 * h + 128, row:row + S], vT[64 * h:64 * h + 64, row:row + S], keep))
                obuf[slot, row:row + S, 128 * j:128 * j + 128] = jnp.concatenate(both, axis=0).astype(BF16).T
        out_copy(i).start()
        return 0

    lax.fori_loop(0, STEPS, step, 0)
    with jax.named_scope('fin_O'):
        comm(SCHED['end'])
    with jax.named_scope('tail_out'):
        for i in (STEPS - 2, STEPS - 1):
            out_copy(i).wait()
        for o in outs:
            o.wait()
    with jax.named_scope('tail_sends'):
        for j, gb in enumerate((gqb, gkvb)):
            pltpu.make_async_copy(gb.at[pl.ds(0, 7)], gb.at[pl.ds(0, 7)], gss.at[j]).wait()
        for p in PIECES:
            take(p[0], units(p[0], 'sent'), ssem.at[PIDX[p[0]]])


def front(x, gains, ws, cos, sin):
    anyspace, vm = pl.BlockSpec(memory_space=pl.ANY), pl.BlockSpec(memory_space=pltpu.VMEM)
    V = pltpu.VMEM
    dma = pltpu.SemaphoreType.DMA
    tab = [cos, sin, np.tile(cos.T, (1, 2)), np.tile(sin.T, (1, 2))]
    return pl.pallas_call(
        front_kernel, name='front',
        in_specs=[anyspace] + [vm] * 3 + [anyspace] * 5 + [vm] * 4,
        out_specs=[anyspace] * 4,
        out_shape=[jax.ShapeDtypeStruct((T, H * VD), BF16), jax.ShapeDtypeStruct((H * VD, D), BF16), jax.ShapeDtypeStruct((T, KR), BF16), jax.ShapeDtypeStruct((T // S, RD, S), BF16)],
        scratch_shapes=[
            V((T, D), BF16), V((D, QR), BF16), V((D, KR + RD), BF16), V((QR, H * 96), BF16), V((KR, H * 128), BF16), V((320, D), BF16),
            V((8, 1, 320), F32), V((8, 1, 96), BF16), V((8, 1, 32), BF16), V((T, QR), F32), V((T, KR + RD), F32), V((T, 128), F32),
            V((QR, T), BF16), V((T, KR), BF16), V((KR, T), BF16), V((T, RD), BF16), V((T // S, RD, S), BF16),
            V((2, HG * 96, QR), BF16), V((2, KR, HG * 64), BF16), V((2, HG * 64, KR), BF16), V((HG * 128, TC), BF16), V((TC, HG * 64), BF16), V((HG * 64, TC), BF16), V((2, TC, HG * 64), BF16),
            V((KR + RD, 320), BF16), V((320, KR + RD), BF16), dma((2, 8)),
            *[V((320,), BF16)] * 8,
            dma((len(PIECES),)), dma((len(PIECES) - 2, 7)), dma((2, 11)), dma((len(PIECES),)), dma((3,)), dma((3,)), dma((T // TA,)), dma((3,)), dma((3,)),
        ],
        compiler_params=pltpu.CompilerParams(collective_id=0, has_side_effects=True, vmem_limit_bytes=63 << 20),
    )(x, *gains, *ws, *(jnp.asarray(t) for t in tab))


def out_kernel(o_ref, w_ref, x_ref, c_ref, r_ref, y_ref, c_out, r_out):
    for n in range(0, y_ref.shape[1], 256):
        cols = slice(n, n + 256)
        y_ref[:, cols] = (x_ref[:, cols].astype(F32) + dot(o_ref[...], w_ref[:, cols])).astype(BF16)
    c_out[...] = c_ref[...]
    r_out[...] = r_ref[...]


def outp(o, w, x, c, r, tm=1024, tn=1280):
    nt = D // tn
    cr = T // ((T // tm) * nt)
    step = lambda j, i: j * (T // tm) + i
    return pl.pallas_call(
        out_kernel, grid=(nt, T // tm), name='outp',
        in_specs=[pl.BlockSpec((tm, D), lambda j, i: (i, 0)), pl.BlockSpec((D, tn), lambda j, i: (0, j)), pl.BlockSpec((tm, tn), lambda j, i: (i, j)),
                  pl.BlockSpec((cr, KR), lambda j, i: (step(j, i), 0)), pl.BlockSpec((cr // S, RD, S), lambda j, i: (step(j, i), 0, 0))],
        out_specs=[pl.BlockSpec((tm, tn), lambda j, i: (i, j)), pl.BlockSpec((cr, KR), lambda j, i: (step(j, i), 0)), pl.BlockSpec((cr // S, RD, S), lambda j, i: (step(j, i), 0, 0))],
        out_shape=[jax.ShapeDtypeStruct((T, D), BF16), jax.ShapeDtypeStruct((T, KR), BF16), jax.ShapeDtypeStruct((T // S, RD, S), BF16)],
        compiler_params=pltpu.CompilerParams(vmem_limit_bytes=62 << 20),
    )(o, w, x, c, r)


def tables():
    half = RD // 2
    freq = np.float32(10000.0) ** (np.float32(-2.0) * np.arange(half, dtype=np.float32) / np.float32(RD))
    ang = np.arange(S, dtype=np.float32)[:, None] * freq[None, :].astype(np.float32)
    return np.cos(ang).astype(np.float32), np.sin(ang).astype(np.float32)


def solution(mesh):
    batch, row, mat = P(('dp', 'fsdp')), P('fsdp'), P('fsdp', None)

    def local(tok, g1, wdq, gq, wuq, wkv, gkv, wukv, wo):
        cos, sin = tables()
        x = tok.reshape(T, D)
        o, w, c, r = front(x, (g1, gq[None], gkv[None]), (wdq, wkv.T, wuq, wukv, wo), cos, sin)
        y, c, r = outp(o, w, x, c, r)
        return y.reshape(tok.shape), c.reshape(-1, S, KR), jnp.swapaxes(r, 1, 2)

    return jax.shard_map(local, mesh=mesh, in_specs=(batch, row, mat, row, mat, mat, row, mat, mat),
                         out_specs=(batch,) * 3, check_vma=False)
```

```python
import functools
import numpy as np
import jax
import jax.numpy as jnp
from jax import lax
from jax.experimental import pallas as pl
from jax.experimental.pallas import tpu as pltpu
from jax.sharding import PartitionSpec as P

F32, BF16 = jnp.float32, jnp.bfloat16
MESH = pl.DeviceIdType.MESH
EPS = 1e-6
T, D, QR, KR, RD, H, ND, VD = 2048, 2560, 768, 256, 32, 40, 64, 64
S = 128
SC = (ND + RD) ** -0.5 * 1.4426950408889634
HG, TC = 8, 512
NCH = T // TC
STEPS = (H // HG) * NCH
TA = 256


def dot(a, b):
    return jnp.dot(a, b, preferred_element_type=F32)


def rms(v):
    return lax.rsqrt(jnp.mean(v * v, axis=-1, keepdims=True) + EPS)


def attn_unit(k, qT, vT, keep):
    s = dot(k, qT) * SC
    s = jnp.where(keep, s, -1e30)
    m = jnp.max(s, axis=0, keepdims=True)
    e = jnp.exp2(s - m)
    p = (e * (1.0 / jnp.sum(e, axis=0, keepdims=True))).astype(BF16)
    return dot(vT, p)


PIECES = (
    ('dq', 'dq', False, 320, 0, 768, 112),
    ('dkv', 'dkv', False, 320, 0, 288, 112),
    ('uq0', 'uq', False, 96, 0, 768, 32),
    ('ukv0', 'ukv', True, 32, 0, 1024, 128),
    ('uq1', 'uq', False, 96, 768, 1536, 32),
    ('ukv1', 'ukv', True, 32, 1024, 2048, 768),
    ('uq2', 'uq', False, 96, 2304, 1536, 32),
    ('ukv2', 'ukv', True, 32, 3072, 2048, 768),
    ('o0', 'o', False, 320, 0, 512, 128),
    ('o1', 'o', False, 320, 512, 512, 112),
    ('o2', 'o', False, 320, 1024, 512, 80),
    ('o3', 'o', False, 320, 1536, 512, 64),
    ('o4', 'o', False, 320, 2048, 512, 96),
)
PIDX = {p[0]: i for i, p in enumerate(PIECES)}
SPLIT = ('S1a', 'S1b', 'S2a', 'S2b', 'S3a', 'S3b')
KINDS = ('XE', 'YE', 'XS', 'YS', 'S0', 'Z1', 'Z2', 'DY', 'DX', 'Z3', 'S1', 'S2', 'S3') + SPLIT
RSEM = {'XE': 0, 'YE': 0, 'XS': 1, 'YS': 1, 'Z1': 2, 'Z2': 3, 'DY': 4, 'DX': 5, 'Z3': 5, 'S0': 6, 'S1': 6, 'S2': 6, 'S3': 6}
RSEM_SPLIT = dict(RSEM, Z3=7, S1a=8, S1b=8, S2a=9, S2b=9, S3a=10, S3b=10)
SPLIT_ARRS = ('dq', 'dkv')
GROUPS = {'K': ('dkv',), 'D': ('dq',), 'U0': ('uq0', 'ukv0'), 'U1': ('uq1', 'ukv1'), 'U2': ('uq2', 'ukv2'),
          'O0': ('o0',), 'O1': ('o1',), 'O2': ('o2',), 'O3': ('o3',), 'O4': ('o4',)}
STAGES = {
    'st0': ((), ('XE', 'YE', 'XS', 'YS', 'S0')),
    'st1': (('XYE',), ('Z1', 'Z2', 'DY')),
    'st2': (('XYS',), ('DX',)),
    'st4x': (('Z1',), ('S1',)),
    'st3': (('DY',), ('Z3',)),
    'st4y': (('Z2',), ('S2',)),
    'st5': (('DXZ',), ('S3',)),
    'fin': (('SS',), ()),
    'st2d': (('XYS',), ('DX', 'S1a', 'S2a')),
    'st4xd': (('Z1',), ('S1b',)),
    'st4yd': (('Z2',), ('S2b',)),
    'st5a': (('DX',), ('S3a',)),
    'st5b': (('Z3',), ('S3b',)),
    'find': ((), ()),
}
SCHED = {
    'stats0': (('st0', 'K'), ('st0', 'D')),
    'norm1': (('st1', 'K'),),
    'norm3': (('st2d', 'K'),),
    'part0': (('recv', 'K', 'S0'), ('recv', 'D', 'S0')),
    'part1': (('st0', 'U0'),),
    'part2': (('st4xd', 'K'), ('st1', 'D')),
    'k0': (('recv', 'K', 'S1a+S1b'),),
    'k1': (('st2d', 'D'),),
    'k2': (('st0', 'U1'), ('st3', 'K'), ('st4yd', 'K'), ('st5a', 'K'), ('recv', 'K', 'S2a+S2b'), ('st4xd', 'D'), ('st1', 'U0')),
    'k3': (('st2', 'U0'),),
    'q0': (('recv', 'D', 'S1a+S1b'),),
    'q3': (('st5b', 'K'), ('st3', 'D'), ('st4yd', 'D'), ('st5a', 'D')),
    'k4': (('st4x', 'U0'), ('recv', 'K', 'S3a+S3b')),
    'q4': (('st1', 'U1'), ('recv', 'D', 'S2a+S2b')),
    'q5': (('st0', 'U2'),),
    'q6': (('st0', 'O0'), ('st5b', 'D')),
    'q7': (('st3', 'U0'), ('st4y', 'U0'), ('st2', 'U1')),
    'd0': (('recv', 'D', 'S3a+S3b'),),
    'd1': (('st4x', 'U1'),),
    'd2': (('st3', 'U1'),),
    'd4': (('st4y', 'U1'),),
    's0': (('st1', 'U2'), ('st5', 'U0'), ('fin', 'U0')),
    's1': (('st2', 'U2'), ('st0', 'O1')),
    's2': (('st4x', 'U2'), ('st1', 'O0'), ('st2', 'O0')),
    's3': (('st5', 'U1'),),
    's4': (('st3', 'U2'), ('st4y', 'U2'), ('st0', 'O2'), ('fin', 'U1')),
    's5': (('st4x', 'O0'), ('st1', 'O1')),
    's6': (('st2', 'O1'),),
    's7': (('st5', 'U2'), ('st3', 'O0'), ('st4y', 'O0'), ('st1', 'O2')),
    's8': (('st4x', 'O1'), ('st0', 'O3'), ('st0', 'O4'), ('fin', 'U2')),
    's9': (('st2', 'O2'),),
    's10': (('st3', 'O1'), ('st4y', 'O1')),
    's11': (('st5', 'O0'), ('st4x', 'O2'), ('st3', 'O2'), ('st1', 'O3')),
    's12': (('fin', 'O0'), ('st4y', 'O2')),
    's13': (('st5', 'O1'), ('st2', 'O3')),
    's14': (('fin', 'O1'), ('st1', 'O4')),
    's15': (('st4x', 'O3'), ('st2', 'O4')),
    's16': (('st5', 'O2'), ('st3', 'O3'), ('st4y', 'O3'), ('st4x', 'O4')),
    's17': (('fin', 'O2'), ('st3', 'O4'), ('st4y', 'O4')),
    's18': (('st5', 'O3'),),
    's19': (('fin', 'O3'), ('st5', 'O4')),
    'end': (('fin', 'O4'),),
    'stats1': (),
}
SWAPPED = ('uq0', 'ukv0', 'uq1', 'ukv1', 'uq2', 'ukv2', 'o0')


def front_kernel(x_hbm, g1_s, gq_s, gkv_s, dq_s, dkv_t, uq_s, ukv_s, o_s, cos_ref, sin_ref, cosT_ref, sinT_ref,
                 attn_hbm, wo_hbm, c_hbm, r_hbm,
                 xa, wdq, wdkv, wuq, wukv, ostage, g1b, gqb, gkvb, accq, acck, inv, cqT, cbuf, cT, rbuf, rT,
                 wqT, wk, wvT, qT, kbuf, vT, obuf,
                 dkv_in, dkv_s, g1sem, g1r0, g1r1, g1r2, g1r3, g1r4, g1r5, g1r6, g1r7,
                 ssem, rsem, dsem, lsem, gss, grs, xsem, osem, csem):
    z, f = lax.axis_index('dp'), lax.axis_index('fsdp')
    g1r = (g1r0, g1r1, g1r2, g1r3, g1r4, g1r5, g1r6, g1r7)
    core, xx, yy = f % 2, (f // 2) % 2, f // 4

    def idx(dx, dy, dc):
        return ((yy + dy) % 2) * 4 + ((xx + dx) % 2) * 2 + (core + dc) % 2

    fx, fy, fd = idx(1, 0, 0), idx(0, 1, 0), idx(1, 1, 0)
    dev = {'X': (z, fx), 'Y': (z, fy), 'Z': (1 - z, f), 'S': (z, idx(0, 0, 1))}
    plane = [idx(dx, dy, dc) for dx in range(2) for dy in range(2) for dc in range(2) if dx + dy + dc]
    src = {'dq': dq_s, 'dkv': dkv_s, 'uq': uq_s, 'ukv': ukv_s, 'o': ostage}
    buf = {'dq': wdq, 'dkv': wdkv, 'uq': wuq, 'ukv': wukv, 'o': wo_hbm}

    def region(piece, shard, part, base):
        name, arr, bycol, rows, c0, nc, e = piece
        n = nc if bycol else rows
        off, size = {'E': (z * (n - e), e), 'S': (e, n - 2 * e), 'A': (0, n), 'B': (z * e, n - e), 'M': ((1 - z) * (n - e), e)}[part]
        if bycol:
            row = shard * rows if base else 0
            return pl.ds(pl.multiple_of(row, 16), rows), pl.ds(pl.multiple_of(c0 + off, 128), size)
        row = (shard * rows if base else 0) + off
        return pl.ds(pl.multiple_of(row, 16), size), pl.ds(c0, nc)

    def copy(name, kind):
        piece = PIECES[PIDX[name]]
        arr = piece[1]
        shard = {'X': f, 'Y': f}.get(kind[0]) if kind in ('XE', 'YE', 'XS', 'YS') else None
        if kind in ('XE', 'YE', 'XS', 'YS', 'S0'):
            part = 'A' if kind == 'S0' else kind[1]
            r0, c0 = region(piece, f, part, False)
            r1, c1 = region(piece, f, part, True)
            s_ref, d_ref = src[arr].at[r0, c0], buf[arr].at[r1, c1]
            to = dev[kind[0]]
        else:
            shard, part, to = {'Z1': (fx, 'E', 'Z'), 'Z2': (fy, 'E', 'Z'), 'Z3': (fd, 'E', 'Z'), 'DY': (fx, 'E', 'Y'),
                               'DX': (fy, 'S', 'X'), 'S1': (fx, 'A', 'S'), 'S2': (fy, 'A', 'S'), 'S3': (fd, 'A', 'S'),
                               'S1a': (fx, 'B', 'S'), 'S1b': (fx, 'M', 'S'), 'S2a': (fy, 'B', 'S'), 'S2b': (fy, 'M', 'S'),
                               'S3a': (fd, 'B', 'S'), 'S3b': (fd, 'M', 'S')}[kind]
            if name in SWAPPED and kind in ('DX', 'DY'):
                shard, to = {'DX': (fx, 'Y'), 'DY': (fy, 'X')}[kind]
            to = dev[to]
            r1, c1 = region(piece, shard, part, True)
            s_ref = d_ref = buf[arr].at[r1, c1]
        return pltpu.make_async_remote_copy(src_ref=s_ref, dst_ref=d_ref, send_sem=ssem.at[PIDX[name]], recv_sem=rsem_of(name, kind),
                                            device_id=to, device_id_type=MESH)

    def rsem_of(name, kind):
        if PIECES[PIDX[name]][1] in SPLIT_ARRS:
            return dsem.at[PIDX[name], RSEM_SPLIT[kind]]
        return rsem.at[PIDX[name] - 2, RSEM[kind]]

    def take(name, n, sem, rows_too=True):
        _, arr, bycol, rows, c0, nc, e = PIECES[PIDX[name]]
        ref = buf[arr]
        if bycol:
            k = max(1, -(-n // nc))
            assert n % k == 0
            part = ref.at[pl.ds(0, rows * k), pl.ds(c0, n // k)]
        else:
            part = ref.at[pl.ds(0, n), pl.ds(c0, nc)]
        pltpu.make_async_copy(part, part, sem).wait()

    def units(name, what):
        _, arr, bycol, rows, c0, nc, e = PIECES[PIDX[name]]
        n = nc if bycol else rows
        return {'XYE': 2 * e, 'XYS': 2 * (n - 2 * e), 'Z1': e, 'Z2': e, 'DY': e, 'DX': n - 2 * e, 'Z3': e, 'DXZ': n - e, 'SS': 4 * n,
                'S0': n, 'S1': n, 'S2': n, 'S3': n, 'sent': 7 * n}[what]

    FIRST = {'XYE': 'XE', 'XYS': 'XS', 'DXZ': 'DX', 'SS': 'S0'}

    def local(name):
        piece = PIECES[PIDX[name]]
        r0, c0 = region(piece, f, 'A', False)
        r1, c1 = region(piece, f, 'A', True)
        return pltpu.make_async_copy(src[piece[1]].at[r0, c0], buf[piece[1]].at[r1, c1], lsem.at[PIDX[name]])

    def start(names, *kinds):
        for k in kinds:
            for n in names:
                copy(n, k).start()

    def recv(names, *kinds):
        for k in kinds:
            for n in names:
                k = {'S1a+S1b': 'S1', 'S2a+S2b': 'S2', 'S3a+S3b': 'S3'}.get(k, k)
                first = k + 'a' if k in ('S1', 'S2', 'S3') else FIRST.get(k, k)
                take(n, units(n, k), rsem_of(n, first))

    def comm(todo):
        for op in todo:
            stage, piece = op[0], op[1]
            names = GROUPS[piece]
            if stage == 'recv':
                recv(names, op[2])
                continue
            if stage == 'st0' and piece == 'O0':
                stage_o.wait()
            waits, starts = STAGES[stage]
            recv(names, *waits)
            start(names, *starts)
            if stage == 'st0':
                for n in names:
                    local(n).start()
            if stage in ('fin', 'find'):
                for n in names:
                    if piece not in ('K', 'D'):
                        local(n).wait()

    def at(seg, i):
        marks = sorted((int(n[len(seg):]), n) for n in SCHED if n.startswith(seg) and n[len(seg):].isdigit() and SCHED[n])

        def tree(ms):
            if len(ms) == 1:
                @pl.when(i == ms[0][0])
                def _():
                    with jax.named_scope('comm_' + ms[0][1]):
                        comm(SCHED[ms[0][1]])
            elif ms:
                h = len(ms) // 2
                lax.cond(i < ms[h][0], lambda: tree(ms[:h]), lambda: tree(ms[h:]))
        tree(marks)

    barrier = pltpu.get_barrier_semaphore()
    for p in plane:
        pl.semaphore_signal(barrier, inc=1, device_id=(z, p), device_id_type=MESH)
    pl.semaphore_signal(barrier, inc=1, device_id=dev['Z'], device_id_type=MESH)
    turn = pltpu.make_async_copy(dkv_t, dkv_in, csem.at[2])
    turn.start()
    stage_o = pltpu.make_async_copy(o_s, ostage, osem.at[2])

    def load_x(lo, hi):
        for i in range(lo, hi):
            pltpu.make_async_copy(x_hbm.at[pl.ds(i * TA, TA)], xa.at[pl.ds(i * TA, TA)], xsem.at[i]).start()

    load_x(0, 1)

    def stat_tile(i, _):
        pltpu.make_async_copy(x_hbm.at[pl.ds(i * TA, TA)], xa.at[pl.ds(i * TA, TA)], xsem.at[i]).wait()
        for h in range(TA // 64):
            rows = pl.ds(pl.multiple_of(i * TA + h * 64, 64), 64)
            inv[rows, :] = jnp.broadcast_to(rms(xa[rows, :].astype(F32)), (64, 128))
        return 0

    turn.wait()
    load_x(1, T // TA)
    dkv_s[...] = dkv_in[...].T
    with jax.named_scope('barrier'):
        pl.semaphore_wait(barrier, 8)

    def g1_copies():
        for r, p in enumerate(plane):
            yield pltpu.make_async_remote_copy(src_ref=g1_s, dst_ref=g1r[r + 1], send_sem=g1sem.at[0, r], recv_sem=g1sem.at[1, r],
                                               device_id=(z, p), device_id_type=MESH)
        yield pltpu.make_async_copy(g1_s, g1r[0], g1sem.at[0, 7])

    for g in g1_copies():
        g.start()
    for j, (gs, gb) in enumerate(((gq_s, gqb), (gkv_s, gkvb))):
        for p in plane:
            pltpu.make_async_remote_copy(src_ref=gs, dst_ref=gb.at[f], send_sem=gss.at[j], recv_sem=grs.at[j],
                                         device_id=(z, p), device_id_type=MESH).start()
        pltpu.make_async_copy(gs, gb.at[f], grs.at[j]).start()
    comm(SCHED['stats0'])

    stage_o.start()
    with jax.named_scope('stats_b'):
        lax.fori_loop(0, T // TA, stat_tile, 0)
    comm(SCHED['stats1'])
    with jax.named_scope('gains'):
        for g in g1_copies():
            g.wait()
        for j, gb in enumerate((gqb, gkvb)):
            pltpu.make_async_copy(gb, gb, grs.at[j]).wait()
        for r, p in enumerate([f] + plane):
            g1b[p] = g1r[r][...].astype(F32).reshape(1, 320)

    def row_of(gb):
        return jnp.concatenate([gb[i].astype(F32) for i in range(8)], axis=-1)

    g1, gq, gkv = row_of(g1b), row_of(gqb), row_of(gkvb)

    def norm_tile(i, _):
        pl.when(i % 2 == 0)(functools.partial(at, 'norm', i // 2))
        for h in range(TA // 64):
            rows = pl.ds(pl.multiple_of(i * TA + h * 64, 64), 64)
            scale = inv[rows, :]
            for j in range(D // 128):
                cols = slice(128 * j, 128 * j + 128)
                xa[rows, cols] = (xa[rows, cols].astype(F32) * scale * g1[:, cols]).astype(BF16)
        return 0

    def quarter_cols(dy, dx):
        quarter = ((yy + dy) % 2) * 2 + (xx + dx) % 2
        return pl.ds(pl.multiple_of(quarter * 640, 128), 640)

    def own_part(i, _):
        at('part', i)
        cols, rows = quarter_cols(0, 0), pl.ds(pl.multiple_of(i * 512, 512), 512)
        a = xa[rows, cols]
        accq[rows, :] = dot(a, wdq[cols, :])
        acck[rows, :] = dot(a, wdkv[cols, :])
        return 0

    def kv_part(i, _):
        at('k', i)
        q = i // 2 + 1
        cols, rows = quarter_cols(q // 2, q % 2), pl.ds(pl.multiple_of((i % 2) * 1024, 1024), 1024)
        acck[rows, :] += dot(xa[rows, cols], wdkv[cols, :])
        return 0

    def q_part(x_not_y, i, _):
        at('q', i if x_not_y else i + 4)
        if not x_not_y:
            finish_kv(2 * i)
            finish_kv(2 * i + 1)
        cols, rows = quarter_cols(0, 1) if x_not_y else quarter_cols(1, 0), pl.ds(pl.multiple_of(i * 512, 512), 512)
        accq[rows, :] += dot(xa[rows, cols], wdq[cols, :])
        return 0

    cos2 = jnp.concatenate([cos_ref[...]] * (TA // S), axis=0)
    sin2 = jnp.concatenate([sin_ref[...]] * (TA // S), axis=0)

    def finish_kv(i):
        rows = pl.ds(pl.multiple_of(i * TA, TA), TA)
        kd = acck[rows, :]
        kc = kd[:, :KR]
        c = (kc * rms(kc) * gkv).astype(BF16)
        cbuf[rows, :] = c
        cT[:, rows] = c.T
        lo, hi = kd[:, KR:KR + 16], kd[:, KR + 16:]
        r = jnp.concatenate([lo * cos2 - hi * sin2, hi * cos2 + lo * sin2], axis=-1).astype(BF16)
        rbuf[rows, :] = r
        for h in range(TA // S):
            rT[i * (TA // S) + h] = r[h * S:h * S + S].T

    def finish_q(i):
        rows = pl.ds(pl.multiple_of(i * TA, TA), TA)
        qd = accq[rows, :]
        cqT[:, rows] = (qd * rms(qd) * gq).astype(BF16).T

    def last_part():
        cols = pl.ds(pl.multiple_of((fd // 2) * 640, 128), 640)

        def tile(i, _):
            at('d', i)
            before = jnp.maximum(i - 1, 0)
            finish_q(2 * before)
            finish_q(2 * before + 1)
            rows = pl.ds(pl.multiple_of(jnp.minimum(i, T // 512 - 1) * 512, 512), 512)
            accq[rows, :] += dot(xa[rows, cols], wdq[cols, :])
            return 0
        lax.fori_loop(0, T // 512 + 1, tile, 0)

    with jax.named_scope('norm'):
        lax.fori_loop(0, T // TA, norm_tile, 0)
    for n in ('dq', 'dkv'):
        local(n).wait()
    with jax.named_scope('own'):
        lax.fori_loop(0, 4, own_part, 0)
    with jax.named_scope('kv'):
        lax.fori_loop(0, 4, kv_part, 0)
    with jax.named_scope('qx'):
        lax.fori_loop(0, 4, functools.partial(q_part, True), 0)
    with jax.named_scope('kd'):
        lax.fori_loop(4, 6, kv_part, 0)
    with jax.named_scope('qy'):
        lax.fori_loop(0, 4, functools.partial(q_part, False), 0)
    with jax.named_scope('last'):
        last_part()
    outs = [pltpu.make_async_copy(cbuf, c_hbm, csem.at[0]), pltpu.make_async_copy(rT, r_hbm, csem.at[1])]
    for o in outs:
        o.start()

    keep = lax.broadcasted_iota(jnp.int32, (S, S), 0) <= lax.broadcasted_iota(jnp.int32, (S, S), 1)
    lane = lax.broadcasted_iota(jnp.int32, (S, 128), 1)
    co, si = cosT_ref[...], sinT_ref[...]
    for h in range(HG):
        zr = 128 * h + (96 if h % 2 == 0 else 32)
        qT[zr:zr + 32, :] = jnp.zeros((32, TC), BF16)

    def prepare(g, k, slot):
        col = 256 * jnp.minimum(k, 2)
        wqT[slot, pl.ds(pl.multiple_of(col, 256), 256), :] = wuq[:, pl.ds(pl.multiple_of(g * (HG * 96) + col, 128), 256)].T
        t0 = wukv[:, pl.ds(pl.multiple_of(g * (HG * 128) + 256 * k, 128), 128)]
        t1 = wukv[:, pl.ds(pl.multiple_of(g * (HG * 128) + 256 * k + 128, 128), 128)]
        lanes = pl.ds(pl.multiple_of(128 * k, 128), 128)
        wk[slot, :, lanes] = jnp.concatenate([t0[:, :64], t1[:, :64]], axis=1)
        wvT[slot, lanes, :] = jnp.concatenate([t0[:, 64:], t1[:, 64:]], axis=1).T

    def out_copy(i):
        g, tc = i // NCH, i % NCH
        return pltpu.make_async_copy(obuf.at[i % 2], attn_hbm.at[pl.ds(pl.multiple_of(tc * TC, TC), TC), pl.ds(pl.multiple_of(g * (HG * 64), 128), HG * 64)], osem.at[i % 2])

    def step(i, _):
        g, tc = i // NCH, i % NCH
        tok = pl.multiple_of(tc * TC, TC)
        at('s', i)

        @pl.when(i * (4 - i) == 0)
        def _():
            with jax.named_scope('prepare'):
                for k in range(4):
                    prepare(g, k, g % 2)

        here = g % 2
        @pl.when(i >= 2)
        def _():
            out_copy(i - 2).wait()

        slot = i % 2
        for n in range(TC // 256):
            q = dot(wqT[here], cqT[:, pl.ds(tok + 256 * n, 256)])
            cols = slice(256 * n, 256 * n + 256)
            for h in range(HG):
                nope = q[96 * h:96 * h + 64]
                lo, hi = q[96 * h + 64:96 * h + 80], q[96 * h + 80:96 * h + 96]
                b = 128 * h
                qn, qp = (b, b + 64) if h % 2 == 0 else (b + 64, b)
                qT[qn:qn + 64, cols] = nope.astype(BF16)
                qT[qp:qp + 16, cols] = (lo * co - hi * si).astype(BF16)
                qT[qp + 16:qp + 32, cols] = (hi * co + lo * si).astype(BF16)
        kbuf[...] = dot(cbuf[pl.ds(tok, TC), :], wk[here]).astype(BF16)
        vT[...] = dot(wvT[here], cT[:, pl.ds(tok, TC)]).astype(BF16)
        prepare(jnp.minimum(g + jnp.minimum(g, 1), H // HG - 1), tc, 1 - here)

        for p in range(TC // S):
            row = p * S
            r = rbuf[pl.ds(tok + row, S), :]
            z32, z64 = jnp.zeros((S, 32), BF16), jnp.zeros((S, 64), BF16)
            r_hi = jnp.concatenate([z64, r, z32], axis=1)
            r_lo = jnp.concatenate([r, z32, z64], axis=1)
            for j in range(HG // 2):
                k2 = kbuf[row:row + S, 128 * j:128 * j + 128]
                both = []
                for par in range(2):
                    h = 2 * j + par
                    k = jnp.where(lane < 64, k2, r_hi) if par == 0 else jnp.where(lane < 64, r_lo, k2)
                    both.append(attn_unit(k, qT[128 * h:128 * h + 128, row:row + S], vT[64 * h:64 * h + 64, row:row + S], keep))
                obuf[slot, row:row + S, 128 * j:128 * j + 128] = jnp.concatenate(both, axis=0).astype(BF16).T
        out_copy(i).start()
        return 0

    lax.fori_loop(0, STEPS, step, 0)
    with jax.named_scope('fin_O'):
        comm(SCHED['end'])
    with jax.named_scope('tail_sends'):
        for j, gb in enumerate((gqb, gkvb)):
            pltpu.make_async_copy(gb.at[pl.ds(0, 7)], gb.at[pl.ds(0, 7)], gss.at[j]).wait()
        for p in PIECES:
            take(p[0], units(p[0], 'sent'), ssem.at[PIDX[p[0]]])
    with jax.named_scope('tail_out'):
        for i in (STEPS - 2, STEPS - 1):
            out_copy(i).wait()
        for o in outs:
            o.wait()


def front(x, gains, ws, cos, sin):
    anyspace, vm = pl.BlockSpec(memory_space=pl.ANY), pl.BlockSpec(memory_space=pltpu.VMEM)
    V = pltpu.VMEM
    dma = pltpu.SemaphoreType.DMA
    tab = [cos, sin, np.tile(cos.T, (1, 2)), np.tile(sin.T, (1, 2))]
    return pl.pallas_call(
        front_kernel, name='front',
        in_specs=[anyspace] + [vm] * 3 + [anyspace] * 5 + [vm] * 4,
        out_specs=[anyspace] * 4,
        out_shape=[jax.ShapeDtypeStruct((T, H * VD), BF16), jax.ShapeDtypeStruct((H * VD, D), BF16), jax.ShapeDtypeStruct((T, KR), BF16), jax.ShapeDtypeStruct((T // S, RD, S), BF16)],
        scratch_shapes=[
            V((T, D), BF16), V((D, QR), BF16), V((D, KR + RD), BF16), V((QR, H * 96), BF16), V((KR, H * 128), BF16), V((320, D), BF16),
            V((8, 1, 320), F32), V((8, 1, 96), BF16), V((8, 1, 32), BF16), V((T, QR), F32), V((T, KR + RD), F32), V((T, 128), F32),
            V((QR, T), BF16), V((T, KR), BF16), V((KR, T), BF16), V((T, RD), BF16), V((T // S, RD, S), BF16),
            V((2, HG * 96, QR), BF16), V((2, KR, HG * 64), BF16), V((2, HG * 64, KR), BF16), V((HG * 128, TC), BF16), V((TC, HG * 64), BF16), V((HG * 64, TC), BF16), V((2, TC, HG * 64), BF16),
            V((KR + RD, 320), BF16), V((320, KR + RD), BF16), dma((2, 8)),
            *[V((320,), BF16)] * 8,
            dma((len(PIECES),)), dma((len(PIECES) - 2, 7)), dma((2, 11)), dma((len(PIECES),)), dma((3,)), dma((3,)), dma((T // TA,)), dma((3,)), dma((3,)),
        ],
        compiler_params=pltpu.CompilerParams(collective_id=0, has_side_effects=True, vmem_limit_bytes=63 << 20),
    )(x, *gains, *ws, *(jnp.asarray(t) for t in tab))


def out_kernel(o_ref, w_ref, x_ref, c_ref, r_ref, y_ref, c_out, r_out):
    for n in range(0, y_ref.shape[1], 256):
        cols = slice(n, n + 256)
        y_ref[:, cols] = (x_ref[:, cols].astype(F32) + dot(o_ref[...], w_ref[:, cols])).astype(BF16)
    c_out[...] = c_ref[...]
    r_out[...] = r_ref[...]


def outp(o, w, x, c, r, tm=1024, tn=1280):
    nt = D // tn
    cr = T // ((T // tm) * nt)
    step = lambda j, i: j * (T // tm) + i
    return pl.pallas_call(
        out_kernel, grid=(nt, T // tm), name='outp',
        in_specs=[pl.BlockSpec((tm, D), lambda j, i: (i, 0)), pl.BlockSpec((D, tn), lambda j, i: (0, j)), pl.BlockSpec((tm, tn), lambda j, i: (i, j)),
                  pl.BlockSpec((cr, KR), lambda j, i: (step(j, i), 0)), pl.BlockSpec((cr // S, RD, S), lambda j, i: (step(j, i), 0, 0))],
        out_specs=[pl.BlockSpec((tm, tn), lambda j, i: (i, j)), pl.BlockSpec((cr, KR), lambda j, i: (step(j, i), 0)), pl.BlockSpec((cr // S, RD, S), lambda j, i: (step(j, i), 0, 0))],
        out_shape=[jax.ShapeDtypeStruct((T, D), BF16), jax.ShapeDtypeStruct((T, KR), BF16), jax.ShapeDtypeStruct((T // S, RD, S), BF16)],
        compiler_params=pltpu.CompilerParams(vmem_limit_bytes=62 << 20),
    )(o, w, x, c, r)


def tables():
    half = RD // 2
    freq = np.float32(10000.0) ** (np.float32(-2.0) * np.arange(half, dtype=np.float32) / np.float32(RD))
    ang = np.arange(S, dtype=np.float32)[:, None] * freq[None, :].astype(np.float32)
    return np.cos(ang).astype(np.float32), np.sin(ang).astype(np.float32)


def solution(mesh):
    batch, row, mat = P(('dp', 'fsdp')), P('fsdp'), P('fsdp', None)

    def local(tok, g1, wdq, gq, wuq, wkv, gkv, wukv, wo):
        cos, sin = tables()
        x = tok.reshape(T, D)
        o, w, c, r = front(x, (g1, gq[None], gkv[None]), (wdq, wkv.T, wuq, wukv, wo), cos, sin)
        y, c, r = outp(o, w, x, c, r)
        return y.reshape(tok.shape), c.reshape(-1, S, KR), jnp.swapaxes(r, 1, 2)

    return jax.shard_map(local, mesh=mesh, in_specs=(batch, row, mat, row, mat, mat, row, mat, mat),
                         out_specs=(batch,) * 3, check_vma=False)
```
